256 devices in a mesh: shard: 64 (over z, y, core), model: 4 (over x).
Axes of the slice: x: 4, y: 4, z: 8, core: 2. Of those that a mesh axis runs over, the one named last changes fastest.
Arguments:
- one_gate: float32 [2048, 8192], P('shard', 'model'), may hold values from -0.375 to 0.375
- other_gate: float32 [2048, 8192], P('shard', 'model'), may hold values from -0.125 to 0.125
- one_up: float32 [2048, 8192], P('shard', 'model'), may hold values from -0.375 to 0.375
- other_up: float32 [2048, 8192], P('shard', 'model'), may hold values from -0.125 to 0.125
- mix_share: float32 [2048], P('shard'), may hold values from 0.2 to 0.8
- norm_train: float32 [2048], P(('shard', 'model')), may hold values from 0.25 to 1.75
- norm_step: float32 [2048], P(('shard', 'model')), may hold values from -0.3 to 0.3
Outputs:
- final_gate: bfloat16 [2048, 8192], P(None, 'model')
- final_up: bfloat16 [2048, 8192], P(None, 'model')
- column_gate: float32 [8192], P('model')
- column_up: float32 [8192], P('model')
- serve_norm: bfloat16 [2048], replicated
The draws below stay inside these ranges and needn't reach their ends.
All inputs are finite; a program needn't handle non-finite values. Where the reference program divides by a largest or mean magnitude, that divisor is 1e-20 or more.
Results may differ from the reference program's by a relative error of at most 0.001.
Values may be sent and summed in bfloat16 or wider, within the bound.
A program may use at most 128 MiB of HBM per device.

```python
import jax
import jax.numpy as jnp

D_MODEL = 2048
D_INNER = 8192


def spiked(entries, rng, source, target, blocks, factor):
    def block_of(position):
        return (jnp.arange(entries.shape[position]) // (entries.shape[position] // blocks)).reshape((-1,) + (1,) * (entries.ndim - 1 - position))

    first = jax.random.permutation(rng, blocks)[block_of(target)]
    far = (block_of(target) + blocks // 2) % blocks
    return jnp.where((block_of(source) == first) | (block_of(source) == far), factor * entries, entries)


def level_of(rng, extent, shards, smallest, top_value):
    gain = 1.0
    for axis_at, parts in shards:
        draws = jax.random.uniform(jax.random.fold_in(jax.random.fold_in(rng, 6), axis_at), (parts,), jnp.float32, smallest / len(shards), top_value / len(shards))
        gain = gain * jnp.repeat(jnp.exp(draws), extent[axis_at] // parts).reshape((-1,) + (1,) * (len(extent) - 1 - axis_at))
    return gain


def centred(own_key, shape, scale, reach, split=(), held_as=jnp.bfloat16):
    values = scale * jax.random.normal(own_key, shape, jnp.float32)
    if split:
        values = values * level_of(own_key, shape, split, -0.22, 0.18)
    return jnp.clip(values, -reach, reach).astype(held_as)


def bell_draw_with(own_key, shape, width, limit, shards, heavy, kind=jnp.bfloat16):
    values = width * jax.random.normal(own_key, shape, jnp.float32)
    if shards:
        values = values * level_of(own_key, shape, shards, -0.22, 0.18)
    return jnp.clip(spiked(values, jax.random.fold_in(own_key, 3), *heavy), -limit, limit).astype(kind)


def setup_inputs(seed: int = 0) -> dict:
    keys = jax.random.split(jax.random.key(seed), 8)
    one_gate = bell_draw_with(keys[0], (D_MODEL, D_INNER), D_MODEL ** -0.5, 0.375, ((0, 64), (1, 4)), (0, 1, 64, 4.0), jnp.float32)
    other_gate = centred(keys[1], (D_MODEL, D_INNER), D_MODEL ** -0.5, 0.125, ((0, 64), (1, 4)), jnp.float32)
    one_up = bell_draw_with(keys[2], (D_MODEL, D_INNER), D_MODEL ** -0.5, 0.375, ((0, 64), (1, 4)), (0, 1, 64, 4.0), jnp.float32)
    other_up = centred(keys[3], (D_MODEL, D_INNER), D_MODEL ** -0.5, 0.125, ((0, 64), (1, 4)), jnp.float32)
    mix_share = jnp.clip(0.2 + 0.6 * jax.random.uniform(keys[4], (D_MODEL,), jnp.float32) ** level_of(keys[4], (D_MODEL,), ((0, 64),), -0.2, 0.2), 0.2, 0.8)
    norm_train = jnp.clip(1.0 + 0.15 * jax.random.normal(keys[5], (D_MODEL,), jnp.float32), 0.25, 1.75)
    norm_step = jnp.clip(jax.random.uniform(keys[6], (D_MODEL,), jnp.float32, -0.3, 0.3) * level_of(keys[6], (D_MODEL,), ((0, 256),), -0.4, 0.0), -0.3, 0.3)
    return {"one_gate": one_gate, "other_gate": other_gate, "one_up": one_up, "other_up": other_up, "mix_share": mix_share, "norm_train": norm_train, "norm_step": norm_step}


def reference(one_gate, other_gate, one_up, other_up, mix_share, norm_train, norm_step):
    result_gate = mix_share[:, None] * one_gate + (1.0 - mix_share[:, None]) * other_gate
    result_up = mix_share[:, None] * one_up + (1.0 - mix_share[:, None]) * other_up
    column_gate = jnp.max(jnp.abs(result_gate), axis=0)
    final_gate = (result_gate / column_gate).astype(jnp.bfloat16)
    column_up = jnp.max(jnp.abs(result_up), axis=0)
    final_up = (result_up / column_up).astype(jnp.bfloat16)
    serve_norm = (norm_train + norm_step).astype(jnp.bfloat16)
    return final_gate, final_up, column_gate, column_up, serve_norm
```

```python
import heapq

import jax
import jax.numpy as jnp
from jax import lax
from jax.experimental import pallas as pl
from jax.experimental.pallas import tpu as pltpu
from jax.sharding import Mesh
from jax.sharding import PartitionSpec as P

SHARD = ("shard_0", "shard_1", "shard_2")
SHARD_MODEL = ("shard_0", "shard_1", "shard_2", "model")

Z, Y, C, X = 8, 4, 2, 4
ROWS, COLS, OWN = 2048, 2048, 32
CHIP = C * OWN
TILES = COLS // 128
LOW = -3.0e38

PIECES = (("B", 0, 6, 11), ("B", 1, 11, 16), ("A", 0, 0, 3), ("A", 1, 3, 6))


def reach(half, n):
    return (n // 2, n // 2 - 1) if half == 0 else (n // 2 - 1, n // 2)


def forwards(piece, dz, dy):
    kind, half = PIECES[piece][:2]
    zp, zm = reach(half, Z)
    yp, ym = reach(half, Y)
    along_z, along_y = [], []
    if 0 <= dz < zp:
        along_z.append(("z+", dz + 1, dy))
    if -zm < dz <= 0:
        along_z.append(("z-", dz - 1, dy))
    if 0 <= dy < yp:
        along_y.append(("y+", dz, dy + 1))
    if -ym < dy <= 0:
        along_y.append(("y-", dz, dy - 1))
    if kind == "A":
        return along_z + (along_y if dz == 0 else [])
    return (along_z if dy == 0 else []) + along_y


def arrivals(hop=2.0, turn=0.05, rate=1.0 / 5.6):
    free = dict.fromkeys(("y+", "y-", "z+", "z-"), 0.0)
    queue, count, clock, order = [], 0, 0.0, []

    def issue(piece, dz, dy, at):
        nonlocal count
        for link, z, y in forwards(piece, dz, dy):
            width = (PIECES[piece][3] - PIECES[piece][2]) / TILES
            free[link] = max(at, free[link]) + width / rate
            count += 1
            heapq.heappush(queue, (free[link] + hop, count, piece, z, y))

    for piece in range(len(PIECES)):
        issue(piece, 0, 0, clock)
        clock += 2 * turn
    while queue:
        at, _, piece, dz, dy = heapq.heappop(queue)
        clock = max(clock, at) + turn
        order.append((piece, dz, dy))
        issue(piece, dz, dy, clock)
        clock += turn
    return order


def gather_kernel(
    mix_h, one_g, other_g, one_u, other_u, train_h, step_h,
    out, cols, norm,
    mix, train, step, ins, theirs, x, peak, peak_y, peak1, peak_z, peak2,
    row0, row_x, row1, row_c, row2, row_y,
    in_sem, x_sem, peak_send, y_sem, z_sem, col_sem, norm_send, norm_sem,
    send_sem, recv_sem, side_send, side_recv,
):
    z, y, c, m = (lax.axis_index(a) for a in ("shard_0", "shard_1", "shard_2", "model"))

    def device(z, y, c, m):
        return (z, y, c, m)

    z_at = [device(lax.rem(z + d, Z), y, c, m) for d in range(Z)]
    y_at = [device(z, lax.rem(y + d, Y), c, m) for d in range(Y)]
    m_at = [device(z, y, c, lax.rem(m + d, X)) for d in range(X)]
    sibling = device(z, y, 1 - c, m)
    link_to = {"z+": z_at[1], "z-": z_at[Z - 1], "y+": y_at[1], "y-": y_at[Y - 1]}

    def remote(src, dst, send, recv, to):
        return pltpu.make_async_remote_copy(
            src_ref=src, dst_ref=dst, send_sem=send, recv_sem=recv,
            device_id=to, device_id_type=pl.DeviceIdType.MESH,
        )

    partners = [sibling, *y_at[1:], *z_at[1:], *m_at[1:]]
    barrier = pltpu.get_barrier_semaphore()
    for to in partners:
        pl.semaphore_signal(barrier, inc=1, device_id=to, device_id_type=pl.DeviceIdType.MESH)

    gate, up = 2 * (1 - c), 2 * c
    small = [
        pltpu.make_async_copy(mix_h, mix, in_sem.at[4]),
        pltpu.make_async_copy(train_h, train, in_sem.at[5]),
        pltpu.make_async_copy(step_h, step, in_sem.at[6]),
    ]
    large = [
        pltpu.make_async_copy(one_g, ins.at[gate], in_sem.at[gate]),
        pltpu.make_async_copy(other_g, ins.at[gate + 1], in_sem.at[gate + 1]),
        pltpu.make_async_copy(one_u, ins.at[up], in_sem.at[up]),
        pltpu.make_async_copy(other_u, ins.at[up + 1], in_sem.at[up + 1]),
    ]
    for copy in small + large:
        copy.start()
    for copy in small:
        copy.wait()

    sub = lax.broadcasted_iota(jnp.int32, (8, 128), 0)
    shares = []
    for r in range(OWN // 8):
        share = jnp.full((8, 128), mix[8 * r], jnp.float32)
        for i in range(1, 8):
            share = jnp.where(sub == i, mix[8 * r + i], share)
        shares.append((share, 1.0 - share))

    def blend(slot, store):
        for k in (slot, slot + 1):
            pltpu.make_async_copy(one_g, ins.at[k], in_sem.at[k]).wait()
        for t in range(TILES):
            lanes = slice(128 * t, 128 * t + 128)
            for r, (share, rest) in enumerate(shares):
                rows = slice(8 * r, 8 * r + 8)
                store(r, lanes, share * ins[slot, rows, lanes] + rest * ins[slot + 1, rows, lanes])

    def store_theirs(r, lanes, value):
        theirs[8 * r : 8 * r + 8, lanes] = value

    def store_own(r, lanes, value):
        x[pl.ds(pl.multiple_of(OWN * c + 8 * r, 8), 8), lanes] = value

    blend(0, store_theirs)

    lane2 = lax.broadcasted_iota(jnp.int32, (2, 128), 1)
    sub2 = lax.broadcasted_iota(jnp.int32, (2, 128), 0)
    start = (lax.rem(y, 2) * C + c) * OWN + m * 8
    line = jnp.full((2, 128), LOW, jnp.float32)
    for i in range(8):
        line = jnp.where((lane2 == start + i) & (sub2 == y // 2), train[i] + step[i], line)
    row0[...] = line

    pl.semaphore_wait(barrier, len(partners))

    to_sibling = remote(
        theirs, x.at[pl.ds(pl.multiple_of(OWN * c, OWN), OWN)], x_sem.at[0], x_sem.at[1], sibling
    )
    to_sibling.start()
    norm_x = [remote(row0, row_x.at[d], norm_send.at[0], norm_sem.at[d], m_at[d]) for d in range(1, X)]
    for copy in norm_x:
        copy.start()
    blend(2, store_own)

    def peak_of(t, first):
        lanes = slice(128 * t, 128 * t + 128)
        best = jnp.abs(x[pl.ds(pl.multiple_of(first, 8), 8), lanes])
        for r in range(1, OWN // 8):
            best = jnp.maximum(best, jnp.abs(x[pl.ds(pl.multiple_of(first + 8 * r, 8), 8), lanes]))
        return best

    own_peaks = [peak_of(t, OWN * c) for t in range(TILES)]
    to_sibling.wait_recv()
    for t in range(TILES):
        best = jnp.maximum(own_peaks[t], peak_of(t, OWN * (1 - c)))
        peak[t : t + 1, :] = jnp.max(best, axis=0, keepdims=True)

    over_y = [remote(peak, peak_y.at[d], peak_send.at[0], y_sem.at[d], y_at[d]) for d in range(1, Y)]
    for copy in over_y:
        copy.start()
    best = peak[...]
    for d, copy in enumerate(over_y, 1):
        copy.wait_recv()
        best = jnp.maximum(best, peak_y[d])
    peak1[...] = best

    over_z = [remote(peak1, peak_z.at[d], peak_send.at[1], z_sem.at[d], z_at[d]) for d in range(1, Z)]
    for copy in over_z:
        copy.start()
    for d, copy in enumerate(over_z, 1):
        copy.wait_recv()
        best = jnp.maximum(best, peak_z[d])
    peak2[...] = best
    cols[c] = best

    def block_at(dz, dy):
        chip = lax.rem(z - dz + Z, Z) * Y + lax.rem(y - dy + Y, Y)
        return pl.multiple_of(chip * CHIP, CHIP)

    home = block_at(0, 0)

    def scale(piece):
        for t in range(*PIECES[piece][2:]):
            lanes = slice(128 * t, 128 * t + 128)
            by = jnp.broadcast_to(peak2[t : t + 1, :], (16, 128))
            for r in range(CHIP // 16):
                rows = pl.ds(pl.multiple_of(home + 16 * r, 16), 16)
                out[c, rows, lanes] = (x[16 * r : 16 * r + 16, lanes] / by).astype(jnp.bfloat16)

    def flag(piece, dz, dy):
        return recv_sem.at[piece, (dz % Z) * Y + dy % Y]

    def part(piece, base):
        first, last = PIECES[piece][2:]
        return out.at[c, pl.ds(base, CHIP), pl.ds(128 * first, 128 * (last - first))]

    def send_on(piece, dz, dy, base):
        ref = part(piece, base)
        for link, to_z, to_y in forwards(piece, dz, dy):
            remote(ref, ref, send_sem.at[0], flag(piece, to_z, to_y), link_to[link]).start()

    def send_aside(base):
        ref = out.at[c, pl.ds(base, CHIP)]
        remote(ref, ref, side_send.at[0], side_recv.at[0], sibling).start()

    scale(0)
    for piece in range(len(PIECES)):
        if piece + 1 < len(PIECES):
            scale(piece + 1)
        send_on(piece, 0, 0, home)
    send_aside(home)
    col_copy = remote(cols.at[c], cols.at[c], col_sem.at[0], col_sem.at[1], sibling)
    col_copy.start()

    n_wait = {}

    def norm_over_x():
        line = row0[...]
        for d, copy in enumerate(norm_x, 1):
            copy.wait_recv()
            line = jnp.maximum(line, row_x[d])
        row1[...] = line
        n_wait["c"] = remote(row1, row_c, norm_send.at[1], norm_sem.at[4], sibling)
        n_wait["c"].start()

    def norm_over_core():
        n_wait["c"].wait_recv()
        row2[...] = jnp.maximum(row1[...], row_c[...])
        n_wait["y"] = [
            remote(row2, row_y.at[d], norm_send.at[2], norm_sem.at[4 + d], y_at[d]) for d in range(1, Y)
        ]
        for copy in n_wait["y"]:
            copy.start()

    def norm_over_y():
        line = row2[...]
        for d, copy in enumerate(n_wait["y"], 1):
            copy.wait_recv()
            line = jnp.maximum(line, row_y[d])
        norm[z] = line
        n_wait["z"] = [
            remote(norm.at[z], norm.at[z], norm_send.at[3], norm_sem.at[7 + d], z_at[d]) for d in range(1, Z)
        ]
        for copy in n_wait["z"]:
            copy.start()

    aside = {12: norm_over_x, 36: norm_over_core, 64: norm_over_y}
    seen = {}
    for k, (piece, dz, dy) in enumerate(arrivals()):
        if k in aside:
            aside[k]()
        base = block_at(dz, dy)
        ref = part(piece, base)
        remote(ref, ref, send_sem.at[0], flag(piece, dz, dy), sibling).wait_recv()
        send_on(piece, dz, dy, base)
        seen[dz % Z, dy % Y] = seen.get((dz % Z, dy % Y), 0) + 1
        if seen[dz % Z, dy % Y] == len(PIECES):
            send_aside(base)

    for copy in n_wait["z"]:
        copy.wait_recv()
    col_copy.wait()
    to_sibling.wait_send()
    for copy in norm_x + [n_wait["c"]] + n_wait["y"] + n_wait["z"] + over_y + over_z:
        copy.wait_send()
    others = out.at[0, pl.ds(0, ROWS - CHIP)]
    pltpu.make_async_copy(others, others, send_sem.at[0]).wait()
    whole = out.at[0]
    pltpu.make_async_copy(whole, whole, side_send.at[0]).wait()
    pltpu.make_async_copy(whole, whole, side_recv.at[0]).wait()


def write_kernel(tiles, cols, norm, gate, up, col_gate, col_up, gain, sem):
    parts = 4
    rows = ROWS // parts
    copies = []
    for i, ref in enumerate((gate, up)):
        for k in range(parts):
            at = pl.ds(k * rows, rows)
            copies.append(pltpu.make_async_copy(tiles.at[i, at], ref.at[at], sem.at[i * parts + k]))
    for copy in copies:
        copy.start()
    col_gate[...] = cols[0]
    col_up[...] = cols[1]
    gain[...] = jnp.concatenate([norm[k] for k in range(Z)], axis=0).astype(jnp.bfloat16)
    for copy in copies:
        copy.wait()


def local(one_gate, other_gate, one_up, other_up, mix_share, norm_train, norm_step):
    f32, bf16 = jnp.float32, jnp.bfloat16
    hbm_spec = pl.BlockSpec(memory_space=pltpu.HBM)
    vmem_spec = pl.BlockSpec(memory_space=pltpu.VMEM)
    dma = pltpu.SemaphoreType.DMA
    tiles, cols, norm = pl.pallas_call(
        gather_kernel,
        out_shape=(
            pltpu.VMEM((2, ROWS, COLS), bf16),
            pltpu.VMEM((2, TILES, 128), f32),
            pltpu.VMEM((Z, 2, 128), f32),
        ),
        in_specs=[hbm_spec] * 7,
        out_specs=(vmem_spec,) * 3,
        scratch_shapes=[
            pltpu.SMEM((OWN,), f32), pltpu.SMEM((8,), f32), pltpu.SMEM((8,), f32),
            pltpu.VMEM((4, OWN, COLS), f32),
            pltpu.VMEM((OWN, COLS), f32),
            pltpu.VMEM((CHIP, COLS), f32),
            pltpu.VMEM((TILES, 128), f32),
            pltpu.VMEM((Y, TILES, 128), f32),
            pltpu.VMEM((TILES, 128), f32),
            pltpu.VMEM((Z, TILES, 128), f32),
            pltpu.VMEM((TILES, 128), f32),
            pltpu.VMEM((2, 128), f32),
            pltpu.VMEM((X, 2, 128), f32),
            pltpu.VMEM((2, 128), f32),
            pltpu.VMEM((2, 128), f32),
            pltpu.VMEM((2, 128), f32),
            pltpu.VMEM((Y, 2, 128), f32),
            dma((7,)), dma((2,)), dma((2,)), dma((Y,)), dma((Z,)), dma((2,)), dma((4,)), dma((7 + Z,)),
            dma((1,)), dma((len(PIECES), Z * Y)), dma((1,)), dma((1,)),
        ],
        compiler_params=pltpu.CompilerParams(
            collective_id=0, has_side_effects=True, vmem_limit_bytes=24 * 2**20
        ),
        name="gather",
    )(
        *(
            pltpu.with_memory_space_constraint(a, pltpu.HBM)
            for a in (mix_share, one_gate, other_gate, one_up, other_up, norm_train, norm_step)
        )
    )
    tiles, cols, norm = (pltpu.with_memory_space_constraint(a, pltpu.VMEM) for a in (tiles, cols, norm))
    gate, up, col_gate, col_up, gain = pl.pallas_call(
        write_kernel,
        out_shape=(
            jax.ShapeDtypeStruct((ROWS, COLS), bf16),
            jax.ShapeDtypeStruct((ROWS, COLS), bf16),
            jax.ShapeDtypeStruct((TILES, 128), f32),
            jax.ShapeDtypeStruct((TILES, 128), f32),
            jax.ShapeDtypeStruct((2 * Z, 128), bf16),
        ),
        in_specs=[vmem_spec] * 3,
        out_specs=(hbm_spec, hbm_spec, vmem_spec, vmem_spec, vmem_spec),
        scratch_shapes=[dma((8,))],
        compiler_params=pltpu.CompilerParams(vmem_limit_bytes=8 * 2**20),
        name="write",
    )(tiles, cols, norm)
    return gate, up, col_gate.reshape(COLS), col_up.reshape(COLS), gain.reshape(ROWS)


def solution(mesh):
    torus = Mesh(mesh.devices.reshape(Z, Y, C, X), SHARD_MODEL)
    return jax.shard_map(
        local,
        mesh=torus,
        in_specs=(
            P(SHARD, "model"), P(SHARD, "model"), P(SHARD, "model"), P(SHARD, "model"),
            P(SHARD), P(SHARD_MODEL), P(SHARD_MODEL),
        ),
        out_specs=(P(None, "model"), P(None, "model"), P("model"), P("model"), P()),
        check_vma=False,
    )
```

```python
import heapq

import jax
import jax.numpy as jnp
from jax import lax
from jax.experimental import pallas as pl
from jax.experimental.pallas import tpu as pltpu
from jax.sharding import Mesh
from jax.sharding import PartitionSpec as P

SHARD = ("shard_0", "shard_1", "shard_2")
SHARD_MODEL = ("shard_0", "shard_1", "shard_2", "model")

Z, Y, C, X = 8, 4, 2, 4
ROWS, COLS, OWN = 2048, 2048, 32
CHIP = C * OWN
TILES = COLS // 128
LOW = -3.0e38

PIECES = (("A", 0, "own", 0, 7), ("B", 0, "own", 7, 16), ("A", 1, "other", 0, 6), ("B", 1, "other", 6, 16))
EARLY = (0, 1, 2)
LINKS = ("y+", "y-", "z+", "z-")
STEP = {"y+": (0, 1), "y-": (0, -1), "z+": (1, 0), "z-": (-1, 0)}


def reach(half, n):
    return (n // 2, n // 2 - 1) if half == 0 else (n // 2 - 1, n // 2)


def forwards(piece, dz, dy):
    kind, half = PIECES[piece][:2]
    zp, zm = reach(half, Z)
    yp, ym = reach(half, Y)
    along_z, along_y = [], []
    if 0 <= dz < zp:
        along_z.append(("z+", dz + 1, dy))
    if -zm < dz <= 0:
        along_z.append(("z-", dz - 1, dy))
    if 0 <= dy < yp:
        along_y.append(("y+", dz, dy + 1))
    if -ym < dy <= 0:
        along_y.append(("y-", dz, dy - 1))
    if kind == "A":
        return along_z + (along_y if dz == 0 else [])
    return (along_z if dy == 0 else []) + along_y


def plan(hop=2.0, turn=0.05, block=5.6):
    free = dict.fromkeys(LINKS, 0.0)
    queue, count, clock = [], 0, 0.0
    first = [(p, 0, 0) for p in range(len(PIECES)) if p not in EARLY]
    first += [(p, *STEP[link]) for p in EARLY for link in LINKS]
    order = []

    def issue(piece, dz, dy, at):
        nonlocal count
        for link, z, y in forwards(piece, dz, dy):
            width = (PIECES[piece][4] - PIECES[piece][3]) / TILES / C
            free[link] = max(at, free[link]) + width * block
            count += 1
            heapq.heappush(queue, (free[link] + hop, count, piece, z, y))

    for piece, dz, dy in first:
        order.append((piece, dz, dy))
        issue(piece, dz, dy, clock)
        clock += 2 * turn
    while queue:
        at, _, piece, dz, dy = heapq.heappop(queue)
        clock = max(clock, at) + turn
        order.append((piece, dz, dy))
        issue(piece, dz, dy, clock)
        clock += turn
    return order, clock


def gather_kernel(
    mix_h, one_g, other_g, one_u, other_u, train_h, step_h,
    out, cols, norm,
    mix, train, step, ins, theirs, x, raw, peak, peak_yc, peak1, peak_z, peak2,
    row0, row_x, row1, row_c, row2, row_y,
    in_sem, x_sem, peak_send, yc_sem, z_sem, col_sem, norm_send, norm_sem,
    raw_send, send_sem, recv_sem, side_send, side_recv,
):
    z, y, c, m = (lax.axis_index(a) for a in SHARD_MODEL)
    mesh_id = pl.DeviceIdType.MESH
    z_at = [(lax.rem(z + d, Z), y, c, m) for d in range(Z)]
    y_at = [(z, lax.rem(y + d, Y), c, m) for d in range(Y)]
    yo_at = [(z, lax.rem(y + d, Y), 1 - c, m) for d in range(Y)]
    m_at = [(z, y, c, lax.rem(m + d, X)) for d in range(X)]
    sibling = yo_at[0]
    link_to = {"z+": z_at[1], "z-": z_at[Z - 1], "y+": y_at[1], "y-": y_at[Y - 1]}

    def remote(src, dst, send, recv, to):
        return pltpu.make_async_remote_copy(
            src_ref=src, dst_ref=dst, send_sem=send, recv_sem=recv, device_id=to, device_id_type=mesh_id
        )

    partners = [*yo_at, *y_at[1:], *z_at[1:], *m_at[1:]]
    barrier = pltpu.get_barrier_semaphore()
    for to in partners:
        pl.semaphore_signal(barrier, inc=1, device_id=to, device_id_type=mesh_id)

    gate, up = 2 * (1 - c), 2 * c
    small = [
        pltpu.make_async_copy(mix_h, mix, in_sem.at[4]),
        pltpu.make_async_copy(train_h, train, in_sem.at[5]),
        pltpu.make_async_copy(step_h, step, in_sem.at[6]),
    ]
    large = [
        pltpu.make_async_copy(one_g, ins.at[gate], in_sem.at[gate]),
        pltpu.make_async_copy(other_g, ins.at[gate + 1], in_sem.at[gate + 1]),
        pltpu.make_async_copy(one_u, ins.at[up], in_sem.at[up]),
        pltpu.make_async_copy(other_u, ins.at[up + 1], in_sem.at[up + 1]),
    ]
    for copy in small + large:
        copy.start()
    for copy in small:
        copy.wait()

    sub = lax.broadcasted_iota(jnp.int32, (8, 128), 0)
    shares = []
    for r in range(OWN // 8):
        share = jnp.full((8, 128), mix[8 * r], jnp.float32)
        for i in range(1, 8):
            share = jnp.where(sub == i, mix[8 * r + i], share)
        shares.append((share, 1.0 - share))

    def blend(slot, to_peak, store):
        for k in (slot, slot + 1):
            pltpu.make_async_copy(one_g, ins.at[k], in_sem.at[k]).wait()
        for t in range(TILES):
            lanes = slice(128 * t, 128 * t + 128)
            best = None
            for r, (share, rest) in enumerate(shares):
                rows = slice(8 * r, 8 * r + 8)
                value = share * ins[slot, rows, lanes] + rest * ins[slot + 1, rows, lanes]
                store(r, lanes, value)
                best = jnp.abs(value) if best is None else jnp.maximum(best, jnp.abs(value))
            peak[to_peak, t : t + 1, :] = jnp.max(best, axis=0, keepdims=True)

    own_row, other_row = pl.multiple_of(OWN * c, OWN), pl.multiple_of(OWN * (1 - c), OWN)

    def store_theirs(r, lanes, value):
        theirs[8 * r : 8 * r + 8, lanes] = value

    def store_own(r, lanes, value):
        x[pl.ds(pl.multiple_of(own_row + 8 * r, 8), 8), lanes] = value

    blend(0, 1, store_theirs)
    blend(2, 0, store_own)

    lane2 = lax.broadcasted_iota(jnp.int32, (2, 128), 1)
    sub2 = lax.broadcasted_iota(jnp.int32, (2, 128), 0)
    start = (lax.rem(y, 2) * C + c) * OWN + m * 8
    line = jnp.full((2, 128), LOW, jnp.float32)
    for i in range(8):
        line = jnp.where((lane2 == start + i) & (sub2 == y // 2), train[i] + step[i], line)
    row0[...] = line

    pl.semaphore_wait(barrier, len(partners))

    over_yc = [remote(peak.at[1], peak_yc.at[0], peak_send.at[0], yc_sem.at[0], sibling)]
    for d in range(1, Y):
        over_yc.append(remote(peak.at[0], peak_yc.at[2 * d - 1], peak_send.at[0], yc_sem.at[2 * d - 1], y_at[d]))
        over_yc.append(remote(peak.at[1], peak_yc.at[2 * d], peak_send.at[0], yc_sem.at[2 * d], yo_at[d]))
    for copy in over_yc:
        copy.start()
    to_sibling = remote(theirs, x.at[pl.ds(own_row, OWN)], x_sem.at[0], x_sem.at[1], sibling)
    to_sibling.start()

    def flag(piece, dz, dy):
        return recv_sem.at[piece, (dz % Z) * Y + dy % Y]

    def rows_of(piece):
        return own_row if PIECES[piece][2] == "own" else other_row

    def lanes_of(piece):
        first, last = PIECES[piece][3:]
        return pl.ds(128 * first, 128 * (last - first))

    def early(piece, link):
        at = (pl.ds(rows_of(piece), OWN), lanes_of(piece))
        return remote(
            x.at[at], raw.at[(LINKS.index(link), *at)], raw_send.at[piece], flag(piece, *STEP[link]), link_to[link]
        )

    for link in LINKS:
        early(0, link).start()
    for link in ("y+", "y-"):
        early(1, link).start()
    norm_x = [remote(row0, row_x.at[d], norm_send.at[0], norm_sem.at[d], m_at[d]) for d in range(1, X)]
    for copy in norm_x:
        copy.start()

    best = peak[0]
    for d, copy in enumerate(over_yc):
        copy.wait_recv()
        best = jnp.maximum(best, peak_yc[d])
    peak1[...] = best

    over_z = [remote(peak1, peak_z.at[d], peak_send.at[1], z_sem.at[d], z_at[d]) for d in range(1, Z)]
    for d in sorted(range(1, Z), key=lambda d: -min(d, Z - d)):
        over_z[d - 1].start()
    for link in ("z+", "z-"):
        early(1, link).start()
    to_sibling.wait_recv()
    for link in LINKS:
        early(2, link).start()
    for d, copy in enumerate(over_z, 1):
        copy.wait_recv()
        best = jnp.maximum(best, peak_z[d])
    peak2[...] = best
    cols[c] = best

    def block_at(dz, dy):
        chip = lax.rem(z - dz + Z, Z) * Y + lax.rem(y - dy + Y, Y)
        return pl.multiple_of(chip * CHIP, CHIP)

    def scale(piece, source, base):
        for t in range(*PIECES[piece][3:]):
            lanes = slice(128 * t, 128 * t + 128)
            by = jnp.broadcast_to(peak2[t : t + 1, :], (16, 128))
            for r in range(OWN // 16):
                at = pl.multiple_of(rows_of(piece) + 16 * r, 16)
                value = source[pl.ds(at, 16), lanes] / by
                out[c, pl.ds(pl.multiple_of(base + at, 16), 16), lanes] = value.astype(jnp.bfloat16)

    def send_on(piece, dz, dy, base):
        ref = out.at[c, pl.ds(pl.multiple_of(base + rows_of(piece), OWN), OWN), lanes_of(piece)]
        for link, to_z, to_y in forwards(piece, dz, dy):
            remote(ref, ref, send_sem.at[piece], flag(piece, to_z, to_y), link_to[link]).start()

    def send_aside(base):
        ref = out.at[c, pl.ds(base, CHIP)]
        remote(ref, ref, side_send.at[0], side_recv.at[0], sibling).start()

    home = block_at(0, 0)
    n_wait = {}

    def norm_over_x():
        line = row0[...]
        for d, copy in enumerate(norm_x, 1):
            copy.wait_recv()
            line = jnp.maximum(line, row_x[d])
        row1[...] = line
        n_wait["c"] = remote(row1, row_c, norm_send.at[1], norm_sem.at[4], sibling)
        n_wait["c"].start()

    def norm_over_core():
        n_wait["c"].wait_recv()
        row2[...] = jnp.maximum(row1[...], row_c[...])
        n_wait["y"] = [
            remote(row2, row_y.at[d], norm_send.at[2], norm_sem.at[4 + d], y_at[d]) for d in range(1, Y)
        ]
        for copy in n_wait["y"]:
            copy.start()

    def norm_over_y():
        line = row2[...]
        for d, copy in enumerate(n_wait["y"], 1):
            copy.wait_recv()
            line = jnp.maximum(line, row_y[d])
        norm[z] = line
        n_wait["z"] = [
            remote(norm.at[z], norm.at[z], norm_send.at[3], norm_sem.at[7 + d], z_at[d]) for d in range(1, Z)
        ]
        for copy in n_wait["z"]:
            copy.start()

    def own_rest():
        for piece in EARLY:
            scale(piece, x, home)
        send_aside(home)
        n_wait["col"] = remote(cols.at[c], cols.at[c], col_sem.at[0], col_sem.at[1], sibling)
        n_wait["col"].start()

    order, _ = plan()
    n = len(order)
    aside = {n // 8: own_rest, n // 6: norm_over_x, n // 3: norm_over_core, n // 2: norm_over_y}
    seen = {}
    pending = None
    for k, (piece, dz, dy) in enumerate(order):
        if k in aside:
            aside[k]()
        base = block_at(dz, dy)
        computed = (dz, dy) == (0, 0) or (piece in EARLY and abs(dz) + abs(dy) == 1)
        if (dz, dy) == (0, 0):
            scale(piece, x, base)
        elif computed:
            link = LINKS[[STEP[l] for l in LINKS].index((dz, dy))]
            early(piece, link).wait_recv()
            scale(piece, raw.at[LINKS.index(link)], base)
        else:
            ref = out.at[c, pl.ds(pl.multiple_of(base + rows_of(piece), OWN), OWN), lanes_of(piece)]
            remote(ref, ref, send_sem.at[piece], flag(piece, dz, dy), sibling).wait_recv()
        if pending:
            send_on(*pending)
        pending = (piece, dz, dy, base)
        if not computed:
            send_on(*pending)
            pending = None
        if (dz, dy) != (0, 0):
            seen[dz % Z, dy % Y] = seen.get((dz % Z, dy % Y), 0) + 1
            if seen[dz % Z, dy % Y] == len(PIECES):
                send_aside(base)

    for copy in n_wait["z"]:
        copy.wait_recv()
    n_wait["col"].wait()
    to_sibling.wait_send()
    for copy in norm_x + [n_wait["c"]] + n_wait["y"] + n_wait["z"] + over_yc + over_z:
        copy.wait_send()
    for piece in range(len(PIECES)):
        sends = Z * Y - 1
        if piece in EARLY:
            sends -= len(LINKS)
            ref = ins.at[:, :, lanes_of(piece)]
            pltpu.make_async_copy(ref, ref, raw_send.at[piece]).wait()
        ref = out.at[0, pl.ds(0, sends * OWN), lanes_of(piece)]
        pltpu.make_async_copy(ref, ref, send_sem.at[piece]).wait()
    whole = out.at[0]
    pltpu.make_async_copy(whole, whole, side_send.at[0]).wait()
    pltpu.make_async_copy(whole, whole, side_recv.at[0]).wait()


def write_kernel(tiles, cols, norm, gate, up, col_gate, col_up, gain, sem):
    parts = 4
    rows = ROWS // parts
    copies = []
    for i, ref in enumerate((gate, up)):
        for k in range(parts):
            at = pl.ds(k * rows, rows)
            copies.append(pltpu.make_async_copy(tiles.at[i, at], ref.at[at], sem.at[i * parts + k]))
    for copy in copies:
        copy.start()
    col_gate[...] = cols[0]
    col_up[...] = cols[1]
    gain[...] = jnp.concatenate([norm[k] for k in range(Z)], axis=0).astype(jnp.bfloat16)
    for copy in copies:
        copy.wait()


def local(one_gate, other_gate, one_up, other_up, mix_share, norm_train, norm_step):
    f32, bf16 = jnp.float32, jnp.bfloat16
    hbm_spec = pl.BlockSpec(memory_space=pltpu.HBM)
    vmem_spec = pl.BlockSpec(memory_space=pltpu.VMEM)
    dma = pltpu.SemaphoreType.DMA
    tiles, cols, norm = pl.pallas_call(
        gather_kernel,
        out_shape=(
            pltpu.VMEM((2, ROWS, COLS), bf16),
            pltpu.VMEM((2, TILES, 128), f32),
            pltpu.VMEM((Z, 2, 128), f32),
        ),
        in_specs=[hbm_spec] * 7,
        out_specs=(vmem_spec,) * 3,
        scratch_shapes=[
            pltpu.SMEM((OWN,), f32), pltpu.SMEM((8,), f32), pltpu.SMEM((8,), f32),
            pltpu.VMEM((4, OWN, COLS), f32),
            pltpu.VMEM((OWN, COLS), f32),
            pltpu.VMEM((CHIP, COLS), f32),
            pltpu.VMEM((len(LINKS), CHIP, COLS), f32),
            pltpu.VMEM((C, TILES, 128), f32),
            pltpu.VMEM((C * Y - 1, TILES, 128), f32),
            pltpu.VMEM((TILES, 128), f32),
            pltpu.VMEM((Z, TILES, 128), f32),
            pltpu.VMEM((TILES, 128), f32),
            pltpu.VMEM((2, 128), f32),
            pltpu.VMEM((X, 2, 128), f32),
            pltpu.VMEM((2, 128), f32),
            pltpu.VMEM((2, 128), f32),
            pltpu.VMEM((2, 128), f32),
            pltpu.VMEM((Y, 2, 128), f32),
            dma((7,)), dma((2,)), dma((2,)), dma((C * Y - 1,)), dma((Z,)), dma((2,)), dma((4,)), dma((7 + Z,)),
            dma((len(PIECES),)), dma((len(PIECES),)), dma((len(PIECES), Z * Y)), dma((1,)), dma((1,)),
        ],
        compiler_params=pltpu.CompilerParams(
            collective_id=0, has_side_effects=True, vmem_limit_bytes=24 * 2**20
        ),
        name="gather",
    )(
        *(
            pltpu.with_memory_space_constraint(a, pltpu.HBM)
            for a in (mix_share, one_gate, other_gate, one_up, other_up, norm_train, norm_step)
        )
    )
    tiles, cols, norm = (pltpu.with_memory_space_constraint(a, pltpu.VMEM) for a in (tiles, cols, norm))
    gate, up, col_gate, col_up, gain = pl.pallas_call(
        write_kernel,
        out_shape=(
            jax.ShapeDtypeStruct((ROWS, COLS), bf16),
            jax.ShapeDtypeStruct((ROWS, COLS), bf16),
            jax.ShapeDtypeStruct((TILES, 128), f32),
            jax.ShapeDtypeStruct((TILES, 128), f32),
            jax.ShapeDtypeStruct((2 * Z, 128), bf16),
        ),
        in_specs=[vmem_spec] * 3,
        out_specs=(hbm_spec, hbm_spec, vmem_spec, vmem_spec, vmem_spec),
        scratch_shapes=[dma((8,))],
        compiler_params=pltpu.CompilerParams(vmem_limit_bytes=8 * 2**20),
        name="write",
    )(tiles, cols, norm)
    return gate, up, col_gate.reshape(COLS), col_up.reshape(COLS), gain.reshape(ROWS)


def solution(mesh):
    torus = Mesh(mesh.devices.reshape(Z, Y, C, X), SHARD_MODEL)
    return jax.shard_map(
        local,
        mesh=torus,
        in_specs=(
            P(SHARD, "model"), P(SHARD, "model"), P(SHARD, "model"), P(SHARD, "model"),
            P(SHARD), P(SHARD_MODEL), P(SHARD_MODEL),
        ),
        out_specs=(P(None, "model"), P(None, "model"), P("model"), P("model"), P()),
        check_vma=False,
    )
```

```python
import heapq

import jax
import jax.numpy as jnp
from jax import lax
from jax.experimental import pallas as pl
from jax.experimental.pallas import tpu as pltpu
from jax.sharding import Mesh
from jax.sharding import PartitionSpec as P

SHARD = ("shard_0", "shard_1", "shard_2")
SHARD_MODEL = ("shard_0", "shard_1", "shard_2", "model")

Z, Y, C, X = 8, 4, 2, 4
ROWS, COLS, OWN = 2048, 2048, 32
CHIP = C * OWN
TILES = COLS // 128
LOW = -3.0e38
LATE = 24

PIECES = (("A", 0, "own", 0, 6), ("B", 0, "own", 6, 16), ("A", 1, "other", 0, 7), ("B", 1, "other", 7, 16))
FIRST = (3, 1, 0, 2)
EARLY = {"y": ((0, 2, 1), ()), "z": ((1,), (3,))}
LINKS = ("y+", "y-", "z+", "z-")
STEP = {"y+": (0, 1), "y-": (0, -1), "z+": (1, 0), "z-": (-1, 0)}


def is_early(piece, link):
    return any(piece in some for some in EARLY[link[0]])


def reach(half, n):
    return (n // 2, n // 2 - 1) if half == 0 else (n // 2 - 1, n // 2)


def forwards(piece, dz, dy):
    kind, half = PIECES[piece][:2]
    zp, zm = reach(half, Z)
    yp, ym = reach(half, Y)
    along_z, along_y = [], []
    if 0 <= dz < zp:
        along_z.append(("z+", dz + 1, dy))
    if -zm < dz <= 0:
        along_z.append(("z-", dz - 1, dy))
    if 0 <= dy < yp:
        along_y.append(("y+", dz, dy + 1))
    if -ym < dy <= 0:
        along_y.append(("y-", dz, dy - 1))
    if kind == "A":
        return along_z + (along_y if dz == 0 else [])
    return (along_z if dy == 0 else []) + along_y


def plan(hop=2.0, turn=0.04, block=5.6, swap=1.6, over_y=4.0, letters=0.9, over_z=8.5, work=0.08):
    free = dict.fromkeys(LINKS, 0.0)
    queue, order, count = [], [], 0

    def put(piece, link, z, y, at, early=False):
        nonlocal count
        width = (PIECES[piece][4] - PIECES[piece][3]) / TILES / C
        free[link] = max(at, free[link]) + width * block * (2 if early else 1)
        count += 1
        rank = FIRST.index(piece) if early else len(PIECES)
        heapq.heappush(queue, (max(free[link] + hop, over_z), rank, count, piece, z, y))

    for k, begin in enumerate((0.0, over_y)):
        for link in LINKS:
            for piece in EARLY[link[0]][k]:
                put(piece, link, *STEP[link], max(begin, swap if PIECES[piece][2] == "other" else 0.0), True)
        if k == 0:
            for link in ("z+", "z-"):
                free[link] = max(free[link], over_y) + letters
    clock = over_z
    for piece in range(len(PIECES)):
        if not all(is_early(piece, link) for link in LINKS):
            heapq.heappush(queue, (over_z, FIRST.index(piece) - 100, 0, piece, 0, 0))
    while queue:
        at, _, _, piece, dz, dy = heapq.heappop(queue)
        clock = max(clock, at) + turn
        order.append((piece, dz, dy))
        links = [l for l in LINKS if STEP[l] == (dz, dy)]
        if (dz, dy) == (0, 0) or links and is_early(piece, links[0]):
            clock += work
        for link, to_z, to_y in forwards(piece, dz, dy):
            if (dz, dy) != (0, 0) or not is_early(piece, link):
                put(piece, link, to_z, to_y, clock)
        clock += turn
    return order, clock


def came_by(piece, dz, dy):
    along_z = dz != 0 and (PIECES[piece][0] == "A" or dy == 0)
    link = ("z" if along_z else "y") + ("+" if (dz if along_z else dy) > 0 else "-")
    return link, (piece, dz - STEP[link][0], dy - STEP[link][1])


def share_flags(order):
    at = {event: k for k, event in enumerate(order)}
    known = {link: [-1] * len(order) for link in LINKS}
    for k, event in enumerate(order):
        for link in LINKS:
            known[link][k] = known[link][k - 1] if k else -1
        if event[1:] != (0, 0):
            link, before = came_by(*event)
            if before[1:] != (0, 0) or not is_early(event[0], link):
                back = link[0] + ("-" if link[1] == "+" else "+")
                known[back][k] = max(known[back][k], at[before])
    flags, last = {}, []
    for k, event in enumerate(order):
        if event[1:] == (0, 0):
            continue
        link, before = came_by(*event)
        early = before[1:] == (0, 0) and is_early(event[0], link)
        free = [] if early else [i for i, used in enumerate(last) if used <= known[link][at[before]]]
        if free:
            i = min(free, key=lambda i: last[i])
            last[i] = k
        else:
            i = len(last)
            last.append(k)
        flags[event] = i
    return flags, len(last)


def gather_kernel(
    mix_h, one_g, other_g, one_u, other_u, train_h, step_h,
    out, cols, norm,
    mix, train, step, ins, theirs, x, raw, peak, peak_yc, peak1, peak_z, peak2,
    row0, row_x, row1, row2, row_y,
    in_sem, x_sem, peak_send, yc_sem, z_sem, norm_send, norm_sem,
    raw_send, send_sem, recv_sem, side_send, side_recv,
):
    order, _ = plan()
    flags, _ = share_flags(order)
    z, y, c, m = (lax.axis_index(a) for a in SHARD_MODEL)
    mesh_id = pl.DeviceIdType.MESH
    z_at = [(lax.rem(z + d, Z), y, c, m) for d in range(Z)]
    y_at = [(z, lax.rem(y + d, Y), c, m) for d in range(Y)]
    yo_at = [(z, lax.rem(y + d, Y), 1 - c, m) for d in range(Y)]
    m_at = [(z, y, c, lax.rem(m + d, X)) for d in range(X)]
    sibling = yo_at[0]
    link_to = {"z+": z_at[1], "z-": z_at[Z - 1], "y+": y_at[1], "y-": y_at[Y - 1]}

    def remote(src, dst, send, recv, to):
        return pltpu.make_async_remote_copy(
            src_ref=src, dst_ref=dst, send_sem=send, recv_sem=recv, device_id=to, device_id_type=mesh_id
        )

    partners = [*yo_at, *y_at[1:], *z_at[1:], *m_at[1:]]
    barrier = pltpu.get_barrier_semaphore()
    for to in partners:
        pl.semaphore_signal(barrier, inc=1, device_id=to, device_id_type=mesh_id)

    small = [
        pltpu.make_async_copy(ref, to, in_sem.at[2 + i])
        for i, (ref, to) in enumerate(((mix_h, mix), (train_h, train), (step_h, step)))
    ]
    for copy in small:
        copy.start()
    for ours, pair in ((1 - c, (one_g, other_g)), (c, (one_u, other_u))):
        for k, ref in enumerate(pair):
            pltpu.make_async_copy(ref, ins.at[2 * ours + k], in_sem.at[ours]).start()
    for copy in small:
        copy.wait()

    sub = lax.broadcasted_iota(jnp.int32, (8, 128), 0)
    shares = []
    for r in range(OWN // 8):
        share = jnp.full((8, 128), mix[8 * r], jnp.float32)
        for i in range(1, 8):
            share = jnp.where(sub == i, mix[8 * r + i], share)
        shares.append((share, 1.0 - share))

    def blend(slot, to_peak, store):
        both = ins.at[pl.ds(slot, 2)]
        pltpu.make_async_copy(both, both, in_sem.at[slot // 2]).wait()
        for t in range(TILES):
            lanes = slice(128 * t, 128 * t + 128)
            best = None
            for r, (share, rest) in enumerate(shares):
                rows = slice(8 * r, 8 * r + 8)
                value = share * ins[slot, rows, lanes] + rest * ins[slot + 1, rows, lanes]
                store(r, lanes, value)
                best = jnp.abs(value) if best is None else jnp.maximum(best, jnp.abs(value))
            peak[to_peak, t : t + 1, :] = jnp.max(best, axis=0, keepdims=True)

    own_row, other_row = pl.multiple_of(OWN * c, OWN), pl.multiple_of(OWN * (1 - c), OWN)

    def store_theirs(r, lanes, value):
        theirs[8 * r : 8 * r + 8, lanes] = value

    def store_own(r, lanes, value):
        x[pl.ds(pl.multiple_of(own_row + 8 * r, 8), 8), lanes] = value

    blend(0, 1, store_theirs)
    blend(2, 0, store_own)

    lane2 = lax.broadcasted_iota(jnp.int32, (2, 128), 1)
    sub2 = lax.broadcasted_iota(jnp.int32, (2, 128), 0)
    start = (lax.rem(y, 2) * C + c) * OWN + m * 8
    line = jnp.full((2, 128), LOW, jnp.float32)
    for i in range(8):
        line = jnp.where((lane2 == start + i) & (sub2 == y // 2), train[i] + step[i], line)
    row0[...] = line

    pl.semaphore_wait(barrier, len(partners))

    over_yc = []
    for d in (2, 1, 3):
        over_yc.append(remote(peak.at[1], peak_yc.at[2 * d], peak_send.at[0], yc_sem.at[0], yo_at[d]))
        over_yc.append(remote(peak.at[0], peak_yc.at[2 * d - 1], peak_send.at[0], yc_sem.at[0], y_at[d]))
    over_yc.append(remote(peak.at[1], peak_yc.at[0], peak_send.at[0], yc_sem.at[0], sibling))
    for copy in over_yc:
        copy.start()
    to_sibling = remote(theirs, x.at[pl.ds(own_row, OWN)], x_sem.at[0], x_sem.at[1], sibling)
    to_sibling.start()
    norm_x = [remote(row0, row_x.at[d], norm_send.at[0], norm_sem.at[0], m_at[d]) for d in range(1, X)]
    for copy in norm_x:
        copy.start()

    def arrived(ref, sem):
        pltpu.make_async_copy(ref, ref, sem).wait()

    def flag(*event):
        return recv_sem.at[flags[event]]

    def rows_of(piece):
        return own_row if PIECES[piece][2] == "own" else other_row

    def lanes_of(piece):
        first, last = PIECES[piece][3:]
        return pl.ds(128 * first, 128 * (last - first))

    def early(piece, link):
        at = (pl.ds(rows_of(piece), OWN), lanes_of(piece))
        return remote(
            x.at[at], raw.at[(LINKS.index(link), *at)], raw_send.at[0], flag(piece, *STEP[link]), link_to[link]
        )

    own_first = {}
    for link in LINKS:
        some = [PIECES[piece][2] for piece in EARLY[link[0]][0]] + ["other"]
        own_first[link] = some.index("other")
        for piece in EARLY[link[0]][0][: own_first[link]]:
            early(piece, link).start()
    to_sibling.wait_recv()
    for link in LINKS:
        for piece in EARLY[link[0]][0][own_first[link] :]:
            early(piece, link).start()

    arrived(peak_yc, yc_sem.at[0])
    best = peak[0]
    for d in range(C * Y - 1):
        best = jnp.maximum(best, peak_yc[d])
    peak1[...] = best

    over_z = [remote(peak1, peak_z.at[d], peak_send.at[0], z_sem.at[0], z_at[d]) for d in range(1, Z)]
    for d in sorted(range(1, Z), key=lambda d: -min(d, Z - d)):
        over_z[d - 1].start()
    for link in LINKS:
        for piece in EARLY[link[0]][1]:
            early(piece, link).start()
    arrived(peak_z.at[pl.ds(1, Z - 1)], z_sem.at[0])
    for d in range(1, Z):
        best = jnp.maximum(best, peak_z[d])
    peak2[...] = best
    cols[c] = best

    def block_at(dz, dy):
        chip = lax.rem(z - dz + Z, Z) * Y + lax.rem(y - dy + Y, Y)
        return pl.multiple_of(chip * CHIP, CHIP)

    def scale(piece, source, base):
        for t in range(*PIECES[piece][3:]):
            lanes = slice(128 * t, 128 * t + 128)
            by = jnp.broadcast_to(peak2[t : t + 1, :], (16, 128))
            for r in range(OWN // 16):
                at = pl.multiple_of(rows_of(piece) + 16 * r, 16)
                value = source[pl.ds(at, 16), lanes] / by
                out[c, pl.ds(pl.multiple_of(base + at, 16), 16), lanes] = value.astype(jnp.bfloat16)

    def send_on(piece, dz, dy, base):
        ref = out.at[c, pl.ds(pl.multiple_of(base + rows_of(piece), OWN), OWN), lanes_of(piece)]
        for link, to_z, to_y in forwards(piece, dz, dy):
            if (dz, dy) == (0, 0) and is_early(piece, link):
                continue
            remote(ref, ref, send_sem.at[0], flag(piece, to_z, to_y), link_to[link]).start()

    def send_aside(base, rows=CHIP, lanes=pl.ds(0, COLS)):
        ref = out.at[c, pl.ds(base, rows), lanes]
        remote(ref, ref, side_send.at[0], side_recv.at[0], sibling).start()

    home = block_at(0, 0)

    def norm_over_x():
        line = row0[...]
        arrived(row_x.at[pl.ds(1, X - 1)], norm_sem.at[0])
        for d in range(1, X):
            line = jnp.maximum(line, row_x[d])
        row1[...] = line
        remote(row1, row_y.at[0], norm_send.at[1], norm_sem.at[1], sibling).start()

    def norm_over_core():
        arrived(row_y.at[0], norm_sem.at[1])
        row2[...] = jnp.maximum(row1[...], row_y[0])
        for d in range(1, Y):
            remote(row2, row_y.at[d], norm_send.at[1], norm_sem.at[2], y_at[d]).start()

    def norm_over_y():
        line = row2[...]
        arrived(row_y.at[pl.ds(1, Y - 1)], norm_sem.at[2])
        for d in range(1, Y):
            line = jnp.maximum(line, row_y[d])
        norm[z] = line
        for d in range(1, Z):
            remote(norm.at[z], norm.at[z], norm_send.at[2], norm_sem.at[3], z_at[d]).start()

    def own_rest():
        for piece in range(len(PIECES)):
            if (piece, 0, 0) not in order:
                scale(piece, x, home)
        send_aside(home)
        remote(cols.at[c], cols.at[c], side_send.at[1], side_recv.at[1], sibling).start()

    n = len(order)
    aside = {n // 8: own_rest, n // 6: norm_over_x, n // 3: norm_over_core, n // 2: norm_over_y}
    blocks = {}
    for k, (_, dz, dy) in enumerate(order):
        blocks.setdefault((dz % Z, dy % Y), []).append(k)
    blocks.pop((0, 0), None)
    pending = None
    for k, (piece, dz, dy) in enumerate(order):
        if k in aside:
            aside[k]()
        base = block_at(dz, dy)
        link = next((l for l in LINKS if STEP[l] == (dz, dy)), None)
        computed = (dz, dy) == (0, 0) or link is not None and is_early(piece, link)
        if (dz, dy) == (0, 0):
            scale(piece, x, base)
        elif computed:
            early(piece, link).wait_recv()
            scale(piece, raw.at[LINKS.index(link)], base)
        else:
            ref = out.at[c, pl.ds(pl.multiple_of(base + rows_of(piece), OWN), OWN), lanes_of(piece)]
            remote(ref, ref, send_sem.at[0], flag(piece, dz, dy), sibling).wait_recv()
        if pending:
            send_on(*pending)
        pending = (piece, dz, dy, base)
        if not computed:
            send_on(*pending)
            pending = None
        if (dz, dy) != (0, 0):
            last = blocks[dz % Z, dy % Y][-1]
            if last >= n - LATE:
                send_aside(pl.multiple_of(base + rows_of(piece), OWN), OWN, lanes_of(piece))
            elif last == k:
                send_aside(base)

    arrived(norm.at[pl.ds(0, Z - 1)], norm_sem.at[3])
    arrived(cols.at[0], side_send.at[1])
    arrived(cols.at[0], side_recv.at[1])
    to_sibling.wait_send()
    arrived(row_x.at[pl.ds(1, X - 1)], norm_send.at[0])
    arrived(row_y, norm_send.at[1])
    arrived(norm.at[pl.ds(0, Z - 1)], norm_send.at[2])
    arrived(theirs.at[:, pl.ds(0, 64 * (C * Y + Z - 2))], peak_send.at[0])
    wide = [last - first for _, _, _, first, last in PIECES]
    soon = [sum(is_early(piece, link) for link in LINKS) for piece in range(len(PIECES))]
    arrived(out.at[0, pl.ds(0, 16 * sum(a * b for a, b in zip(soon, wide))), pl.ds(0, 512)], raw_send.at[0])
    arrived(out.at[0, pl.ds(0, 2 * sum((Z * Y - 1 - a) * b for a, b in zip(soon, wide)))], send_sem.at[0])
    whole = out.at[0]
    arrived(whole, side_send.at[0])
    arrived(whole, side_recv.at[0])


def write_kernel(tiles, cols, norm, gate, up, col_gate, col_up, gain, sem):
    parts = 4
    rows = ROWS // parts
    copies = []
    for i, ref in enumerate((gate, up)):
        for k in range(parts):
            at = pl.ds(k * rows, rows)
            copies.append(pltpu.make_async_copy(tiles.at[i, at], ref.at[at], sem.at[i * parts + k]))
    for copy in copies:
        copy.start()
    col_gate[...] = cols[0]
    col_up[...] = cols[1]
    gain[...] = jnp.concatenate([norm[k] for k in range(Z)], axis=0).astype(jnp.bfloat16)
    for copy in copies:
        copy.wait()


def local(one_gate, other_gate, one_up, other_up, mix_share, norm_train, norm_step):
    f32, bf16 = jnp.float32, jnp.bfloat16
    hbm_spec = pl.BlockSpec(memory_space=pltpu.HBM)
    vmem_spec = pl.BlockSpec(memory_space=pltpu.VMEM)
    dma = pltpu.SemaphoreType.DMA
    tiles, cols, norm = pl.pallas_call(
        gather_kernel,
        out_shape=(
            pltpu.VMEM((2, ROWS, COLS), bf16),
            pltpu.VMEM((2, TILES, 128), f32),
            pltpu.VMEM((Z, 2, 128), f32),
        ),
        in_specs=[hbm_spec] * 7,
        out_specs=(vmem_spec,) * 3,
        scratch_shapes=[
            pltpu.SMEM((OWN,), f32), pltpu.SMEM((8,), f32), pltpu.SMEM((8,), f32),
            pltpu.VMEM((4, OWN, COLS), f32),
            pltpu.VMEM((OWN, COLS), f32),
            pltpu.VMEM((CHIP, COLS), f32),
            pltpu.VMEM((len(LINKS), CHIP, COLS), f32),
            pltpu.VMEM((C, TILES, 128), f32),
            pltpu.VMEM((C * Y - 1, TILES, 128), f32),
            pltpu.VMEM((TILES, 128), f32),
            pltpu.VMEM((Z, TILES, 128), f32),
            pltpu.VMEM((TILES, 128), f32),
            pltpu.VMEM((2, 128), f32),
            pltpu.VMEM((X, 2, 128), f32),
            pltpu.VMEM((2, 128), f32),
            pltpu.VMEM((2, 128), f32),
            pltpu.VMEM((Y, 2, 128), f32),
            dma((5,)), dma((2,)), dma((1,)), dma((1,)), dma((1,)), dma((3,)), dma((4,)),
            dma((1,)), dma((1,)), dma((share_flags(plan()[0])[1],)), dma((2,)), dma((2,)),
        ],
        compiler_params=pltpu.CompilerParams(
            collective_id=0, has_side_effects=True, vmem_limit_bytes=24 * 2**20
        ),
        name="gather",
    )(
        *(
            pltpu.with_memory_space_constraint(a, pltpu.HBM)
            for a in (mix_share, one_gate, other_gate, one_up, other_up, norm_train, norm_step)
        )
    )
    tiles, cols, norm = (pltpu.with_memory_space_constraint(a, pltpu.VMEM) for a in (tiles, cols, norm))
    gate, up, col_gate, col_up, gain = pl.pallas_call(
        write_kernel,
        out_shape=(
            jax.ShapeDtypeStruct((ROWS, COLS), bf16),
            jax.ShapeDtypeStruct((ROWS, COLS), bf16),
            jax.ShapeDtypeStruct((TILES, 128), f32),
            jax.ShapeDtypeStruct((TILES, 128), f32),
            jax.ShapeDtypeStruct((2 * Z, 128), bf16),
        ),
        in_specs=[vmem_spec] * 3,
        out_specs=(hbm_spec, hbm_spec, vmem_spec, vmem_spec, vmem_spec),
        scratch_shapes=[dma((8,))],
        compiler_params=pltpu.CompilerParams(vmem_limit_bytes=8 * 2**20),
        name="write",
    )(tiles, cols, norm)
    return gate, up, col_gate.reshape(COLS), col_up.reshape(COLS), gain.reshape(ROWS)


def solution(mesh):
    torus = Mesh(mesh.devices.reshape(Z, Y, C, X), SHARD_MODEL)
    return jax.shard_map(
        local,
        mesh=torus,
        in_specs=(
            P(SHARD, "model"), P(SHARD, "model"), P(SHARD, "model"), P(SHARD, "model"),
            P(SHARD), P(SHARD_MODEL), P(SHARD_MODEL),
        ),
        out_specs=(P(None, "model"), P(None, "model"), P("model"), P("model"), P()),
        check_vma=False,
    )
```

```python
import heapq

import jax
import jax.numpy as jnp
from jax import lax
from jax.experimental import pallas as pl
from jax.experimental.pallas import tpu as pltpu
from jax.sharding import Mesh
from jax.sharding import PartitionSpec as P

SHARD = ("shard_0", "shard_1", "shard_2")
SHARD_MODEL = ("shard_0", "shard_1", "shard_2", "model")

Z, Y, C, X = 8, 4, 2, 4
ROWS, COLS, OWN = 2048, 2048, 32
CHIP = C * OWN
TILES = COLS // 128
LOW = -3.0e38
LATE = 24

PIECES = (("A", 0, "own", 0, 6), ("B", 0, "own", 6, 16), ("A", 1, "other", 0, 7), ("B", 1, "other", 7, 16))
FIRST = (3, 1, 0, 2)
EARLY = {"y": ((0, 2, 1), ()), "z": ((1,), (3,))}
LINKS = ("y+", "y-", "z+", "z-")
STEP = {"y+": (0, 1), "y-": (0, -1), "z+": (1, 0), "z-": (-1, 0)}


def is_early(piece, link):
    return any(piece in some for some in EARLY[link[0]])


def reach(half, n):
    return (n // 2, n // 2 - 1) if half == 0 else (n // 2 - 1, n // 2)


def forwards(piece, dz, dy):
    kind, half = PIECES[piece][:2]
    zp, zm = reach(half, Z)
    yp, ym = reach(half, Y)
    along_z, along_y = [], []
    if 0 <= dz < zp:
        along_z.append(("z+", dz + 1, dy))
    if -zm < dz <= 0:
        along_z.append(("z-", dz - 1, dy))
    if 0 <= dy < yp:
        along_y.append(("y+", dz, dy + 1))
    if -ym < dy <= 0:
        along_y.append(("y-", dz, dy - 1))
    if kind == "A":
        return along_z + (along_y if dz == 0 else [])
    return (along_z if dy == 0 else []) + along_y


def plan(hop=2.0, turn=0.04, block=5.6, swap=1.6, over_y=4.0, letters=0.9, over_z=8.5, work=0.08):
    free = dict.fromkeys(LINKS, 0.0)
    queue, order, count = [], [], 0

    def put(piece, link, z, y, at, early=False):
        nonlocal count
        width = (PIECES[piece][4] - PIECES[piece][3]) / TILES / C
        free[link] = max(at, free[link]) + width * block * (2 if early else 1)
        count += 1
        rank = FIRST.index(piece) if early else len(PIECES)
        heapq.heappush(queue, (max(free[link] + hop, over_z), rank, count, piece, z, y))

    for k, begin in enumerate((0.0, over_y)):
        for link in LINKS:
            for piece in EARLY[link[0]][k]:
                put(piece, link, *STEP[link], max(begin, swap if PIECES[piece][2] == "other" else 0.0), True)
        if k == 0:
            for link in ("z+", "z-"):
                free[link] = max(free[link], over_y) + letters
    clock = over_z
    for piece in range(len(PIECES)):
        if not all(is_early(piece, link) for link in LINKS):
            heapq.heappush(queue, (over_z, FIRST.index(piece) - 100, 0, piece, 0, 0))
    while queue:
        at, _, _, piece, dz, dy = heapq.heappop(queue)
        clock = max(clock, at) + turn
        order.append((piece, dz, dy))
        links = [l for l in LINKS if STEP[l] == (dz, dy)]
        if (dz, dy) == (0, 0) or links and is_early(piece, links[0]):
            clock += work
        for link, to_z, to_y in forwards(piece, dz, dy):
            if (dz, dy) != (0, 0) or not is_early(piece, link):
                put(piece, link, to_z, to_y, clock)
        clock += turn
    return order, clock


def came_by(piece, dz, dy):
    along_z = dz != 0 and (PIECES[piece][0] == "A" or dy == 0)
    link = ("z" if along_z else "y") + ("+" if (dz if along_z else dy) > 0 else "-")
    return link, (piece, dz - STEP[link][0], dy - STEP[link][1])


def share_flags(order):
    at = {event: k for k, event in enumerate(order)}
    known = {link: [-1] * len(order) for link in LINKS}
    for k, event in enumerate(order):
        for link in LINKS:
            known[link][k] = known[link][k - 1] if k else -1
        if event[1:] != (0, 0):
            link, before = came_by(*event)
            if before[1:] != (0, 0) or not is_early(event[0], link):
                back = link[0] + ("-" if link[1] == "+" else "+")
                known[back][k] = max(known[back][k], at[before])
    flags, last = {}, []
    for k, event in enumerate(order):
        if event[1:] == (0, 0):
            continue
        link, before = came_by(*event)
        early = before[1:] == (0, 0) and is_early(event[0], link)
        free = [] if early else [i for i, used in enumerate(last) if used <= known[link][at[before]]]
        if free:
            i = min(free, key=lambda i: last[i])
            last[i] = k
        else:
            i = len(last)
            last.append(k)
        flags[event] = i
    return flags, len(last)


def gather_kernel(
    mix_h, one_g, other_g, one_u, other_u, train_h, step_h,
    out, cols, norm,
    mix, train, step, ins, theirs, x, raw, peak, peak_yc, peak1, peak_z, peak2,
    row0, row_yc, rows_z, rows_x,
    in_sem, x_sem, peak_send, yc_sem, z_sem, norm_send, norm_sem,
    raw_send, send_sem, recv_sem, side_send, side_recv, known,
):
    order, _ = plan()
    flags, _ = share_flags(order)
    z, y, c, m = (lax.axis_index(a) for a in SHARD_MODEL)
    mesh_id = pl.DeviceIdType.MESH
    z_at = [(lax.rem(z + d, Z), y, c, m) for d in range(Z)]
    y_at = [(z, lax.rem(y + d, Y), c, m) for d in range(Y)]
    yo_at = [(z, lax.rem(y + d, Y), 1 - c, m) for d in range(Y)]
    m_at = [(z, y, c, lax.rem(m + d, X)) for d in range(X)]
    sibling = yo_at[0]
    link_to = {"z+": z_at[1], "z-": z_at[Z - 1], "y+": y_at[1], "y-": y_at[Y - 1]}

    def remote(src, dst, send, recv, to):
        return pltpu.make_async_remote_copy(
            src_ref=src, dst_ref=dst, send_sem=send, recv_sem=recv, device_id=to, device_id_type=mesh_id
        )

    partners = [*yo_at, *y_at[1:], z_at[1], z_at[Z - 1], *m_at[1:]]
    barrier = pltpu.get_barrier_semaphore()
    for to in partners:
        pl.semaphore_signal(barrier, inc=1, device_id=to, device_id_type=mesh_id)

    small = [
        pltpu.make_async_copy(ref, to, in_sem.at[2 + i])
        for i, (ref, to) in enumerate(((mix_h, mix), (train_h, train), (step_h, step)))
    ]
    for copy in small:
        copy.start()
    for ours, pair in ((1 - c, (one_g, other_g)), (c, (one_u, other_u))):
        for k, ref in enumerate(pair):
            pltpu.make_async_copy(ref, ins.at[2 * ours + k], in_sem.at[ours]).start()
    for copy in small:
        copy.wait()

    sub = lax.broadcasted_iota(jnp.int32, (8, 128), 0)
    shares = []
    for r in range(OWN // 8):
        share = jnp.full((8, 128), mix[8 * r], jnp.float32)
        for i in range(1, 8):
            share = jnp.where(sub == i, mix[8 * r + i], share)
        shares.append((share, 1.0 - share))

    def blend(slot, to_peak, store):
        both = ins.at[pl.ds(slot, 2)]
        pltpu.make_async_copy(both, both, in_sem.at[slot // 2]).wait()
        for t in range(TILES):
            lanes = slice(128 * t, 128 * t + 128)
            best = None
            for r, (share, rest) in enumerate(shares):
                rows = slice(8 * r, 8 * r + 8)
                value = share * ins[slot, rows, lanes] + rest * ins[slot + 1, rows, lanes]
                store(r, lanes, value)
                best = jnp.abs(value) if best is None else jnp.maximum(best, jnp.abs(value))
            peak[to_peak, t : t + 1, :] = jnp.max(best, axis=0, keepdims=True)

    own_row, other_row = pl.multiple_of(OWN * c, OWN), pl.multiple_of(OWN * (1 - c), OWN)

    def store_theirs(r, lanes, value):
        theirs[8 * r : 8 * r + 8, lanes] = value

    def store_own(r, lanes, value):
        x[pl.ds(pl.multiple_of(own_row + 8 * r, 8), 8), lanes] = value

    blend(0, 1, store_theirs)
    blend(2, 0, store_own)

    lane2 = lax.broadcasted_iota(jnp.int32, (2, 128), 1)
    sub2 = lax.broadcasted_iota(jnp.int32, (2, 128), 0)
    start = (lax.rem(y, 2) * C + c) * OWN + m * 8
    line = jnp.full((2, 128), LOW, jnp.float32)
    for i in range(8):
        line = jnp.where((lane2 == start + i) & (sub2 == y // 2), train[i] + step[i], line)
    row0[...] = line

    pl.semaphore_wait(barrier, len(partners))

    over_yc = []
    for d in (2, 1, 3):
        over_yc.append(remote(peak.at[1], peak_yc.at[2 * d], peak_send.at[0], yc_sem.at[0], yo_at[d]))
        over_yc.append(remote(peak.at[0], peak_yc.at[2 * d - 1], peak_send.at[0], yc_sem.at[0], y_at[d]))
    over_yc.append(remote(peak.at[1], peak_yc.at[0], peak_send.at[0], yc_sem.at[0], sibling))
    for copy in over_yc:
        copy.start()
    to_sibling = remote(theirs, x.at[pl.ds(own_row, OWN)], x_sem.at[0], x_sem.at[1], sibling)
    to_sibling.start()
    for d in (2, 1, 3):
        remote(row0, row_yc.at[2 * d], norm_send.at[0], norm_sem.at[0], yo_at[d]).start()
        remote(row0, row_yc.at[2 * d - 1], norm_send.at[0], norm_sem.at[0], y_at[d]).start()
    remote(row0, row_yc.at[0], norm_send.at[0], norm_sem.at[0], sibling).start()

    def tell_z():
        for way, to in enumerate((z_at[1], z_at[Z - 1])):
            pl.semaphore_signal(known.at[way], inc=1, device_id=to, device_id_type=mesh_id)

    def hear_z():
        for way in range(2):
            pl.semaphore_wait(known.at[way], 1)

    def arrived(ref, sem):
        pltpu.make_async_copy(ref, ref, sem).wait()

    def flag(*event):
        return recv_sem.at[flags[event]]

    def rows_of(piece):
        return own_row if PIECES[piece][2] == "own" else other_row

    def lanes_of(piece):
        first, last = PIECES[piece][3:]
        return pl.ds(128 * first, 128 * (last - first))

    def early(piece, link):
        at = (pl.ds(rows_of(piece), OWN), lanes_of(piece))
        return remote(
            x.at[at], raw.at[(LINKS.index(link), *at)], raw_send.at[0], flag(piece, *STEP[link]), link_to[link]
        )

    own_first = {}
    for link in LINKS:
        some = [PIECES[piece][2] for piece in EARLY[link[0]][0]] + ["other"]
        own_first[link] = some.index("other")
        for piece in EARLY[link[0]][0][: own_first[link]]:
            early(piece, link).start()
    tell_z()
    hear_z()
    tell_z()
    to_sibling.wait_recv()
    for link in LINKS:
        for piece in EARLY[link[0]][0][own_first[link] :]:
            early(piece, link).start()
    for _ in range(Z // 2 - 3):
        hear_z()
        tell_z()
    hear_z()

    arrived(peak_yc, yc_sem.at[0])
    best = peak[0]
    for d in range(C * Y - 1):
        best = jnp.maximum(best, peak_yc[d])
    peak1[...] = best

    over_z = [remote(peak1, peak_z.at[d], peak_send.at[0], z_sem.at[0], z_at[d]) for d in range(1, Z)]
    for d in sorted(range(1, Z), key=lambda d: -min(d, Z - d)):
        over_z[d - 1].start()
    arrived(row_yc, norm_sem.at[0])
    line = row0[...]
    for d in range(C * Y - 1):
        line = jnp.maximum(line, row_yc[d])
    rows_z[z] = line
    for d in range(1, Z):
        remote(rows_z.at[z], rows_z.at[z], norm_send.at[1], norm_sem.at[1], z_at[d]).start()
    for link in LINKS:
        for piece in EARLY[link[0]][1]:
            early(piece, link).start()
    arrived(peak_z.at[pl.ds(1, Z - 1)], z_sem.at[0])
    for d in range(1, Z):
        best = jnp.maximum(best, peak_z[d])
    peak2[...] = best
    cols[c] = best

    def block_at(dz, dy):
        chip = lax.rem(z - dz + Z, Z) * Y + lax.rem(y - dy + Y, Y)
        return pl.multiple_of(chip * CHIP, CHIP)

    def scale(piece, source, base):
        for t in range(*PIECES[piece][3:]):
            lanes = slice(128 * t, 128 * t + 128)
            by = jnp.broadcast_to(peak2[t : t + 1, :], (16, 128))
            for r in range(OWN // 16):
                at = pl.multiple_of(rows_of(piece) + 16 * r, 16)
                value = source[pl.ds(at, 16), lanes] / by
                out[c, pl.ds(pl.multiple_of(base + at, 16), 16), lanes] = value.astype(jnp.bfloat16)

    def send_on(piece, dz, dy, base):
        ref = out.at[c, pl.ds(pl.multiple_of(base + rows_of(piece), OWN), OWN), lanes_of(piece)]
        for link, to_z, to_y in forwards(piece, dz, dy):
            if (dz, dy) == (0, 0) and is_early(piece, link):
                continue
            remote(ref, ref, send_sem.at[0], flag(piece, to_z, to_y), link_to[link]).start()

    def send_aside(base, rows=CHIP, lanes=pl.ds(0, COLS)):
        ref = out.at[c, pl.ds(base, rows), lanes]
        remote(ref, ref, side_send.at[0], side_recv.at[0], sibling).start()

    home = block_at(0, 0)

    def norm_over_x():
        arrived(rows_z.at[pl.ds(0, Z - 1)], norm_sem.at[1])
        for d in range(1, X):
            remote(rows_z, rows_x.at[d], norm_send.at[2], norm_sem.at[2], m_at[d]).start()

    def norm_done():
        arrived(rows_x.at[pl.ds(1, X - 1)], norm_sem.at[2])
        for k in range(Z):
            line = rows_z[k]
            for d in range(1, X):
                line = jnp.maximum(line, rows_x[d, k])
            norm[k] = line

    def own_rest():
        for piece in range(len(PIECES)):
            if (piece, 0, 0) not in order:
                scale(piece, x, home)
        send_aside(home)
        remote(cols.at[c], cols.at[c], side_send.at[1], side_recv.at[1], sibling).start()

    n = len(order)
    aside = {n // 8: own_rest, n // 4: norm_over_x, n // 2: norm_done}
    blocks = {}
    for k, (_, dz, dy) in enumerate(order):
        blocks.setdefault((dz % Z, dy % Y), []).append(k)
    blocks.pop((0, 0), None)
    pending = None
    for k, (piece, dz, dy) in enumerate(order):
        if k in aside:
            aside[k]()
        base = block_at(dz, dy)
        link = next((l for l in LINKS if STEP[l] == (dz, dy)), None)
        computed = (dz, dy) == (0, 0) or link is not None and is_early(piece, link)
        if (dz, dy) == (0, 0):
            scale(piece, x, base)
        elif computed:
            early(piece, link).wait_recv()
            scale(piece, raw.at[LINKS.index(link)], base)
        else:
            ref = out.at[c, pl.ds(pl.multiple_of(base + rows_of(piece), OWN), OWN), lanes_of(piece)]
            remote(ref, ref, send_sem.at[0], flag(piece, dz, dy), sibling).wait_recv()
        if pending:
            send_on(*pending)
        pending = (piece, dz, dy, base)
        if not computed:
            send_on(*pending)
            pending = None
        if (dz, dy) != (0, 0):
            last = blocks[dz % Z, dy % Y][-1]
            if last >= n - LATE:
                send_aside(pl.multiple_of(base + rows_of(piece), OWN), OWN, lanes_of(piece))
            elif last == k:
                send_aside(base)

    arrived(cols.at[0], side_send.at[1])
    arrived(cols.at[0], side_recv.at[1])
    to_sibling.wait_send()
    arrived(row_yc, norm_send.at[0])
    arrived(rows_z.at[pl.ds(0, Z - 1)], norm_send.at[1])
    arrived(rows_x.at[pl.ds(1, X - 1)], norm_send.at[2])
    arrived(theirs.at[:, pl.ds(0, 64 * (C * Y + Z - 2))], peak_send.at[0])
    wide = [last - first for _, _, _, first, last in PIECES]
    soon = [sum(is_early(piece, link) for link in LINKS) for piece in range(len(PIECES))]
    arrived(out.at[0, pl.ds(0, 16 * sum(a * b for a, b in zip(soon, wide))), pl.ds(0, 512)], raw_send.at[0])
    arrived(out.at[0, pl.ds(0, 2 * sum((Z * Y - 1 - a) * b for a, b in zip(soon, wide)))], send_sem.at[0])
    whole = out.at[0]
    arrived(whole, side_send.at[0])
    arrived(whole, side_recv.at[0])


def write_kernel(tiles, cols, norm, gate, up, col_gate, col_up, gain, sem):
    parts = 4
    rows = ROWS // parts
    copies = []
    for i, ref in enumerate((gate, up)):
        for k in range(parts):
            at = pl.ds(k * rows, rows)
            copies.append(pltpu.make_async_copy(tiles.at[i, at], ref.at[at], sem.at[i * parts + k]))
    for copy in copies:
        copy.start()
    col_gate[...] = cols[0]
    col_up[...] = cols[1]
    gain[...] = jnp.concatenate([norm[k] for k in range(Z)], axis=0).astype(jnp.bfloat16)
    for copy in copies:
        copy.wait()


def local(one_gate, other_gate, one_up, other_up, mix_share, norm_train, norm_step):
    f32, bf16 = jnp.float32, jnp.bfloat16
    hbm_spec = pl.BlockSpec(memory_space=pltpu.HBM)
    vmem_spec = pl.BlockSpec(memory_space=pltpu.VMEM)
    dma = pltpu.SemaphoreType.DMA
    tiles, cols, norm = pl.pallas_call(
        gather_kernel,
        out_shape=(
            pltpu.VMEM((2, ROWS, COLS), bf16),
            pltpu.VMEM((2, TILES, 128), f32),
            pltpu.VMEM((Z, 2, 128), f32),
        ),
        in_specs=[hbm_spec] * 7,
        out_specs=(vmem_spec,) * 3,
        scratch_shapes=[
            pltpu.SMEM((OWN,), f32), pltpu.SMEM((8,), f32), pltpu.SMEM((8,), f32),
            pltpu.VMEM((4, OWN, COLS), f32),
            pltpu.VMEM((OWN, COLS), f32),
            pltpu.VMEM((CHIP, COLS), f32),
            pltpu.VMEM((len(LINKS), CHIP, COLS), f32),
            pltpu.VMEM((C, TILES, 128), f32),
            pltpu.VMEM((C * Y - 1, TILES, 128), f32),
            pltpu.VMEM((TILES, 128), f32),
            pltpu.VMEM((Z, TILES, 128), f32),
            pltpu.VMEM((TILES, 128), f32),
            pltpu.VMEM((2, 128), f32),
            pltpu.VMEM((C * Y - 1, 2, 128), f32),
            pltpu.VMEM((Z, 2, 128), f32),
            pltpu.VMEM((X, Z, 2, 128), f32),
            dma((5,)), dma((2,)), dma((1,)), dma((1,)), dma((1,)), dma((3,)), dma((3,)),
            dma((1,)), dma((1,)), dma((share_flags(plan()[0])[1],)), dma((2,)), dma((2,)),
            pltpu.SemaphoreType.REGULAR((2,)),
        ],
        compiler_params=pltpu.CompilerParams(
            collective_id=0, has_side_effects=True, vmem_limit_bytes=24 * 2**20
        ),
        name="gather",
    )(
        *(
            pltpu.with_memory_space_constraint(a, pltpu.HBM)
            for a in (mix_share, one_gate, other_gate, one_up, other_up, norm_train, norm_step)
        )
    )
    tiles, cols, norm = (pltpu.with_memory_space_constraint(a, pltpu.VMEM) for a in (tiles, cols, norm))
    gate, up, col_gate, col_up, gain = pl.pallas_call(
        write_kernel,
        out_shape=(
            jax.ShapeDtypeStruct((ROWS, COLS), bf16),
            jax.ShapeDtypeStruct((ROWS, COLS), bf16),
            jax.ShapeDtypeStruct((TILES, 128), f32),
            jax.ShapeDtypeStruct((TILES, 128), f32),
            jax.ShapeDtypeStruct((2 * Z, 128), bf16),
        ),
        in_specs=[vmem_spec] * 3,
        out_specs=(hbm_spec, hbm_spec, vmem_spec, vmem_spec, vmem_spec),
        scratch_shapes=[dma((8,))],
        compiler_params=pltpu.CompilerParams(vmem_limit_bytes=8 * 2**20),
        name="write",
    )(tiles, cols, norm)
    return gate, up, col_gate.reshape(COLS), col_up.reshape(COLS), gain.reshape(ROWS)


def solution(mesh):
    torus = Mesh(mesh.devices.reshape(Z, Y, C, X), SHARD_MODEL)
    return jax.shard_map(
        local,
        mesh=torus,
        in_specs=(
            P(SHARD, "model"), P(SHARD, "model"), P(SHARD, "model"), P(SHARD, "model"),
            P(SHARD), P(SHARD_MODEL), P(SHARD_MODEL),
        ),
        out_specs=(P(None, "model"), P(None, "model"), P("model"), P("model"), P()),
        check_vma=False,
    )
```

```python
import heapq

import jax
import jax.numpy as jnp
from jax import lax
from jax.experimental import pallas as pl
from jax.experimental.pallas import tpu as pltpu
from jax.sharding import Mesh
from jax.sharding import PartitionSpec as P

SHARD = ("shard_0", "shard_1", "shard_2")
SHARD_MODEL = ("shard_0", "shard_1", "shard_2", "model")

Z, Y, C, X = 8, 4, 2, 4
ROWS, COLS, OWN = 2048, 2048, 32
CHIP = C * OWN
TILES = COLS // 128
LOW = -3.0e38
LATE = 24

PIECES = (("A", 0, "own", 0, 6), ("B", 0, "own", 6, 16), ("A", 1, "other", 0, 7), ("B", 1, "other", 7, 16))
FIRST = (3, 1, 0, 2)
EARLY = {"y": ((0, 2, 1), ()), "z": ((1,), (3,))}
LINKS = ("y+", "y-", "z+", "z-")
STEP = {"y+": (0, 1), "y-": (0, -1), "z+": (1, 0), "z-": (-1, 0)}


def is_early(piece, link):
    return any(piece in some for some in EARLY[link[0]])


def reach(half, n):
    return (n // 2, n // 2 - 1) if half == 0 else (n // 2 - 1, n // 2)


def forwards(piece, dz, dy):
    kind, half = PIECES[piece][:2]
    zp, zm = reach(half, Z)
    yp, ym = reach(half, Y)
    along_z, along_y = [], []
    if 0 <= dz < zp:
        along_z.append(("z+", dz + 1, dy))
    if -zm < dz <= 0:
        along_z.append(("z-", dz - 1, dy))
    if 0 <= dy < yp:
        along_y.append(("y+", dz, dy + 1))
    if -ym < dy <= 0:
        along_y.append(("y-", dz, dy - 1))
    if kind == "A":
        return along_z + (along_y if dz == 0 else [])
    return (along_z if dy == 0 else []) + along_y


def plan(hop=2.0, turn=0.04, block=5.6, swap=1.6, over_y=4.0, letters=0.9, over_z=8.5, work=0.08):
    free = dict.fromkeys(LINKS, 0.0)
    queue, order, count = [], [], 0

    def put(piece, link, z, y, at, early=False):
        nonlocal count
        width = (PIECES[piece][4] - PIECES[piece][3]) / TILES / C
        free[link] = max(at, free[link]) + width * block * (2 if early else 1)
        count += 1
        rank = FIRST.index(piece) if early else len(PIECES)
        heapq.heappush(queue, (max(free[link] + hop, over_z), rank, count, piece, z, y))

    for k, begin in enumerate((0.0, over_y)):
        for link in LINKS:
            for piece in EARLY[link[0]][k]:
                put(piece, link, *STEP[link], max(begin, swap if PIECES[piece][2] == "other" else 0.0), True)
        if k == 0:
            for link in ("z+", "z-"):
                free[link] = max(free[link], over_y) + letters
    clock = over_z
    for piece in range(len(PIECES)):
        if not all(is_early(piece, link) for link in LINKS):
            heapq.heappush(queue, (over_z, FIRST.index(piece) - 100, 0, piece, 0, 0))
    while queue:
        at, _, _, piece, dz, dy = heapq.heappop(queue)
        clock = max(clock, at) + turn
        order.append((piece, dz, dy))
        links = [l for l in LINKS if STEP[l] == (dz, dy)]
        if (dz, dy) == (0, 0) or links and is_early(piece, links[0]):
            clock += work
        for link, to_z, to_y in forwards(piece, dz, dy):
            if (dz, dy) != (0, 0) or not is_early(piece, link):
                put(piece, link, to_z, to_y, clock)
        clock += turn
    return order, clock


def came_by(piece, dz, dy):
    along_z = dz != 0 and (PIECES[piece][0] == "A" or dy == 0)
    link = ("z" if along_z else "y") + ("+" if (dz if along_z else dy) > 0 else "-")
    return link, (piece, dz - STEP[link][0], dy - STEP[link][1])


def share_flags(order):
    at = {event: k for k, event in enumerate(order)}
    known = {link: [-1] * len(order) for link in LINKS}
    for k, event in enumerate(order):
        for link in LINKS:
            known[link][k] = known[link][k - 1] if k else -1
        if event[1:] != (0, 0):
            link, before = came_by(*event)
            if before[1:] != (0, 0) or not is_early(event[0], link):
                back = link[0] + ("-" if link[1] == "+" else "+")
                known[back][k] = max(known[back][k], at[before])
    flags, last = {}, []
    for k, event in enumerate(order):
        if event[1:] == (0, 0):
            continue
        link, before = came_by(*event)
        early = before[1:] == (0, 0) and is_early(event[0], link)
        free = [] if early else [i for i, used in enumerate(last) if used <= known[link][at[before]]]
        if free:
            i = min(free, key=lambda i: last[i])
            last[i] = k
        else:
            i = len(last)
            last.append(k)
        flags[event] = i
    return flags, len(last)


def gather_kernel(
    mix_h, one_g, other_g, one_u, other_u, train_h, step_h,
    out, cols, norm,
    mix, train, step, ins, theirs, x, raw, peak, peak_yc, peak1, peak_z, peak2,
    row0, row_yc, rows_z, rows_x,
    in_sem, x_sem, peak_send, yc_sem, z_sem, norm_send, norm_sem,
    raw_send, send_sem, recv_sem, side_send, side_recv, known,
):
    order, _ = plan()
    flags, _ = share_flags(order)
    z, y, c, m = (lax.axis_index(a) for a in SHARD_MODEL)
    mesh_id = pl.DeviceIdType.MESH
    z_at = [(lax.rem(z + d, Z), y, c, m) for d in range(Z)]
    y_at = [(z, lax.rem(y + d, Y), c, m) for d in range(Y)]
    yo_at = [(z, lax.rem(y + d, Y), 1 - c, m) for d in range(Y)]
    m_at = [(z, y, c, lax.rem(m + d, X)) for d in range(X)]
    sibling = yo_at[0]
    link_to = {"z+": z_at[1], "z-": z_at[Z - 1], "y+": y_at[1], "y-": y_at[Y - 1]}

    def remote(src, dst, send, recv, to):
        return pltpu.make_async_remote_copy(
            src_ref=src, dst_ref=dst, send_sem=send, recv_sem=recv, device_id=to, device_id_type=mesh_id
        )

    partners = [*yo_at, *y_at[1:], *(z_at[d] for d in (1, 2, Z - 2, Z - 1)), *m_at[1:]]
    barrier = pltpu.get_barrier_semaphore()
    for to in partners:
        pl.semaphore_signal(barrier, inc=1, device_id=to, device_id_type=mesh_id)

    small = [
        pltpu.make_async_copy(ref, to, in_sem.at[2 + i])
        for i, (ref, to) in enumerate(((mix_h, mix), (train_h, train), (step_h, step)))
    ]
    for copy in small:
        copy.start()
    for ours, pair in ((1 - c, (one_g, other_g)), (c, (one_u, other_u))):
        for k, ref in enumerate(pair):
            pltpu.make_async_copy(ref, ins.at[2 * ours + k], in_sem.at[ours]).start()
    for copy in small:
        copy.wait()

    sub = lax.broadcasted_iota(jnp.int32, (8, 128), 0)
    shares = []
    for r in range(OWN // 8):
        share = jnp.full((8, 128), mix[8 * r], jnp.float32)
        for i in range(1, 8):
            share = jnp.where(sub == i, mix[8 * r + i], share)
        shares.append((share, 1.0 - share))

    def blend(slot, to_peak, store):
        both = ins.at[pl.ds(slot, 2)]
        pltpu.make_async_copy(both, both, in_sem.at[slot // 2]).wait()
        for t in range(TILES):
            lanes = slice(128 * t, 128 * t + 128)
            best = None
            for r, (share, rest) in enumerate(shares):
                rows = slice(8 * r, 8 * r + 8)
                value = share * ins[slot, rows, lanes] + rest * ins[slot + 1, rows, lanes]
                store(r, lanes, value)
                best = jnp.abs(value) if best is None else jnp.maximum(best, jnp.abs(value))
            peak[to_peak, t : t + 1, :] = jnp.max(best, axis=0, keepdims=True)

    own_row, other_row = pl.multiple_of(OWN * c, OWN), pl.multiple_of(OWN * (1 - c), OWN)

    def store_theirs(r, lanes, value):
        theirs[8 * r : 8 * r + 8, lanes] = value

    def store_own(r, lanes, value):
        x[pl.ds(pl.multiple_of(own_row + 8 * r, 8), 8), lanes] = value

    blend(0, 1, store_theirs)
    blend(2, 0, store_own)

    lane2 = lax.broadcasted_iota(jnp.int32, (2, 128), 1)
    sub2 = lax.broadcasted_iota(jnp.int32, (2, 128), 0)
    start = (lax.rem(y, 2) * C + c) * OWN + m * 8
    line = jnp.full((2, 128), LOW, jnp.float32)
    for i in range(8):
        line = jnp.where((lane2 == start + i) & (sub2 == y // 2), train[i] + step[i], line)
    row0[...] = line

    pl.semaphore_wait(barrier, len(partners))

    for way, to in enumerate((z_at[2], z_at[Z - 2])):
        pl.semaphore_signal(known.at[way], inc=1, device_id=to, device_id_type=mesh_id)

    over_yc = []
    for d in (2, 1, 3):
        over_yc.append(remote(peak.at[1], peak_yc.at[2 * d], peak_send.at[0], yc_sem.at[0], yo_at[d]))
        over_yc.append(remote(peak.at[0], peak_yc.at[2 * d - 1], peak_send.at[0], yc_sem.at[0], y_at[d]))
    over_yc.append(remote(peak.at[1], peak_yc.at[0], peak_send.at[0], yc_sem.at[0], sibling))
    for copy in over_yc:
        copy.start()
    to_sibling = remote(theirs, x.at[pl.ds(own_row, OWN)], x_sem.at[0], x_sem.at[1], sibling)
    to_sibling.start()
    for d in (2, 1, 3):
        remote(row0, row_yc.at[2 * d], norm_send.at[0], norm_sem.at[0], yo_at[d]).start()
        remote(row0, row_yc.at[2 * d - 1], norm_send.at[0], norm_sem.at[0], y_at[d]).start()
    remote(row0, row_yc.at[0], norm_send.at[0], norm_sem.at[0], sibling).start()

    def arrived(ref, sem):
        pltpu.make_async_copy(ref, ref, sem).wait()

    def flag(*event):
        return recv_sem.at[flags[event]]

    def rows_of(piece):
        return own_row if PIECES[piece][2] == "own" else other_row

    def lanes_of(piece):
        first, last = PIECES[piece][3:]
        return pl.ds(128 * first, 128 * (last - first))

    def early(piece, link):
        at = (pl.ds(rows_of(piece), OWN), lanes_of(piece))
        return remote(
            x.at[at], raw.at[(LINKS.index(link), *at)], raw_send.at[0], flag(piece, *STEP[link]), link_to[link]
        )

    own_first = {}
    for link in LINKS:
        some = [PIECES[piece][2] for piece in EARLY[link[0]][0]] + ["other"]
        own_first[link] = some.index("other")
        for piece in EARLY[link[0]][0][: own_first[link]]:
            early(piece, link).start()
    to_sibling.wait_recv()
    for link in LINKS:
        for piece in EARLY[link[0]][0][own_first[link] :]:
            early(piece, link).start()

    arrived(peak_yc, yc_sem.at[0])
    best = peak[0]
    for d in range(C * Y - 1):
        best = jnp.maximum(best, peak_yc[d])
    peak1[...] = best

    for way in range(2):
        pl.semaphore_wait(known.at[way], 1)
    over_z = [remote(peak1, peak_z.at[d], peak_send.at[0], z_sem.at[0], z_at[d]) for d in range(1, Z)]
    for d in sorted(range(1, Z), key=lambda d: -min(d, Z - d)):
        over_z[d - 1].start()
    arrived(row_yc, norm_sem.at[0])
    line = row0[...]
    for d in range(C * Y - 1):
        line = jnp.maximum(line, row_yc[d])
    rows_z[z] = line
    for d in range(1, Z):
        remote(rows_z.at[z], rows_z.at[z], norm_send.at[1], norm_sem.at[1], z_at[d]).start()
    for link in LINKS:
        for piece in EARLY[link[0]][1]:
            early(piece, link).start()
    arrived(peak_z.at[pl.ds(1, Z - 1)], z_sem.at[0])
    for d in range(1, Z):
        best = jnp.maximum(best, peak_z[d])
    peak2[...] = best
    cols[c] = best

    def block_at(dz, dy):
        chip = lax.rem(z - dz + Z, Z) * Y + lax.rem(y - dy + Y, Y)
        return pl.multiple_of(chip * CHIP, CHIP)

    def scale(piece, source, base):
        for t in range(*PIECES[piece][3:]):
            lanes = slice(128 * t, 128 * t + 128)
            by = jnp.broadcast_to(peak2[t : t + 1, :], (16, 128))
            for r in range(OWN // 16):
                at = pl.multiple_of(rows_of(piece) + 16 * r, 16)
                value = source[pl.ds(at, 16), lanes] / by
                out[c, pl.ds(pl.multiple_of(base + at, 16), 16), lanes] = value.astype(jnp.bfloat16)

    def send_on(piece, dz, dy, base):
        ref = out.at[c, pl.ds(pl.multiple_of(base + rows_of(piece), OWN), OWN), lanes_of(piece)]
        for link, to_z, to_y in forwards(piece, dz, dy):
            if (dz, dy) == (0, 0) and is_early(piece, link):
                continue
            remote(ref, ref, send_sem.at[0], flag(piece, to_z, to_y), link_to[link]).start()

    def send_aside(base, rows=CHIP, lanes=pl.ds(0, COLS)):
        ref = out.at[c, pl.ds(base, rows), lanes]
        remote(ref, ref, side_send.at[0], side_recv.at[0], sibling).start()

    home = block_at(0, 0)

    def norm_over_x():
        arrived(rows_z.at[pl.ds(0, Z - 1)], norm_sem.at[1])
        for d in range(1, X):
            remote(rows_z, rows_x.at[d], norm_send.at[2], norm_sem.at[2], m_at[d]).start()

    def norm_done():
        arrived(rows_x.at[pl.ds(1, X - 1)], norm_sem.at[2])
        for k in range(Z):
            line = rows_z[k]
            for d in range(1, X):
                line = jnp.maximum(line, rows_x[d, k])
            norm[k] = line

    def own_rest():
        for piece in range(len(PIECES)):
            if (piece, 0, 0) not in order:
                scale(piece, x, home)
        send_aside(home)
        remote(cols.at[c], cols.at[c], side_send.at[1], side_recv.at[1], sibling).start()

    n = len(order)
    aside = {n // 8: own_rest, n // 4: norm_over_x, n // 2: norm_done}
    blocks = {}
    for k, (_, dz, dy) in enumerate(order):
        blocks.setdefault((dz % Z, dy % Y), []).append(k)
    blocks.pop((0, 0), None)
    pending = None
    for k, (piece, dz, dy) in enumerate(order):
        if k in aside:
            aside[k]()
        base = block_at(dz, dy)
        link = next((l for l in LINKS if STEP[l] == (dz, dy)), None)
        computed = (dz, dy) == (0, 0) or link is not None and is_early(piece, link)
        if (dz, dy) == (0, 0):
            scale(piece, x, base)
        elif computed:
            early(piece, link).wait_recv()
            scale(piece, raw.at[LINKS.index(link)], base)
        else:
            ref = out.at[c, pl.ds(pl.multiple_of(base + rows_of(piece), OWN), OWN), lanes_of(piece)]
            remote(ref, ref, send_sem.at[0], flag(piece, dz, dy), sibling).wait_recv()
        if pending:
            send_on(*pending)
        pending = (piece, dz, dy, base)
        if not computed:
            send_on(*pending)
            pending = None
        if (dz, dy) != (0, 0):
            last = blocks[dz % Z, dy % Y][-1]
            if last >= n - LATE:
                send_aside(pl.multiple_of(base + rows_of(piece), OWN), OWN, lanes_of(piece))
            elif last == k:
                send_aside(base)

    arrived(cols.at[0], side_send.at[1])
    arrived(cols.at[0], side_recv.at[1])
    to_sibling.wait_send()
    arrived(row_yc, norm_send.at[0])
    arrived(rows_z.at[pl.ds(0, Z - 1)], norm_send.at[1])
    arrived(rows_x.at[pl.ds(1, X - 1)], norm_send.at[2])
    arrived(theirs.at[:, pl.ds(0, 64 * (C * Y + Z - 2))], peak_send.at[0])
    wide = [last - first for _, _, _, first, last in PIECES]
    soon = [sum(is_early(piece, link) for link in LINKS) for piece in range(len(PIECES))]
    arrived(out.at[0, pl.ds(0, 16 * sum(a * b for a, b in zip(soon, wide))), pl.ds(0, 512)], raw_send.at[0])
    arrived(out.at[0, pl.ds(0, 2 * sum((Z * Y - 1 - a) * b for a, b in zip(soon, wide)))], send_sem.at[0])
    whole = out.at[0]
    arrived(whole, side_send.at[0])
    arrived(whole, side_recv.at[0])


def write_kernel(tiles, cols, norm, gate, up, col_gate, col_up, gain, sem):
    parts = 8
    rows = ROWS // parts
    copies = []
    for i, ref in enumerate((gate, up)):
        for k in range(parts):
            at = pl.ds(k * rows, rows)
            copies.append(pltpu.make_async_copy(tiles.at[i, at], ref.at[at], sem.at[i * parts + k]))
    for copy in copies:
        copy.start()
    col_gate[...] = cols[0]
    col_up[...] = cols[1]
    gain[...] = jnp.concatenate([norm[k] for k in range(Z)], axis=0).astype(jnp.bfloat16)
    for copy in copies:
        copy.wait()


def local(one_gate, other_gate, one_up, other_up, mix_share, norm_train, norm_step):
    f32, bf16 = jnp.float32, jnp.bfloat16
    hbm_spec = pl.BlockSpec(memory_space=pltpu.HBM)
    vmem_spec = pl.BlockSpec(memory_space=pltpu.VMEM)
    dma = pltpu.SemaphoreType.DMA
    tiles, cols, norm = pl.pallas_call(
        gather_kernel,
        out_shape=(
            pltpu.VMEM((2, ROWS, COLS), bf16),
            pltpu.VMEM((2, TILES, 128), f32),
            pltpu.VMEM((Z, 2, 128), f32),
        ),
        in_specs=[hbm_spec] * 7,
        out_specs=(vmem_spec,) * 3,
        scratch_shapes=[
            pltpu.SMEM((OWN,), f32), pltpu.SMEM((8,), f32), pltpu.SMEM((8,), f32),
            pltpu.VMEM((4, OWN, COLS), f32),
            pltpu.VMEM((OWN, COLS), f32),
            pltpu.VMEM((CHIP, COLS), f32),
            pltpu.VMEM((len(LINKS), CHIP, COLS), f32),
            pltpu.VMEM((C, TILES, 128), f32),
            pltpu.VMEM((C * Y - 1, TILES, 128), f32),
            pltpu.VMEM((TILES, 128), f32),
            pltpu.VMEM((Z, TILES, 128), f32),
            pltpu.VMEM((TILES, 128), f32),
            pltpu.VMEM((2, 128), f32),
            pltpu.VMEM((C * Y - 1, 2, 128), f32),
            pltpu.VMEM((Z, 2, 128), f32),
            pltpu.VMEM((X, Z, 2, 128), f32),
            dma((5,)), dma((2,)), dma((1,)), dma((1,)), dma((1,)), dma((3,)), dma((3,)),
            dma((1,)), dma((1,)), dma((share_flags(plan()[0])[1],)), dma((2,)), dma((2,)),
            pltpu.SemaphoreType.REGULAR((2,)),
        ],
        compiler_params=pltpu.CompilerParams(
            collective_id=0, has_side_effects=True, vmem_limit_bytes=24 * 2**20
        ),
        name="gather",
    )(
        *(
            pltpu.with_memory_space_constraint(a, pltpu.HBM)
            for a in (mix_share, one_gate, other_gate, one_up, other_up, norm_train, norm_step)
        )
    )
    tiles, cols, norm = (pltpu.with_memory_space_constraint(a, pltpu.VMEM) for a in (tiles, cols, norm))
    gate, up, col_gate, col_up, gain = pl.pallas_call(
        write_kernel,
        out_shape=(
            jax.ShapeDtypeStruct((ROWS, COLS), bf16),
            jax.ShapeDtypeStruct((ROWS, COLS), bf16),
            jax.ShapeDtypeStruct((TILES, 128), f32),
            jax.ShapeDtypeStruct((TILES, 128), f32),
            jax.ShapeDtypeStruct((2 * Z, 128), bf16),
        ),
        in_specs=[vmem_spec] * 3,
        out_specs=(hbm_spec, hbm_spec, vmem_spec, vmem_spec, vmem_spec),
        scratch_shapes=[dma((16,))],
        compiler_params=pltpu.CompilerParams(vmem_limit_bytes=8 * 2**20),
        name="write",
    )(tiles, cols, norm)
    return gate, up, col_gate.reshape(COLS), col_up.reshape(COLS), gain.reshape(ROWS)


def solution(mesh):
    torus = Mesh(mesh.devices.reshape(Z, Y, C, X), SHARD_MODEL)
    return jax.shard_map(
        local,
        mesh=torus,
        in_specs=(
            P(SHARD, "model"), P(SHARD, "model"), P(SHARD, "model"), P(SHARD, "model"),
            P(SHARD), P(SHARD_MODEL), P(SHARD_MODEL),
        ),
        out_specs=(P(None, "model"), P(None, "model"), P("model"), P("model"), P()),
        check_vma=False,
    )
```

```python
import heapq

import jax
import jax.numpy as jnp
from jax import lax
from jax.experimental import pallas as pl
from jax.experimental.pallas import tpu as pltpu
from jax.sharding import Mesh
from jax.sharding import PartitionSpec as P

SHARD = ("shard_0", "shard_1", "shard_2")
SHARD_MODEL = ("shard_0", "shard_1", "shard_2", "model")

Z, Y, C, X = 8, 4, 2, 4
ROWS, COLS, OWN = 2048, 2048, 32
CHIP = C * OWN
TILES = COLS // 128
LOW = -3.0e38
LATE = 24

PIECES = (("A", 0, "own", 0, 6), ("B", 0, "own", 6, 16), ("A", 1, "other", 0, 7), ("B", 1, "other", 7, 16))
FIRST = (3, 1, 0, 2)
EARLY = {"y": ((0, 2, 1), ()), "z": ((1,), (3,))}
LINKS = ("y+", "y-", "z+", "z-")
STEP = {"y+": (0, 1), "y-": (0, -1), "z+": (1, 0), "z-": (-1, 0)}


def is_early(piece, link):
    return any(piece in some for some in EARLY[link[0]])


def reach(half, n):
    return (n // 2, n // 2 - 1) if half == 0 else (n // 2 - 1, n // 2)


def forwards(piece, dz, dy):
    kind, half = PIECES[piece][:2]
    zp, zm = reach(half, Z)
    yp, ym = reach(half, Y)
    along_z, along_y = [], []
    if 0 <= dz < zp:
        along_z.append(("z+", dz + 1, dy))
    if -zm < dz <= 0:
        along_z.append(("z-", dz - 1, dy))
    if 0 <= dy < yp:
        along_y.append(("y+", dz, dy + 1))
    if -ym < dy <= 0:
        along_y.append(("y-", dz, dy - 1))
    if kind == "A":
        return along_z + (along_y if dz == 0 else [])
    return (along_z if dy == 0 else []) + along_y


def plan(hop=2.0, turn=0.04, block=5.6, swap=1.6, over_y=4.0, letters=0.9, over_z=8.5, work=0.08):
    free = dict.fromkeys(LINKS, 0.0)
    queue, order, count = [], [], 0

    def put(piece, link, z, y, at, early=False):
        nonlocal count
        width = (PIECES[piece][4] - PIECES[piece][3]) / TILES / C
        free[link] = max(at, free[link]) + width * block * (2 if early else 1)
        count += 1
        rank = FIRST.index(piece) if early else len(PIECES)
        heapq.heappush(queue, (max(free[link] + hop, over_z), rank, count, piece, z, y))

    for k, begin in enumerate((0.0, over_y)):
        for link in LINKS:
            for piece in EARLY[link[0]][k]:
                put(piece, link, *STEP[link], max(begin, swap if PIECES[piece][2] == "other" else 0.0), True)
        if k == 0:
            for link in ("z+", "z-"):
                free[link] = max(free[link], over_y) + letters
    clock = over_z
    for piece in range(len(PIECES)):
        if not all(is_early(piece, link) for link in LINKS):
            heapq.heappush(queue, (over_z, FIRST.index(piece) - 100, 0, piece, 0, 0))
    while queue:
        at, _, _, piece, dz, dy = heapq.heappop(queue)
        clock = max(clock, at) + turn
        order.append((piece, dz, dy))
        links = [l for l in LINKS if STEP[l] == (dz, dy)]
        if (dz, dy) == (0, 0) or links and is_early(piece, links[0]):
            clock += work
        for link, to_z, to_y in forwards(piece, dz, dy):
            if (dz, dy) != (0, 0) or not is_early(piece, link):
                put(piece, link, to_z, to_y, clock)
        clock += turn
    return order, clock


def came_by(piece, dz, dy):
    along_z = dz != 0 and (PIECES[piece][0] == "A" or dy == 0)
    link = ("z" if along_z else "y") + ("+" if (dz if along_z else dy) > 0 else "-")
    return link, (piece, dz - STEP[link][0], dy - STEP[link][1])


def share_flags(order):
    at = {event: k for k, event in enumerate(order)}
    known = {link: [-1] * len(order) for link in LINKS}
    for k, event in enumerate(order):
        for link in LINKS:
            known[link][k] = known[link][k - 1] if k else -1
        if event[1:] != (0, 0):
            link, before = came_by(*event)
            if before[1:] != (0, 0) or not is_early(event[0], link):
                back = link[0] + ("-" if link[1] == "+" else "+")
                known[back][k] = max(known[back][k], at[before])
    flags, last = {}, []
    for k, event in enumerate(order):
        if event[1:] == (0, 0):
            continue
        link, before = came_by(*event)
        early = before[1:] == (0, 0) and is_early(event[0], link)
        free = [] if early else [i for i, used in enumerate(last) if used <= known[link][at[before]]]
        if free:
            i = min(free, key=lambda i: last[i])
            last[i] = k
        else:
            i = len(last)
            last.append(k)
        flags[event] = i
    return flags, len(last)


def gather_kernel(
    mix_h, one_g, other_g, one_u, other_u, train_h, step_h,
    out, cols, norm,
    mix, train, step, ins, theirs, x, raw, peak, peak_yc, peak1, peak_z, peak2,
    row0, row_yc, rows_z, rows_x,
    in_sem, x_sem, peak_send, yc_sem, z_sem, norm_send, norm_sem,
    raw_send, send_sem, recv_sem, side_send, side_recv, known,
):
    order, _ = plan()
    flags, _ = share_flags(order)
    z, y, c, m = (lax.axis_index(a) for a in SHARD_MODEL)
    mesh_id = pl.DeviceIdType.MESH
    z_at = [(lax.rem(z + d, Z), y, c, m) for d in range(Z)]
    y_at = [(z, lax.rem(y + d, Y), c, m) for d in range(Y)]
    yo_at = [(z, lax.rem(y + d, Y), 1 - c, m) for d in range(Y)]
    m_at = [(z, y, c, lax.rem(m + d, X)) for d in range(X)]
    sibling = yo_at[0]
    link_to = {"z+": z_at[1], "z-": z_at[Z - 1], "y+": y_at[1], "y-": y_at[Y - 1]}

    def remote(src, dst, send, recv, to):
        return pltpu.make_async_remote_copy(
            src_ref=src, dst_ref=dst, send_sem=send, recv_sem=recv, device_id=to, device_id_type=mesh_id
        )

    partners = [z_at[2], z_at[Z - 2], yo_at[2], y_at[2], *(z_at[d] for d in (1, Z - 1)), *(yo_at[d] for d in (1, 3))]
    partners += [y_at[1], y_at[3], sibling, *m_at[1:]]
    barrier = pltpu.get_barrier_semaphore()
    for to in partners:
        pl.semaphore_signal(barrier, inc=1, device_id=to, device_id_type=mesh_id)

    small = [
        pltpu.make_async_copy(ref, to, in_sem.at[2 + i])
        for i, (ref, to) in enumerate(((mix_h, mix), (train_h, train), (step_h, step)))
    ]
    for copy in small:
        copy.start()
    for ours, pair in ((1 - c, (one_g, other_g)), (c, (one_u, other_u))):
        for k, ref in enumerate(pair):
            pltpu.make_async_copy(ref, ins.at[2 * ours + k], in_sem.at[ours]).start()
    for copy in small:
        copy.wait()

    sub = lax.broadcasted_iota(jnp.int32, (8, 128), 0)
    shares = []
    for r in range(OWN // 8):
        share = jnp.full((8, 128), mix[8 * r], jnp.float32)
        for i in range(1, 8):
            share = jnp.where(sub == i, mix[8 * r + i], share)
        shares.append((share, 1.0 - share))

    def blend(slot, to_peak, store):
        both = ins.at[pl.ds(slot, 2)]
        pltpu.make_async_copy(both, both, in_sem.at[slot // 2]).wait()
        for t in range(TILES):
            lanes = slice(128 * t, 128 * t + 128)
            best = None
            for r, (share, rest) in enumerate(shares):
                rows = slice(8 * r, 8 * r + 8)
                value = share * ins[slot, rows, lanes] + rest * ins[slot + 1, rows, lanes]
                store(r, lanes, value)
                best = jnp.abs(value) if best is None else jnp.maximum(best, jnp.abs(value))
            peak[to_peak, t : t + 1, :] = jnp.max(best, axis=0, keepdims=True)

    own_row, other_row = pl.multiple_of(OWN * c, OWN), pl.multiple_of(OWN * (1 - c), OWN)

    def store_theirs(r, lanes, value):
        theirs[8 * r : 8 * r + 8, lanes] = value

    def store_own(r, lanes, value):
        x[pl.ds(pl.multiple_of(own_row + 8 * r, 8), 8), lanes] = value

    blend(0, 1, store_theirs)
    blend(2, 0, store_own)

    lane2 = lax.broadcasted_iota(jnp.int32, (2, 128), 1)
    sub2 = lax.broadcasted_iota(jnp.int32, (2, 128), 0)
    start = (lax.rem(y, 2) * C + c) * OWN + m * 8
    line = jnp.full((2, 128), LOW, jnp.float32)
    for i in range(8):
        line = jnp.where((lane2 == start + i) & (sub2 == y // 2), train[i] + step[i], line)
    row0[...] = line

    pl.semaphore_wait(barrier, len(partners))

    for way, to in enumerate((z_at[2], z_at[Z - 2])):
        pl.semaphore_signal(known.at[way], inc=1, device_id=to, device_id_type=mesh_id)

    over_yc = []
    for d in (2, 1, 3):
        over_yc.append(remote(peak.at[1], peak_yc.at[2 * d], peak_send.at[0], yc_sem.at[0], yo_at[d]))
        over_yc.append(remote(peak.at[0], peak_yc.at[2 * d - 1], peak_send.at[0], yc_sem.at[0], y_at[d]))
    over_yc.append(remote(peak.at[1], peak_yc.at[0], peak_send.at[0], yc_sem.at[0], sibling))
    for copy in over_yc:
        copy.start()
    to_sibling = remote(theirs, x.at[pl.ds(own_row, OWN)], x_sem.at[0], x_sem.at[1], sibling)
    to_sibling.start()
    for d in (2, 1, 3):
        remote(row0, row_yc.at[2 * d], norm_send.at[0], norm_sem.at[0], yo_at[d]).start()
        remote(row0, row_yc.at[2 * d - 1], norm_send.at[0], norm_sem.at[0], y_at[d]).start()
    remote(row0, row_yc.at[0], norm_send.at[0], norm_sem.at[0], sibling).start()

    def arrived(ref, sem):
        pltpu.make_async_copy(ref, ref, sem).wait()

    def flag(*event):
        return recv_sem.at[flags[event]]

    def rows_of(piece):
        return own_row if PIECES[piece][2] == "own" else other_row

    def lanes_of(piece):
        first, last = PIECES[piece][3:]
        return pl.ds(128 * first, 128 * (last - first))

    def early(piece, link):
        at = (pl.ds(rows_of(piece), OWN), lanes_of(piece))
        return remote(
            x.at[at], raw.at[(LINKS.index(link), *at)], raw_send.at[0], flag(piece, *STEP[link]), link_to[link]
        )

    own_first = {}
    for link in LINKS:
        some = [PIECES[piece][2] for piece in EARLY[link[0]][0]] + ["other"]
        own_first[link] = some.index("other")
        for piece in EARLY[link[0]][0][: own_first[link]]:
            early(piece, link).start()
    to_sibling.wait_recv()
    for link in LINKS:
        for piece in EARLY[link[0]][0][own_first[link] :]:
            early(piece, link).start()

    arrived(peak_yc, yc_sem.at[0])
    best = peak[0]
    for d in range(C * Y - 1):
        best = jnp.maximum(best, peak_yc[d])
    peak1[...] = best

    for way in range(2):
        pl.semaphore_wait(known.at[way], 1)
    over_z = [remote(peak1, peak_z.at[d], peak_send.at[0], z_sem.at[0], z_at[d]) for d in range(1, Z)]
    for d in sorted(range(1, Z), key=lambda d: -min(d, Z - d)):
        over_z[d - 1].start()
    arrived(row_yc, norm_sem.at[0])
    line = row0[...]
    for d in range(C * Y - 1):
        line = jnp.maximum(line, row_yc[d])
    rows_z[z] = line
    for d in range(1, Z):
        remote(rows_z.at[z], rows_z.at[z], norm_send.at[1], norm_sem.at[1], z_at[d]).start()
    for link in LINKS:
        for piece in EARLY[link[0]][1]:
            early(piece, link).start()
    arrived(peak_z.at[pl.ds(1, Z - 1)], z_sem.at[0])
    for d in range(1, Z):
        best = jnp.maximum(best, peak_z[d])
    peak2[...] = best
    cols[c] = best

    def block_at(dz, dy):
        chip = lax.rem(z - dz + Z, Z) * Y + lax.rem(y - dy + Y, Y)
        return pl.multiple_of(chip * CHIP, CHIP)

    def scale(piece, source, base):
        for t in range(*PIECES[piece][3:]):
            lanes = slice(128 * t, 128 * t + 128)
            by = jnp.broadcast_to(peak2[t : t + 1, :], (16, 128))
            for r in range(OWN // 16):
                at = pl.multiple_of(rows_of(piece) + 16 * r, 16)
                value = source[pl.ds(at, 16), lanes] / by
                out[c, pl.ds(pl.multiple_of(base + at, 16), 16), lanes] = value.astype(jnp.bfloat16)

    def send_on(piece, dz, dy, base):
        ref = out.at[c, pl.ds(pl.multiple_of(base + rows_of(piece), OWN), OWN), lanes_of(piece)]
        for link, to_z, to_y in forwards(piece, dz, dy):
            if (dz, dy) == (0, 0) and is_early(piece, link):
                continue
            remote(ref, ref, send_sem.at[0], flag(piece, to_z, to_y), link_to[link]).start()

    def send_aside(base, rows=CHIP, lanes=pl.ds(0, COLS)):
        ref = out.at[c, pl.ds(base, rows), lanes]
        remote(ref, ref, side_send.at[0], side_recv.at[0], sibling).start()

    home = block_at(0, 0)

    def norm_over_x():
        arrived(rows_z.at[pl.ds(0, Z - 1)], norm_sem.at[1])
        for d in range(1, X):
            remote(rows_z, rows_x.at[d], norm_send.at[2], norm_sem.at[2], m_at[d]).start()

    def norm_done():
        arrived(rows_x.at[pl.ds(1, X - 1)], norm_sem.at[2])
        for k in range(Z):
            line = rows_z[k]
            for d in range(1, X):
                line = jnp.maximum(line, rows_x[d, k])
            norm[k] = line

    def own_rest():
        for piece in range(len(PIECES)):
            if (piece, 0, 0) not in order:
                scale(piece, x, home)
        send_aside(home)
        remote(cols.at[c], cols.at[c], side_send.at[1], side_recv.at[1], sibling).start()

    n = len(order)
    aside = {n // 8: own_rest, n // 4: norm_over_x, n // 2: norm_done}
    blocks = {}
    for k, (_, dz, dy) in enumerate(order):
        blocks.setdefault((dz % Z, dy % Y), []).append(k)
    blocks.pop((0, 0), None)
    pending = None
    for k, (piece, dz, dy) in enumerate(order):
        if k in aside:
            aside[k]()
        base = block_at(dz, dy)
        link = next((l for l in LINKS if STEP[l] == (dz, dy)), None)
        computed = (dz, dy) == (0, 0) or link is not None and is_early(piece, link)
        if (dz, dy) == (0, 0):
            scale(piece, x, base)
        elif computed:
            early(piece, link).wait_recv()
            scale(piece, raw.at[LINKS.index(link)], base)
        else:
            ref = out.at[c, pl.ds(pl.multiple_of(base + rows_of(piece), OWN), OWN), lanes_of(piece)]
            remote(ref, ref, send_sem.at[0], flag(piece, dz, dy), sibling).wait_recv()
        if pending:
            send_on(*pending)
        pending = (piece, dz, dy, base)
        if not computed:
            send_on(*pending)
            pending = None
        if (dz, dy) != (0, 0):
            last = blocks[dz % Z, dy % Y][-1]
            if last >= n - LATE:
                send_aside(pl.multiple_of(base + rows_of(piece), OWN), OWN, lanes_of(piece))
            elif last == k:
                send_aside(base)

    arrived(cols.at[0], side_send.at[1])
    arrived(cols.at[0], side_recv.at[1])
    to_sibling.wait_send()
    arrived(row_yc, norm_send.at[0])
    arrived(rows_z.at[pl.ds(0, Z - 1)], norm_send.at[1])
    arrived(rows_x.at[pl.ds(1, X - 1)], norm_send.at[2])
    arrived(theirs.at[:, pl.ds(0, 64 * (C * Y + Z - 2))], peak_send.at[0])
    wide = [last - first for _, _, _, first, last in PIECES]
    soon = [sum(is_early(piece, link) for link in LINKS) for piece in range(len(PIECES))]
    arrived(out.at[0, pl.ds(0, 16 * sum(a * b for a, b in zip(soon, wide))), pl.ds(0, 512)], raw_send.at[0])
    arrived(out.at[0, pl.ds(0, 2 * sum((Z * Y - 1 - a) * b for a, b in zip(soon, wide)))], send_sem.at[0])
    whole = out.at[0]
    arrived(whole, side_send.at[0])
    arrived(whole, side_recv.at[0])


def write_kernel(tiles, cols, norm, gate, up, col_gate, col_up, gain, narrow, sem):
    parts = 4
    rows = ROWS // parts
    copies = []
    for i, ref in enumerate((gate, up)):
        for k in range(parts):
            at = pl.ds(k * rows, rows)
            copies.append(pltpu.make_async_copy(tiles.at[i, at], ref.at[at], sem.at[i * parts + k]))
    copies.append(pltpu.make_async_copy(cols.at[0], col_gate, sem.at[2 * parts]))
    copies.append(pltpu.make_async_copy(cols.at[1], col_up, sem.at[2 * parts + 1]))
    for copy in copies:
        copy.start()
    narrow[...] = jnp.concatenate([norm[k] for k in range(Z)], axis=0).astype(jnp.bfloat16)
    copies.append(pltpu.make_async_copy(narrow, gain, sem.at[2 * parts + 2]))
    copies[-1].start()
    for copy in copies:
        copy.wait()


def local(one_gate, other_gate, one_up, other_up, mix_share, norm_train, norm_step):
    f32, bf16 = jnp.float32, jnp.bfloat16
    hbm_spec = pl.BlockSpec(memory_space=pltpu.HBM)
    vmem_spec = pl.BlockSpec(memory_space=pltpu.VMEM)
    dma = pltpu.SemaphoreType.DMA
    tiles, cols, norm = pl.pallas_call(
        gather_kernel,
        out_shape=(
            pltpu.VMEM((2, ROWS, COLS), bf16),
            pltpu.VMEM((2, TILES, 128), f32),
            pltpu.VMEM((Z, 2, 128), f32),
        ),
        in_specs=[hbm_spec] * 7,
        out_specs=(vmem_spec,) * 3,
        scratch_shapes=[
            pltpu.SMEM((OWN,), f32), pltpu.SMEM((8,), f32), pltpu.SMEM((8,), f32),
            pltpu.VMEM((4, OWN, COLS), f32),
            pltpu.VMEM((OWN, COLS), f32),
            pltpu.VMEM((CHIP, COLS), f32),
            pltpu.VMEM((len(LINKS), CHIP, COLS), f32),
            pltpu.VMEM((C, TILES, 128), f32),
            pltpu.VMEM((C * Y - 1, TILES, 128), f32),
            pltpu.VMEM((TILES, 128), f32),
            pltpu.VMEM((Z, TILES, 128), f32),
            pltpu.VMEM((TILES, 128), f32),
            pltpu.VMEM((2, 128), f32),
            pltpu.VMEM((C * Y - 1, 2, 128), f32),
            pltpu.VMEM((Z, 2, 128), f32),
            pltpu.VMEM((X, Z, 2, 128), f32),
            dma((5,)), dma((2,)), dma((1,)), dma((1,)), dma((1,)), dma((3,)), dma((3,)),
            dma((1,)), dma((1,)), dma((share_flags(plan()[0])[1],)), dma((2,)), dma((2,)),
            pltpu.SemaphoreType.REGULAR((2,)),
        ],
        compiler_params=pltpu.CompilerParams(
            collective_id=0, has_side_effects=True, vmem_limit_bytes=24 * 2**20
        ),
        name="gather",
    )(
        *(
            pltpu.with_memory_space_constraint(a, pltpu.HBM)
            for a in (mix_share, one_gate, other_gate, one_up, other_up, norm_train, norm_step)
        )
    )
    tiles, cols, norm = (pltpu.with_memory_space_constraint(a, pltpu.VMEM) for a in (tiles, cols, norm))
    gate, up, col_gate, col_up, gain = pl.pallas_call(
        write_kernel,
        out_shape=(
            jax.ShapeDtypeStruct((ROWS, COLS), bf16),
            jax.ShapeDtypeStruct((ROWS, COLS), bf16),
            jax.ShapeDtypeStruct((TILES, 128), f32),
            jax.ShapeDtypeStruct((TILES, 128), f32),
            jax.ShapeDtypeStruct((2 * Z, 128), bf16),
        ),
        in_specs=[vmem_spec] * 3,
        out_specs=(hbm_spec,) * 5,
        scratch_shapes=[pltpu.VMEM((2 * Z, 128), bf16), dma((11,))],
        compiler_params=pltpu.CompilerParams(vmem_limit_bytes=8 * 2**20),
        name="write",
    )(tiles, cols, norm)
    return gate, up, col_gate.reshape(COLS), col_up.reshape(COLS), gain.reshape(ROWS)


def solution(mesh):
    torus = Mesh(mesh.devices.reshape(Z, Y, C, X), SHARD_MODEL)
    return jax.shard_map(
        local,
        mesh=torus,
        in_specs=(
            P(SHARD, "model"), P(SHARD, "model"), P(SHARD, "model"), P(SHARD, "model"),
            P(SHARD), P(SHARD_MODEL), P(SHARD_MODEL),
        ),
        out_specs=(P(None, "model"), P(None, "model"), P("model"), P("model"), P()),
        check_vma=False,
    )
```

```python
import heapq

import jax
import jax.numpy as jnp
from jax import lax
from jax.experimental import pallas as pl
from jax.experimental.pallas import tpu as pltpu
from jax.sharding import Mesh
from jax.sharding import PartitionSpec as P

SHARD = ("shard_0", "shard_1", "shard_2")
SHARD_MODEL = ("shard_0", "shard_1", "shard_2", "model")

Z, Y, C, X = 8, 4, 2, 4
ROWS, COLS, OWN = 2048, 2048, 32
CHIP = C * OWN
TILES = COLS // 128
LOW = -3.0e38
LATE = 24

PIECES = (("A", 0, "own", 0, 6), ("B", 0, "own", 6, 16), ("A", 1, "other", 0, 7), ("B", 1, "other", 7, 16))
FIRST = (3, 1, 0, 2)
EARLY = {"y": ((0, 2, 1), ()), "z": ((1,), (3,))}
LINKS = ("y+", "y-", "z+", "z-")
STEP = {"y+": (0, 1), "y-": (0, -1), "z+": (1, 0), "z-": (-1, 0)}


def is_early(piece, link):
    return any(piece in some for some in EARLY[link[0]])


def reach(half, n):
    return (n // 2, n // 2 - 1) if half == 0 else (n // 2 - 1, n // 2)


def forwards(piece, dz, dy):
    kind, half = PIECES[piece][:2]
    zp, zm = reach(half, Z)
    yp, ym = reach(half, Y)
    along_z, along_y = [], []
    if 0 <= dz < zp:
        along_z.append(("z+", dz + 1, dy))
    if -zm < dz <= 0:
        along_z.append(("z-", dz - 1, dy))
    if 0 <= dy < yp:
        along_y.append(("y+", dz, dy + 1))
    if -ym < dy <= 0:
        along_y.append(("y-", dz, dy - 1))
    if kind == "A":
        return along_z + (along_y if dz == 0 else [])
    return (along_z if dy == 0 else []) + along_y


def plan(hop=2.0, turn=0.04, block=5.6, swap=1.6, over_y=4.0, letters=0.9, over_z=8.5, work=0.08):
    free = dict.fromkeys(LINKS, 0.0)
    queue, order, count = [], [], 0

    def put(piece, link, z, y, at, early=False):
        nonlocal count
        width = (PIECES[piece][4] - PIECES[piece][3]) / TILES / C
        free[link] = max(at, free[link]) + width * block * (2 if early else 1)
        count += 1
        rank = FIRST.index(piece) if early else len(PIECES)
        heapq.heappush(queue, (max(free[link] + hop, over_z), rank, count, piece, z, y))

    for k, begin in enumerate((0.0, over_y)):
        for link in LINKS:
            for piece in EARLY[link[0]][k]:
                put(piece, link, *STEP[link], max(begin, swap if PIECES[piece][2] == "other" else 0.0), True)
        if k == 0:
            for link in ("z+", "z-"):
                free[link] = max(free[link], over_y) + letters
    clock = over_z
    for piece in range(len(PIECES)):
        if not all(is_early(piece, link) for link in LINKS):
            heapq.heappush(queue, (over_z, FIRST.index(piece) - 100, 0, piece, 0, 0))
    while queue:
        at, _, _, piece, dz, dy = heapq.heappop(queue)
        clock = max(clock, at) + turn
        order.append((piece, dz, dy))
        links = [l for l in LINKS if STEP[l] == (dz, dy)]
        if (dz, dy) == (0, 0) or links and is_early(piece, links[0]):
            clock += work
        for link, to_z, to_y in forwards(piece, dz, dy):
            if (dz, dy) != (0, 0) or not is_early(piece, link):
                put(piece, link, to_z, to_y, clock)
        clock += turn
    return order, clock


def came_by(piece, dz, dy):
    along_z = dz != 0 and (PIECES[piece][0] == "A" or dy == 0)
    link = ("z" if along_z else "y") + ("+" if (dz if along_z else dy) > 0 else "-")
    return link, (piece, dz - STEP[link][0], dy - STEP[link][1])


def share_flags(order):
    at = {event: k for k, event in enumerate(order)}
    known = {link: [-1] * len(order) for link in LINKS}
    for k, event in enumerate(order):
        for link in LINKS:
            known[link][k] = known[link][k - 1] if k else -1
        if event[1:] != (0, 0):
            link, before = came_by(*event)
            if before[1:] != (0, 0) or not is_early(event[0], link):
                back = link[0] + ("-" if link[1] == "+" else "+")
                known[back][k] = max(known[back][k], at[before])
    flags, last = {}, []
    for k, event in enumerate(order):
        if event[1:] == (0, 0):
            continue
        link, before = came_by(*event)
        early = before[1:] == (0, 0) and is_early(event[0], link)
        free = [] if early else [i for i, used in enumerate(last) if used <= known[link][at[before]]]
        if free:
            i = min(free, key=lambda i: last[i])
            last[i] = k
        else:
            i = len(last)
            last.append(k)
        flags[event] = i
    return flags, len(last)


def gather_kernel(
    mix_h, one_g, other_g, one_u, other_u, train_h, step_h,
    out, cols, norm,
    mix, train, step, ins, theirs, x, raw, peak, peak_yc, peak1, peak_z, peak2,
    row0, row_yc, rows_z, rows_x,
    in_sem, x_sem, peak_send, yc_sem, z_sem, norm_send, norm_sem,
    raw_send, send_sem, recv_sem, side_send, side_recv, known,
):
    order, _ = plan()
    flags, _ = share_flags(order)
    z, y, c, m = (lax.axis_index(a) for a in SHARD_MODEL)
    mesh_id = pl.DeviceIdType.MESH
    z_at = [(lax.rem(z + d, Z), y, c, m) for d in range(Z)]
    y_at = [(z, lax.rem(y + d, Y), c, m) for d in range(Y)]
    yo_at = [(z, lax.rem(y + d, Y), 1 - c, m) for d in range(Y)]
    m_at = [(z, y, c, lax.rem(m + d, X)) for d in range(X)]
    sibling = yo_at[0]
    link_to = {"z+": z_at[1], "z-": z_at[Z - 1], "y+": y_at[1], "y-": y_at[Y - 1]}

    def remote(src, dst, send, recv, to):
        return pltpu.make_async_remote_copy(
            src_ref=src, dst_ref=dst, send_sem=send, recv_sem=recv, device_id=to, device_id_type=mesh_id
        )

    partners = [z_at[2], z_at[Z - 2], yo_at[2], y_at[2], *(z_at[d] for d in (1, Z - 1)), *(yo_at[d] for d in (1, 3))]
    partners += [y_at[1], y_at[3], sibling, m_at[1], m_at[X - 1]]
    barrier = pltpu.get_barrier_semaphore()
    for to in partners:
        pl.semaphore_signal(barrier, inc=1, device_id=to, device_id_type=mesh_id)

    small = [
        pltpu.make_async_copy(ref, to, in_sem.at[2 + i])
        for i, (ref, to) in enumerate(((mix_h, mix), (train_h, train), (step_h, step)))
    ]
    for copy in small:
        copy.start()
    for ours, pair in ((1 - c, (one_g, other_g)), (c, (one_u, other_u))):
        for k, ref in enumerate(pair):
            pltpu.make_async_copy(ref, ins.at[2 * ours + k], in_sem.at[ours]).start()
    for copy in small:
        copy.wait()

    sub = lax.broadcasted_iota(jnp.int32, (8, 128), 0)
    shares = []
    for r in range(OWN // 8):
        share = jnp.full((8, 128), mix[8 * r], jnp.float32)
        for i in range(1, 8):
            share = jnp.where(sub == i, mix[8 * r + i], share)
        shares.append((share, 1.0 - share))

    def blend(slot, to_peak, store):
        both = ins.at[pl.ds(slot, 2)]
        pltpu.make_async_copy(both, both, in_sem.at[slot // 2]).wait()
        for t in range(TILES):
            lanes = slice(128 * t, 128 * t + 128)
            best = None
            for r, (share, rest) in enumerate(shares):
                rows = slice(8 * r, 8 * r + 8)
                value = share * ins[slot, rows, lanes] + rest * ins[slot + 1, rows, lanes]
                store(r, lanes, value)
                best = jnp.abs(value) if best is None else jnp.maximum(best, jnp.abs(value))
            peak[to_peak, t : t + 1, :] = jnp.max(best, axis=0, keepdims=True)

    own_row, other_row = pl.multiple_of(OWN * c, OWN), pl.multiple_of(OWN * (1 - c), OWN)

    def store_theirs(r, lanes, value):
        theirs[8 * r : 8 * r + 8, lanes] = value

    def store_own(r, lanes, value):
        x[pl.ds(pl.multiple_of(own_row + 8 * r, 8), 8), lanes] = value

    blend(0, 1, store_theirs)
    blend(2, 0, store_own)

    lane2 = lax.broadcasted_iota(jnp.int32, (2, 128), 1)
    sub2 = lax.broadcasted_iota(jnp.int32, (2, 128), 0)
    start = (lax.rem(y, 2) * C + c) * OWN + m * 8
    line = jnp.full((2, 128), LOW, jnp.float32)
    for i in range(8):
        line = jnp.where((lane2 == start + i) & (sub2 == y // 2), train[i] + step[i], line)
    row0[...] = line

    pl.semaphore_wait(barrier, len(partners))

    for way, to in enumerate((z_at[2], z_at[Z - 2])):
        pl.semaphore_signal(known.at[way], inc=1, device_id=to, device_id_type=mesh_id)

    over_yc = []
    for d in (2, 1, 3):
        over_yc.append(remote(peak.at[1], peak_yc.at[2 * d], peak_send.at[0], yc_sem.at[0], yo_at[d]))
        over_yc.append(remote(peak.at[0], peak_yc.at[2 * d - 1], peak_send.at[0], yc_sem.at[0], y_at[d]))
    over_yc.append(remote(peak.at[1], peak_yc.at[0], peak_send.at[0], yc_sem.at[0], sibling))
    for copy in over_yc:
        copy.start()
    to_sibling = remote(theirs, x.at[pl.ds(own_row, OWN)], x_sem.at[0], x_sem.at[1], sibling)
    to_sibling.start()
    for d in (2, 1, 3):
        remote(row0, row_yc.at[2 * d], norm_send.at[0], norm_sem.at[0], yo_at[d]).start()
        remote(row0, row_yc.at[2 * d - 1], norm_send.at[0], norm_sem.at[0], y_at[d]).start()
    remote(row0, row_yc.at[0], norm_send.at[0], norm_sem.at[0], sibling).start()

    def arrived(ref, sem):
        pltpu.make_async_copy(ref, ref, sem).wait()

    def flag(*event):
        return recv_sem.at[flags[event]]

    def rows_of(piece):
        return own_row if PIECES[piece][2] == "own" else other_row

    def lanes_of(piece):
        first, last = PIECES[piece][3:]
        return pl.ds(128 * first, 128 * (last - first))

    def early(piece, link):
        at = (pl.ds(rows_of(piece), OWN), lanes_of(piece))
        return remote(
            x.at[at], raw.at[(LINKS.index(link), *at)], raw_send.at[0], flag(piece, *STEP[link]), link_to[link]
        )

    own_first = {}
    for link in LINKS:
        some = [PIECES[piece][2] for piece in EARLY[link[0]][0]] + ["other"]
        own_first[link] = some.index("other")
        for piece in EARLY[link[0]][0][: own_first[link]]:
            early(piece, link).start()
    to_sibling.wait_recv()
    for link in LINKS:
        for piece in EARLY[link[0]][0][own_first[link] :]:
            early(piece, link).start()

    arrived(peak_yc, yc_sem.at[0])
    best = peak[0]
    for d in range(C * Y - 1):
        best = jnp.maximum(best, peak_yc[d])
    peak1[...] = best

    for way in range(2):
        pl.semaphore_wait(known.at[way], 1)
    over_z = [remote(peak1, peak_z.at[d], peak_send.at[0], z_sem.at[0], z_at[d]) for d in range(1, Z)]
    for d in sorted(range(1, Z), key=lambda d: -min(d, Z - d)):
        over_z[d - 1].start()
    arrived(row_yc, norm_sem.at[0])
    line = row0[...]
    for d in range(C * Y - 1):
        line = jnp.maximum(line, row_yc[d])
    rows_z[z] = line
    for d in range(1, Z):
        remote(rows_z.at[z], rows_z.at[z], norm_send.at[1], norm_sem.at[1], z_at[d]).start()
    for link in LINKS:
        for piece in EARLY[link[0]][1]:
            early(piece, link).start()
    arrived(peak_z.at[pl.ds(1, Z - 1)], z_sem.at[0])
    for d in range(1, Z):
        best = jnp.maximum(best, peak_z[d])
    peak2[...] = best
    cols[c] = best

    def block_at(dz, dy):
        chip = lax.rem(z - dz + Z, Z) * Y + lax.rem(y - dy + Y, Y)
        return pl.multiple_of(chip * CHIP, CHIP)

    def scale(piece, source, base):
        for t in range(*PIECES[piece][3:]):
            lanes = slice(128 * t, 128 * t + 128)
            by = jnp.broadcast_to(peak2[t : t + 1, :], (16, 128))
            for r in range(OWN // 16):
                at = pl.multiple_of(rows_of(piece) + 16 * r, 16)
                value = source[pl.ds(at, 16), lanes] / by
                out[c, pl.ds(pl.multiple_of(base + at, 16), 16), lanes] = value.astype(jnp.bfloat16)

    def send_on(piece, dz, dy, base):
        ref = out.at[c, pl.ds(pl.multiple_of(base + rows_of(piece), OWN), OWN), lanes_of(piece)]
        for link, to_z, to_y in forwards(piece, dz, dy):
            if (dz, dy) == (0, 0) and is_early(piece, link):
                continue
            remote(ref, ref, send_sem.at[0], flag(piece, to_z, to_y), link_to[link]).start()

    def send_aside(base, rows=CHIP, lanes=pl.ds(0, COLS)):
        ref = out.at[c, pl.ds(base, rows), lanes]
        remote(ref, ref, side_send.at[0], side_recv.at[0], sibling).start()

    home = block_at(0, 0)

    def norm_beside():
        arrived(rows_z.at[pl.ds(0, Z - 1)], norm_sem.at[1])
        for d in (1, X - 1):
            remote(rows_z, rows_x.at[d], norm_send.at[2], norm_sem.at[2], m_at[d]).start()

    def norm_across():
        arrived(rows_x.at[pl.ds(0, 2)], norm_sem.at[2])
        remote(rows_x.at[1], rows_x.at[2], norm_send.at[2], norm_sem.at[3], m_at[1]).start()

    def norm_done():
        arrived(rows_x.at[2], norm_sem.at[3])
        for k in range(Z):
            line = rows_z[k]
            for d in range(1, X):
                line = jnp.maximum(line, rows_x[d, k])
            norm[k] = line

    def own_rest():
        for piece in range(len(PIECES)):
            if (piece, 0, 0) not in order:
                scale(piece, x, home)
        send_aside(home)
        remote(cols.at[c], cols.at[c], side_send.at[1], side_recv.at[1], sibling).start()

    n = len(order)
    aside = {n // 8: own_rest, n // 4: norm_beside, n // 2: norm_across, 3 * n // 4: norm_done}
    blocks = {}
    for k, (_, dz, dy) in enumerate(order):
        blocks.setdefault((dz % Z, dy % Y), []).append(k)
    blocks.pop((0, 0), None)
    pending = None
    for k, (piece, dz, dy) in enumerate(order):
        if k in aside:
            aside[k]()
        base = block_at(dz, dy)
        link = next((l for l in LINKS if STEP[l] == (dz, dy)), None)
        computed = (dz, dy) == (0, 0) or link is not None and is_early(piece, link)
        if (dz, dy) == (0, 0):
            scale(piece, x, base)
        elif computed:
            early(piece, link).wait_recv()
            scale(piece, raw.at[LINKS.index(link)], base)
        else:
            ref = out.at[c, pl.ds(pl.multiple_of(base + rows_of(piece), OWN), OWN), lanes_of(piece)]
            remote(ref, ref, send_sem.at[0], flag(piece, dz, dy), sibling).wait_recv()
        if pending:
            send_on(*pending)
        pending = (piece, dz, dy, base)
        if not computed:
            send_on(*pending)
            pending = None
        if (dz, dy) != (0, 0):
            last = blocks[dz % Z, dy % Y][-1]
            if last >= n - LATE:
                send_aside(pl.multiple_of(base + rows_of(piece), OWN), OWN, lanes_of(piece))
            elif last == k:
                send_aside(base)

    arrived(cols.at[0], side_send.at[1])
    arrived(cols.at[0], side_recv.at[1])
    to_sibling.wait_send()
    arrived(row_yc, norm_send.at[0])
    arrived(rows_z.at[pl.ds(0, Z - 1)], norm_send.at[1])
    arrived(rows_x.at[pl.ds(1, X - 1)], norm_send.at[2])
    arrived(theirs.at[:, pl.ds(0, 64 * (C * Y + Z - 2))], peak_send.at[0])
    wide = [last - first for _, _, _, first, last in PIECES]
    soon = [sum(is_early(piece, link) for link in LINKS) for piece in range(len(PIECES))]
    arrived(out.at[0, pl.ds(0, 16 * sum(a * b for a, b in zip(soon, wide))), pl.ds(0, 512)], raw_send.at[0])
    arrived(out.at[0, pl.ds(0, 2 * sum((Z * Y - 1 - a) * b for a, b in zip(soon, wide)))], send_sem.at[0])
    whole = out.at[0]
    arrived(whole, side_send.at[0])
    arrived(whole, side_recv.at[0])


def write_kernel(tiles, cols, norm, gate, up, col_gate, col_up, gain, narrow, sem):
    parts = 4
    rows = ROWS // parts
    copies = []
    for i, ref in enumerate((gate, up)):
        for k in range(parts):
            at = pl.ds(k * rows, rows)
            copies.append(pltpu.make_async_copy(tiles.at[i, at], ref.at[at], sem.at[i * parts + k]))
    copies.append(pltpu.make_async_copy(cols.at[0], col_gate, sem.at[2 * parts]))
    copies.append(pltpu.make_async_copy(cols.at[1], col_up, sem.at[2 * parts + 1]))
    for copy in copies:
        copy.start()
    narrow[...] = jnp.concatenate([norm[k] for k in range(Z)], axis=0).astype(jnp.bfloat16)
    copies.append(pltpu.make_async_copy(narrow, gain, sem.at[2 * parts + 2]))
    copies[-1].start()
    for copy in copies:
        copy.wait()


def local(one_gate, other_gate, one_up, other_up, mix_share, norm_train, norm_step):
    f32, bf16 = jnp.float32, jnp.bfloat16
    hbm_spec = pl.BlockSpec(memory_space=pltpu.HBM)
    vmem_spec = pl.BlockSpec(memory_space=pltpu.VMEM)
    dma = pltpu.SemaphoreType.DMA
    tiles, cols, norm = pl.pallas_call(
        gather_kernel,
        out_shape=(
            pltpu.VMEM((2, ROWS, COLS), bf16),
            pltpu.VMEM((2, TILES, 128), f32),
            pltpu.VMEM((Z, 2, 128), f32),
        ),
        in_specs=[hbm_spec] * 7,
        out_specs=(vmem_spec,) * 3,
        scratch_shapes=[
            pltpu.SMEM((OWN,), f32), pltpu.SMEM((8,), f32), pltpu.SMEM((8,), f32),
            pltpu.VMEM((4, OWN, COLS), f32),
            pltpu.VMEM((OWN, COLS), f32),
            pltpu.VMEM((CHIP, COLS), f32),
            pltpu.VMEM((len(LINKS), CHIP, COLS), f32),
            pltpu.VMEM((C, TILES, 128), f32),
            pltpu.VMEM((C * Y - 1, TILES, 128), f32),
            pltpu.VMEM((TILES, 128), f32),
            pltpu.VMEM((Z, TILES, 128), f32),
            pltpu.VMEM((TILES, 128), f32),
            pltpu.VMEM((2, 128), f32),
            pltpu.VMEM((C * Y - 1, 2, 128), f32),
            pltpu.VMEM((Z, 2, 128), f32),
            pltpu.VMEM((X, Z, 2, 128), f32),
            dma((5,)), dma((2,)), dma((1,)), dma((1,)), dma((1,)), dma((3,)), dma((4,)),
            dma((1,)), dma((1,)), dma((share_flags(plan()[0])[1],)), dma((2,)), dma((2,)),
            pltpu.SemaphoreType.REGULAR((2,)),
        ],
        compiler_params=pltpu.CompilerParams(
            collective_id=0, has_side_effects=True, vmem_limit_bytes=24 * 2**20
        ),
        name="gather",
    )(
        *(
            pltpu.with_memory_space_constraint(a, pltpu.HBM)
            for a in (mix_share, one_gate, other_gate, one_up, other_up, norm_train, norm_step)
        )
    )
    tiles, cols, norm = (pltpu.with_memory_space_constraint(a, pltpu.VMEM) for a in (tiles, cols, norm))
    gate, up, col_gate, col_up, gain = pl.pallas_call(
        write_kernel,
        out_shape=(
            jax.ShapeDtypeStruct((ROWS, COLS), bf16),
            jax.ShapeDtypeStruct((ROWS, COLS), bf16),
            jax.ShapeDtypeStruct((TILES, 128), f32),
            jax.ShapeDtypeStruct((TILES, 128), f32),
            jax.ShapeDtypeStruct((2 * Z, 128), bf16),
        ),
        in_specs=[vmem_spec] * 3,
        out_specs=(hbm_spec,) * 5,
        scratch_shapes=[pltpu.VMEM((2 * Z, 128), bf16), dma((11,))],
        compiler_params=pltpu.CompilerParams(vmem_limit_bytes=8 * 2**20),
        name="write",
    )(tiles, cols, norm)
    return gate, up, col_gate.reshape(COLS), col_up.reshape(COLS), gain.reshape(ROWS)


def solution(mesh):
    torus = Mesh(mesh.devices.reshape(Z, Y, C, X), SHARD_MODEL)
    return jax.shard_map(
        local,
        mesh=torus,
        in_specs=(
            P(SHARD, "model"), P(SHARD, "model"), P(SHARD, "model"), P(SHARD, "model"),
            P(SHARD), P(SHARD_MODEL), P(SHARD_MODEL),
        ),
        out_specs=(P(None, "model"), P(None, "model"), P("model"), P("model"), P()),
        check_vma=False,
    )
```

```python
import heapq

import jax
import jax.numpy as jnp
from jax import lax
from jax.experimental import pallas as pl
from jax.experimental.pallas import tpu as pltpu
from jax.sharding import Mesh
from jax.sharding import PartitionSpec as P

SHARD = ("shard_0", "shard_1", "shard_2")
SHARD_MODEL = ("shard_0", "shard_1", "shard_2", "model")

Z, Y, C, X = 8, 4, 2, 4
ROWS, COLS, OWN = 2048, 2048, 32
CHIP = C * OWN
TILES = COLS // 128
LOW = -3.0e38
LATE = 24

PIECES = (("A", 1, "own", 0, 6), ("B", 0, "own", 6, 16), ("A", 0, "other", 0, 7), ("B", 1, "other", 7, 16))
FIRST = (3, 1, 0, 2)
EARLY = {"y": ((0, 2, 3), ()), "z": ((1,), (3,))}
LINKS = ("y+", "y-", "z+", "z-")
STEP = {"y+": (0, 1), "y-": (0, -1), "z+": (1, 0), "z-": (-1, 0)}


def is_early(piece, link):
    return any(piece in some for some in EARLY[link[0]])


def reach(half, n):
    return (n // 2, n // 2 - 1) if half == 0 else (n // 2 - 1, n // 2)


def forwards(piece, dz, dy):
    kind, half = PIECES[piece][:2]
    zp, zm = reach(half, Z)
    yp, ym = reach(half, Y)
    along_z, along_y = [], []
    if 0 <= dz < zp:
        along_z.append(("z+", dz + 1, dy))
    if -zm < dz <= 0:
        along_z.append(("z-", dz - 1, dy))
    if 0 <= dy < yp:
        along_y.append(("y+", dz, dy + 1))
    if -ym < dy <= 0:
        along_y.append(("y-", dz, dy - 1))
    if kind == "A":
        return along_z + (along_y if dz == 0 else [])
    return (along_z if dy == 0 else []) + along_y


def plan(hop=2.0, turn=0.04, block=5.6, swap=1.6, first=0.8, over_y=4.2, letters=0.9, over_z=8.2, work=0.08):
    free = {link: first if link[0] == "y" else 0.0 for link in LINKS}
    queue, order, count = [], [], 0

    def put(piece, link, z, y, at, early=False):
        nonlocal count
        width = (PIECES[piece][4] - PIECES[piece][3]) / TILES / C
        free[link] = max(at, free[link]) + width * block * (2 if early else 1)
        count += 1
        rank = FIRST.index(piece) if early else len(PIECES)
        heapq.heappush(queue, (max(free[link] + hop, over_z), rank, count, piece, z, y))

    for k, begin in enumerate((0.0, over_y)):
        for link in LINKS:
            for piece in EARLY[link[0]][k]:
                put(piece, link, *STEP[link], max(begin, swap if PIECES[piece][2] == "other" else 0.0), True)
        if k == 0:
            for link in ("z+", "z-"):
                free[link] = max(free[link], over_y) + letters
    clock = over_z
    for piece in range(len(PIECES)):
        if not all(is_early(piece, link) for link in LINKS):
            heapq.heappush(queue, (over_z, FIRST.index(piece) - 100, 0, piece, 0, 0))
    while queue:
        at, _, _, piece, dz, dy = heapq.heappop(queue)
        clock = max(clock, at) + turn
        order.append((piece, dz, dy))
        links = [l for l in LINKS if STEP[l] == (dz, dy)]
        if (dz, dy) == (0, 0) or links and is_early(piece, links[0]):
            clock += work
        for link, to_z, to_y in forwards(piece, dz, dy):
            if (dz, dy) != (0, 0) or not is_early(piece, link):
                put(piece, link, to_z, to_y, clock)
        clock += turn
    return order, clock


def came_by(piece, dz, dy):
    along_z = dz != 0 and (PIECES[piece][0] == "A" or dy == 0)
    link = ("z" if along_z else "y") + ("+" if (dz if along_z else dy) > 0 else "-")
    return link, (piece, dz - STEP[link][0], dy - STEP[link][1])


def share_flags(order):
    at = {event: k for k, event in enumerate(order)}
    known = {link: [-1] * len(order) for link in LINKS}
    for k, event in enumerate(order):
        for link in LINKS:
            known[link][k] = known[link][k - 1] if k else -1
        if event[1:] != (0, 0):
            link, before = came_by(*event)
            if before[1:] != (0, 0) or not is_early(event[0], link):
                back = link[0] + ("-" if link[1] == "+" else "+")
                known[back][k] = max(known[back][k], at[before])
    flags, last = {}, []
    for k, event in enumerate(order):
        if event[1:] == (0, 0):
            continue
        link, before = came_by(*event)
        early = before[1:] == (0, 0) and is_early(event[0], link)
        free = [] if early else [i for i, used in enumerate(last) if used <= known[link][at[before]]]
        if free:
            i = min(free, key=lambda i: last[i])
            last[i] = k
        else:
            i = len(last)
            last.append(k)
        flags[event] = i
    return flags, len(last)


def gather_kernel(
    mix_h, one_g, other_g, one_u, other_u, train_h, step_h,
    out, cols, norm,
    mix, train, step, ins, theirs, x, raw, peak, peak_yc, peak1, peak_z, peak2,
    row0, row_yc, rows_z, rows_x,
    in_sem, x_sem, peak_send, yc_sem, z_sem, norm_send, norm_sem,
    raw_send, send_sem, recv_sem, side_send, side_recv, known,
):
    order, _ = plan()
    flags, _ = share_flags(order)
    z, y, c, m = (lax.axis_index(a) for a in SHARD_MODEL)
    mesh_id = pl.DeviceIdType.MESH
    z_at = [(lax.rem(z + d, Z), y, c, m) for d in range(Z)]
    y_at = [(z, lax.rem(y + d, Y), c, m) for d in range(Y)]
    yo_at = [(z, lax.rem(y + d, Y), 1 - c, m) for d in range(Y)]
    m_at = [(z, y, c, lax.rem(m + d, X)) for d in range(X)]
    sibling = yo_at[0]
    link_to = {"z+": z_at[1], "z-": z_at[Z - 1], "y+": y_at[1], "y-": y_at[Y - 1]}

    def remote(src, dst, send, recv, to):
        return pltpu.make_async_remote_copy(
            src_ref=src, dst_ref=dst, send_sem=send, recv_sem=recv, device_id=to, device_id_type=mesh_id
        )

    partners = [z_at[2], z_at[Z - 2], yo_at[2], y_at[2], *(z_at[d] for d in (1, Z - 1)), *(yo_at[d] for d in (1, 3))]
    partners += [y_at[1], y_at[3], sibling, m_at[1], m_at[X - 1]]
    barrier = pltpu.get_barrier_semaphore()
    for to in partners:
        pl.semaphore_signal(barrier, inc=1, device_id=to, device_id_type=mesh_id)

    small = [
        pltpu.make_async_copy(ref, to, in_sem.at[2 + i])
        for i, (ref, to) in enumerate(((mix_h, mix), (train_h, train), (step_h, step)))
    ]
    for copy in small:
        copy.start()
    for ours, pair in ((1 - c, (one_g, other_g)), (c, (one_u, other_u))):
        for k, ref in enumerate(pair):
            pltpu.make_async_copy(ref, ins.at[2 * ours + k], in_sem.at[ours]).start()
    for copy in small:
        copy.wait()

    sub = lax.broadcasted_iota(jnp.int32, (8, 128), 0)
    shares = []
    for r in range(OWN // 8):
        share = jnp.full((8, 128), mix[8 * r], jnp.float32)
        for i in range(1, 8):
            share = jnp.where(sub == i, mix[8 * r + i], share)
        shares.append((share, 1.0 - share))

    def blend(slot, to_peak, store):
        both = ins.at[pl.ds(slot, 2)]
        pltpu.make_async_copy(both, both, in_sem.at[slot // 2]).wait()
        for t in range(TILES):
            lanes = slice(128 * t, 128 * t + 128)
            best = None
            for r, (share, rest) in enumerate(shares):
                rows = slice(8 * r, 8 * r + 8)
                value = share * ins[slot, rows, lanes] + rest * ins[slot + 1, rows, lanes]
                store(r, lanes, value)
                best = jnp.abs(value) if best is None else jnp.maximum(best, jnp.abs(value))
            peak[to_peak, t : t + 1, :] = jnp.max(best, axis=0, keepdims=True)

    own_row, other_row = pl.multiple_of(OWN * c, OWN), pl.multiple_of(OWN * (1 - c), OWN)

    def store_theirs(r, lanes, value):
        theirs[8 * r : 8 * r + 8, lanes] = value

    def store_own(r, lanes, value):
        x[pl.ds(pl.multiple_of(own_row + 8 * r, 8), 8), lanes] = value

    blend(0, 1, store_theirs)
    blend(2, 0, store_own)

    lane2 = lax.broadcasted_iota(jnp.int32, (2, 128), 1)
    sub2 = lax.broadcasted_iota(jnp.int32, (2, 128), 0)
    start = (lax.rem(y, 2) * C + c) * OWN + m * 8
    line = jnp.full((2, 128), LOW, jnp.float32)
    for i in range(8):
        line = jnp.where((lane2 == start + i) & (sub2 == y // 2), train[i] + step[i], line)
    row0[...] = line

    pl.semaphore_wait(barrier, len(partners))

    for way, to in enumerate((z_at[2], z_at[Z - 2])):
        pl.semaphore_signal(known.at[way], inc=1, device_id=to, device_id_type=mesh_id)

    over_yc = []
    for d in (2, 1, 3):
        over_yc.append(remote(peak.at[1], peak_yc.at[2 * d], peak_send.at[0], yc_sem.at[0], yo_at[d]))
        over_yc.append(remote(peak.at[0], peak_yc.at[2 * d - 1], peak_send.at[0], yc_sem.at[0], y_at[d]))
    over_yc.append(remote(peak.at[1], peak_yc.at[0], peak_send.at[0], yc_sem.at[0], sibling))
    for copy in over_yc:
        copy.start()
    to_sibling = remote(theirs, x.at[pl.ds(own_row, OWN)], x_sem.at[0], x_sem.at[1], sibling)
    to_sibling.start()
    for d in (2, 1, 3):
        remote(row0, row_yc.at[2 * d], norm_send.at[0], norm_sem.at[0], yo_at[d]).start()
        remote(row0, row_yc.at[2 * d - 1], norm_send.at[0], norm_sem.at[0], y_at[d]).start()
    remote(row0, row_yc.at[0], norm_send.at[0], norm_sem.at[0], sibling).start()

    def arrived(ref, sem):
        pltpu.make_async_copy(ref, ref, sem).wait()

    def flag(*event):
        return recv_sem.at[flags[event]]

    def rows_of(piece):
        return own_row if PIECES[piece][2] == "own" else other_row

    def lanes_of(piece):
        first, last = PIECES[piece][3:]
        return pl.ds(128 * first, 128 * (last - first))

    def early(piece, link):
        at = (pl.ds(rows_of(piece), OWN), lanes_of(piece))
        return remote(
            x.at[at], raw.at[(LINKS.index(link), *at)], raw_send.at[0], flag(piece, *STEP[link]), link_to[link]
        )

    own_first = {}
    for link in LINKS:
        some = [PIECES[piece][2] for piece in EARLY[link[0]][0]] + ["other"]
        own_first[link] = some.index("other")
        for piece in EARLY[link[0]][0][: own_first[link]]:
            early(piece, link).start()
    to_sibling.wait_recv()
    for link in LINKS:
        for piece in EARLY[link[0]][0][own_first[link] :]:
            early(piece, link).start()

    arrived(peak_yc, yc_sem.at[0])
    best = peak[0]
    for d in range(C * Y - 1):
        best = jnp.maximum(best, peak_yc[d])
    peak1[...] = best

    for way in range(2):
        pl.semaphore_wait(known.at[way], 1)
    over_z = [remote(peak1, peak_z.at[d], peak_send.at[0], z_sem.at[0], z_at[d]) for d in range(1, Z)]
    for d in sorted(range(1, Z), key=lambda d: -min(d, Z - d)):
        over_z[d - 1].start()
    arrived(row_yc, norm_sem.at[0])
    line = row0[...]
    for d in range(C * Y - 1):
        line = jnp.maximum(line, row_yc[d])
    rows_z[z] = line
    for d in range(1, Z):
        remote(rows_z.at[z], rows_z.at[z], norm_send.at[1], norm_sem.at[1], z_at[d]).start()
    for link in LINKS:
        for piece in EARLY[link[0]][1]:
            early(piece, link).start()
    arrived(peak_z.at[pl.ds(1, Z - 1)], z_sem.at[0])
    for d in range(1, Z):
        best = jnp.maximum(best, peak_z[d])
    peak2[...] = best
    cols[c] = best

    def block_at(dz, dy):
        chip = lax.rem(z - dz + Z, Z) * Y + lax.rem(y - dy + Y, Y)
        return pl.multiple_of(chip * CHIP, CHIP)

    def scale(piece, source, base):
        for t in range(*PIECES[piece][3:]):
            lanes = slice(128 * t, 128 * t + 128)
            by = jnp.broadcast_to(peak2[t : t + 1, :], (16, 128))
            for r in range(OWN // 16):
                at = pl.multiple_of(rows_of(piece) + 16 * r, 16)
                value = source[pl.ds(at, 16), lanes] / by
                out[c, pl.ds(pl.multiple_of(base + at, 16), 16), lanes] = value.astype(jnp.bfloat16)

    def send_on(piece, dz, dy, base):
        ref = out.at[c, pl.ds(pl.multiple_of(base + rows_of(piece), OWN), OWN), lanes_of(piece)]
        for link, to_z, to_y in forwards(piece, dz, dy):
            if (dz, dy) == (0, 0) and is_early(piece, link):
                continue
            remote(ref, ref, send_sem.at[0], flag(piece, to_z, to_y), link_to[link]).start()

    def send_aside(base, rows=CHIP, lanes=pl.ds(0, COLS)):
        ref = out.at[c, pl.ds(base, rows), lanes]
        remote(ref, ref, side_send.at[0], side_recv.at[0], sibling).start()

    home = block_at(0, 0)

    def norm_beside():
        arrived(rows_z.at[pl.ds(0, Z - 1)], norm_sem.at[1])
        for d in (1, X - 1):
            remote(rows_z, rows_x.at[d], norm_send.at[2], norm_sem.at[2], m_at[d]).start()

    def norm_across():
        arrived(rows_x.at[pl.ds(0, 2)], norm_sem.at[2])
        remote(rows_x.at[1], rows_x.at[2], norm_send.at[2], norm_sem.at[3], m_at[1]).start()

    def norm_done():
        arrived(rows_x.at[2], norm_sem.at[3])
        for k in range(Z):
            line = rows_z[k]
            for d in range(1, X):
                line = jnp.maximum(line, rows_x[d, k])
            norm[k] = line

    def own_rest():
        for piece in range(len(PIECES)):
            if (piece, 0, 0) not in order:
                scale(piece, x, home)
        send_aside(home)
        remote(cols.at[c], cols.at[c], side_send.at[1], side_recv.at[1], sibling).start()

    n = len(order)
    aside = {n // 8: own_rest, n // 4: norm_beside, n // 2: norm_across, 3 * n // 4: norm_done}
    blocks = {}
    for k, (_, dz, dy) in enumerate(order):
        blocks.setdefault((dz % Z, dy % Y), []).append(k)
    blocks.pop((0, 0), None)
    pending = None
    for k, (piece, dz, dy) in enumerate(order):
        if k in aside:
            aside[k]()
        base = block_at(dz, dy)
        link = next((l for l in LINKS if STEP[l] == (dz, dy)), None)
        computed = (dz, dy) == (0, 0) or link is not None and is_early(piece, link)
        if (dz, dy) == (0, 0):
            scale(piece, x, base)
        elif computed:
            early(piece, link).wait_recv()
            scale(piece, raw.at[LINKS.index(link)], base)
        else:
            ref = out.at[c, pl.ds(pl.multiple_of(base + rows_of(piece), OWN), OWN), lanes_of(piece)]
            remote(ref, ref, send_sem.at[0], flag(piece, dz, dy), sibling).wait_recv()
        if pending:
            send_on(*pending)
        pending = (piece, dz, dy, base)
        if not computed:
            send_on(*pending)
            pending = None
        if (dz, dy) != (0, 0):
            last = blocks[dz % Z, dy % Y][-1]
            if last >= n - LATE:
                send_aside(pl.multiple_of(base + rows_of(piece), OWN), OWN, lanes_of(piece))
            elif last == k:
                send_aside(base)

    arrived(cols.at[0], side_send.at[1])
    arrived(cols.at[0], side_recv.at[1])
    to_sibling.wait_send()
    arrived(row_yc, norm_send.at[0])
    arrived(rows_z.at[pl.ds(0, Z - 1)], norm_send.at[1])
    arrived(rows_x.at[pl.ds(1, X - 1)], norm_send.at[2])
    arrived(theirs.at[:, pl.ds(0, 64 * (C * Y + Z - 2))], peak_send.at[0])
    wide = [last - first for _, _, _, first, last in PIECES]
    soon = [sum(is_early(piece, link) for link in LINKS) for piece in range(len(PIECES))]
    arrived(out.at[0, pl.ds(0, 16 * sum(a * b for a, b in zip(soon, wide))), pl.ds(0, 512)], raw_send.at[0])
    tiles = OWN // 8 * sum((Z * Y - 1 - a) * b for a, b in zip(soon, wide))
    across = max(w for w in range(1, TILES + 1) if tiles % w == 0)
    deep = 1 if tiles // across <= ROWS // 8 else 2
    arrived(out.at[pl.ds(0, deep), pl.ds(0, tiles // across // deep * 8), pl.ds(0, 128 * across)], send_sem.at[0])
    whole = out.at[0]
    arrived(whole, side_send.at[0])
    arrived(whole, side_recv.at[0])


def write_kernel(tiles, cols, norm, gate, up, col_gate, col_up, gain, narrow, sem):
    parts = 4
    rows = ROWS // parts
    copies = []
    for i, ref in enumerate((gate, up)):
        for k in range(parts):
            at = pl.ds(k * rows, rows)
            copies.append(pltpu.make_async_copy(tiles.at[i, at], ref.at[at], sem.at[i * parts + k]))
    copies.append(pltpu.make_async_copy(cols.at[0], col_gate, sem.at[2 * parts]))
    copies.append(pltpu.make_async_copy(cols.at[1], col_up, sem.at[2 * parts + 1]))
    for copy in copies:
        copy.start()
    narrow[...] = jnp.concatenate([norm[k] for k in range(Z)], axis=0).astype(jnp.bfloat16)
    copies.append(pltpu.make_async_copy(narrow, gain, sem.at[2 * parts + 2]))
    copies[-1].start()
    for copy in copies:
        copy.wait()


def local(one_gate, other_gate, one_up, other_up, mix_share, norm_train, norm_step):
    f32, bf16 = jnp.float32, jnp.bfloat16
    hbm_spec = pl.BlockSpec(memory_space=pltpu.HBM)
    vmem_spec = pl.BlockSpec(memory_space=pltpu.VMEM)
    dma = pltpu.SemaphoreType.DMA
    tiles, cols, norm = pl.pallas_call(
        gather_kernel,
        out_shape=(
            pltpu.VMEM((2, ROWS, COLS), bf16),
            pltpu.VMEM((2, TILES, 128), f32),
            pltpu.VMEM((Z, 2, 128), f32),
        ),
        in_specs=[hbm_spec] * 7,
        out_specs=(vmem_spec,) * 3,
        scratch_shapes=[
            pltpu.SMEM((OWN,), f32), pltpu.SMEM((8,), f32), pltpu.SMEM((8,), f32),
            pltpu.VMEM((4, OWN, COLS), f32),
            pltpu.VMEM((OWN, COLS), f32),
            pltpu.VMEM((CHIP, COLS), f32),
            pltpu.VMEM((len(LINKS), CHIP, COLS), f32),
            pltpu.VMEM((C, TILES, 128), f32),
            pltpu.VMEM((C * Y - 1, TILES, 128), f32),
            pltpu.VMEM((TILES, 128), f32),
            pltpu.VMEM((Z, TILES, 128), f32),
            pltpu.VMEM((TILES, 128), f32),
            pltpu.VMEM((2, 128), f32),
            pltpu.VMEM((C * Y - 1, 2, 128), f32),
            pltpu.VMEM((Z, 2, 128), f32),
            pltpu.VMEM((X, Z, 2, 128), f32),
            dma((5,)), dma((2,)), dma((1,)), dma((1,)), dma((1,)), dma((3,)), dma((4,)),
            dma((1,)), dma((1,)), dma((share_flags(plan()[0])[1],)), dma((2,)), dma((2,)),
            pltpu.SemaphoreType.REGULAR((2,)),
        ],
        compiler_params=pltpu.CompilerParams(
            collective_id=0, has_side_effects=True, vmem_limit_bytes=24 * 2**20
        ),
        name="gather",
    )(
        *(
            pltpu.with_memory_space_constraint(a, pltpu.HBM)
            for a in (mix_share, one_gate, other_gate, one_up, other_up, norm_train, norm_step)
        )
    )
    tiles, cols, norm = (pltpu.with_memory_space_constraint(a, pltpu.VMEM) for a in (tiles, cols, norm))
    gate, up, col_gate, col_up, gain = pl.pallas_call(
        write_kernel,
        out_shape=(
            jax.ShapeDtypeStruct((ROWS, COLS), bf16),
            jax.ShapeDtypeStruct((ROWS, COLS), bf16),
            jax.ShapeDtypeStruct((TILES, 128), f32),
            jax.ShapeDtypeStruct((TILES, 128), f32),
            jax.ShapeDtypeStruct((2 * Z, 128), bf16),
        ),
        in_specs=[vmem_spec] * 3,
        out_specs=(hbm_spec,) * 5,
        scratch_shapes=[pltpu.VMEM((2 * Z, 128), bf16), dma((11,))],
        compiler_params=pltpu.CompilerParams(vmem_limit_bytes=8 * 2**20),
        name="write",
    )(tiles, cols, norm)
    return gate, up, col_gate.reshape(COLS), col_up.reshape(COLS), gain.reshape(ROWS)


def solution(mesh):
    torus = Mesh(mesh.devices.reshape(Z, Y, C, X), SHARD_MODEL)
    return jax.shard_map(
        local,
        mesh=torus,
        in_specs=(
            P(SHARD, "model"), P(SHARD, "model"), P(SHARD, "model"), P(SHARD, "model"),
            P(SHARD), P(SHARD_MODEL), P(SHARD_MODEL),
        ),
        out_specs=(P(None, "model"), P(None, "model"), P("model"), P("model"), P()),
        check_vma=False,
    )
```

```python
import heapq

import jax
import jax.numpy as jnp
from jax import lax
from jax.experimental import pallas as pl
from jax.experimental.pallas import tpu as pltpu
from jax.sharding import Mesh
from jax.sharding import PartitionSpec as P

SHARD = ("shard_0", "shard_1", "shard_2")
SHARD_MODEL = ("shard_0", "shard_1", "shard_2", "model")

Z, Y, C, X = 8, 4, 2, 4
ROWS, COLS, OWN = 2048, 2048, 32
CHIP = C * OWN
TILES = COLS // 128
LOW = -3.0e38
LATE = 60

PIECES = (("A", 1, "own", 0, 6), ("B", 0, "own", 6, 16), ("A", 0, "other", 0, 7), ("B", 1, "other", 7, 16))
FIRST = (3, 1, 0, 2)
EARLY = {"y": ((0, 2, 3), ()), "z": ((1,), (3,))}
LINKS = ("y+", "y-", "z+", "z-")
STEP = {"y+": (0, 1), "y-": (0, -1), "z+": (1, 0), "z-": (-1, 0)}


def is_early(piece, link):
    return any(piece in some for some in EARLY[link[0]])


def reach(half, n):
    return (n // 2, n // 2 - 1) if half == 0 else (n // 2 - 1, n // 2)


def forwards(piece, dz, dy):
    kind, half = PIECES[piece][:2]
    zp, zm = reach(half, Z)
    yp, ym = reach(half, Y)
    along_z, along_y = [], []
    if 0 <= dz < zp:
        along_z.append(("z+", dz + 1, dy))
    if -zm < dz <= 0:
        along_z.append(("z-", dz - 1, dy))
    if 0 <= dy < yp:
        along_y.append(("y+", dz, dy + 1))
    if -ym < dy <= 0:
        along_y.append(("y-", dz, dy - 1))
    if kind == "A":
        return along_z + (along_y if dz == 0 else [])
    return (along_z if dy == 0 else []) + along_y


def plan(hop=2.0, turn=0.04, block=5.6, swap=1.6, first=0.8, over_y=4.2, letters=0.9, over_z=8.2, work=0.08):
    free = {link: first if link[0] == "y" else 0.0 for link in LINKS}
    queue, order, count = [], [], 0

    def put(piece, link, z, y, at, early=False):
        nonlocal count
        width = (PIECES[piece][4] - PIECES[piece][3]) / TILES / C
        free[link] = max(at, free[link]) + width * block * (2 if early else 1)
        count += 1
        rank = FIRST.index(piece) if early else len(PIECES)
        heapq.heappush(queue, (max(free[link] + hop, over_z), rank, count, piece, z, y))

    for k, begin in enumerate((0.0, over_y)):
        for link in LINKS:
            for piece in EARLY[link[0]][k]:
                put(piece, link, *STEP[link], max(begin, swap if PIECES[piece][2] == "other" else 0.0), True)
        if k == 0:
            for link in ("z+", "z-"):
                free[link] = max(free[link], over_y) + letters
    clock = over_z
    for piece in range(len(PIECES)):
        if not all(is_early(piece, link) for link in LINKS):
            heapq.heappush(queue, (over_z, FIRST.index(piece) - 100, 0, piece, 0, 0))
    while queue:
        at, _, _, piece, dz, dy = heapq.heappop(queue)
        clock = max(clock, at) + turn
        order.append((piece, dz, dy))
        links = [l for l in LINKS if STEP[l] == (dz, dy)]
        if (dz, dy) == (0, 0) or links and is_early(piece, links[0]):
            clock += work
        for link, to_z, to_y in forwards(piece, dz, dy):
            if (dz, dy) != (0, 0) or not is_early(piece, link):
                put(piece, link, to_z, to_y, clock)
        clock += turn
    return order, clock


def came_by(piece, dz, dy):
    along_z = dz != 0 and (PIECES[piece][0] == "A" or dy == 0)
    link = ("z" if along_z else "y") + ("+" if (dz if along_z else dy) > 0 else "-")
    return link, (piece, dz - STEP[link][0], dy - STEP[link][1])


def share_flags(order):
    at = {event: k for k, event in enumerate(order)}
    known = {link: [-1] * len(order) for link in LINKS}
    for k, event in enumerate(order):
        for link in LINKS:
            known[link][k] = known[link][k - 1] if k else -1
        if event[1:] != (0, 0):
            link, before = came_by(*event)
            if before[1:] != (0, 0) or not is_early(event[0], link):
                back = link[0] + ("-" if link[1] == "+" else "+")
                known[back][k] = max(known[back][k], at[before])
    flags, last = {}, []
    for k, event in enumerate(order):
        if event[1:] == (0, 0):
            continue
        link, before = came_by(*event)
        early = before[1:] == (0, 0) and is_early(event[0], link)
        free = [] if early else [i for i, used in enumerate(last) if used <= known[link][at[before]]]
        if free:
            i = min(free, key=lambda i: last[i])
            last[i] = k
        else:
            i = len(last)
            last.append(k)
        flags[event] = i
    return flags, len(last)


def gather_kernel(
    mix_h, one_g, other_g, one_u, other_u, train_h, step_h,
    out, cols, norm,
    mix, train, step, ins, theirs, x, raw, peak, peak_yc, peak1, peak_z, peak2,
    row0, row_yc, rows_z, rows_x,
    in_sem, x_sem, peak_send, yc_sem, z_sem, norm_send, norm_sem,
    raw_send, send_sem, recv_sem, side_send, side_recv, known,
):
    order, _ = plan()
    flags, _ = share_flags(order)
    z, y, c, m = (lax.axis_index(a) for a in SHARD_MODEL)
    mesh_id = pl.DeviceIdType.MESH
    z_at = [(lax.rem(z + d, Z), y, c, m) for d in range(Z)]
    y_at = [(z, lax.rem(y + d, Y), c, m) for d in range(Y)]
    yo_at = [(z, lax.rem(y + d, Y), 1 - c, m) for d in range(Y)]
    m_at = [(z, y, c, lax.rem(m + d, X)) for d in range(X)]
    sibling = yo_at[0]
    link_to = {"z+": z_at[1], "z-": z_at[Z - 1], "y+": y_at[1], "y-": y_at[Y - 1]}

    def remote(src, dst, send, recv, to):
        return pltpu.make_async_remote_copy(
            src_ref=src, dst_ref=dst, send_sem=send, recv_sem=recv, device_id=to, device_id_type=mesh_id
        )

    partners = [z_at[2], z_at[Z - 2], yo_at[2], y_at[2], *(z_at[d] for d in (1, Z - 1)), *(yo_at[d] for d in (1, 3))]
    partners += [y_at[1], y_at[3], sibling, m_at[1], m_at[X - 1]]
    barrier = pltpu.get_barrier_semaphore()
    for to in partners:
        pl.semaphore_signal(barrier, inc=1, device_id=to, device_id_type=mesh_id)

    small = [
        pltpu.make_async_copy(ref, to, in_sem.at[2 + i])
        for i, (ref, to) in enumerate(((mix_h, mix), (train_h, train), (step_h, step)))
    ]
    for copy in small:
        copy.start()
    for ours, pair in ((1 - c, (one_g, other_g)), (c, (one_u, other_u))):
        for k, ref in enumerate(pair):
            pltpu.make_async_copy(ref, ins.at[2 * ours + k], in_sem.at[ours]).start()
    for copy in small:
        copy.wait()

    sub = lax.broadcasted_iota(jnp.int32, (8, 128), 0)
    shares = []
    for r in range(OWN // 8):
        share = jnp.full((8, 128), mix[8 * r], jnp.float32)
        for i in range(1, 8):
            share = jnp.where(sub == i, mix[8 * r + i], share)
        shares.append((share, 1.0 - share))

    def blend(slot, to_peak, store):
        both = ins.at[pl.ds(slot, 2)]
        pltpu.make_async_copy(both, both, in_sem.at[slot // 2]).wait()
        for t in range(TILES):
            lanes = slice(128 * t, 128 * t + 128)
            best = None
            for r, (share, rest) in enumerate(shares):
                rows = slice(8 * r, 8 * r + 8)
                value = share * ins[slot, rows, lanes] + rest * ins[slot + 1, rows, lanes]
                store(r, lanes, value)
                best = jnp.abs(value) if best is None else jnp.maximum(best, jnp.abs(value))
            peak[to_peak, t : t + 1, :] = jnp.max(best, axis=0, keepdims=True)

    own_row, other_row = pl.multiple_of(OWN * c, OWN), pl.multiple_of(OWN * (1 - c), OWN)

    def store_theirs(r, lanes, value):
        theirs[8 * r : 8 * r + 8, lanes] = value

    def store_own(r, lanes, value):
        x[pl.ds(pl.multiple_of(own_row + 8 * r, 8), 8), lanes] = value

    blend(0, 1, store_theirs)
    blend(2, 0, store_own)

    lane2 = lax.broadcasted_iota(jnp.int32, (2, 128), 1)
    sub2 = lax.broadcasted_iota(jnp.int32, (2, 128), 0)
    start = (lax.rem(y, 2) * C + c) * OWN + m * 8
    line = jnp.full((2, 128), LOW, jnp.float32)
    for i in range(8):
        line = jnp.where((lane2 == start + i) & (sub2 == y // 2), train[i] + step[i], line)
    row0[...] = line

    pl.semaphore_wait(barrier, len(partners))

    for way, to in enumerate((z_at[2], z_at[Z - 2])):
        pl.semaphore_signal(known.at[way], inc=1, device_id=to, device_id_type=mesh_id)

    over_yc = []
    for d in (2, 1, 3):
        over_yc.append(remote(peak.at[1], peak_yc.at[2 * d], peak_send.at[0], yc_sem.at[0], yo_at[d]))
        over_yc.append(remote(peak.at[0], peak_yc.at[2 * d - 1], peak_send.at[0], yc_sem.at[0], y_at[d]))
    over_yc.append(remote(peak.at[1], peak_yc.at[0], peak_send.at[0], yc_sem.at[0], sibling))
    for copy in over_yc:
        copy.start()
    to_sibling = remote(theirs, x.at[pl.ds(own_row, OWN)], x_sem.at[0], x_sem.at[1], sibling)
    to_sibling.start()
    for d in (2, 1, 3):
        remote(row0, row_yc.at[2 * d], norm_send.at[0], norm_sem.at[0], yo_at[d]).start()
        remote(row0, row_yc.at[2 * d - 1], norm_send.at[0], norm_sem.at[0], y_at[d]).start()
    remote(row0, row_yc.at[0], norm_send.at[0], norm_sem.at[0], sibling).start()

    def arrived(ref, sem):
        pltpu.make_async_copy(ref, ref, sem).wait()

    def flag(*event):
        return recv_sem.at[flags[event]]

    def rows_of(piece):
        return own_row if PIECES[piece][2] == "own" else other_row

    def lanes_of(piece):
        first, last = PIECES[piece][3:]
        return pl.ds(128 * first, 128 * (last - first))

    def early(piece, link):
        at = (pl.ds(rows_of(piece), OWN), lanes_of(piece))
        return remote(
            x.at[at], raw.at[(LINKS.index(link), *at)], raw_send.at[0], flag(piece, *STEP[link]), link_to[link]
        )

    own_first = {}
    for link in LINKS:
        some = [PIECES[piece][2] for piece in EARLY[link[0]][0]] + ["other"]
        own_first[link] = some.index("other")
        for piece in EARLY[link[0]][0][: own_first[link]]:
            early(piece, link).start()
    to_sibling.wait_recv()
    for link in LINKS:
        for piece in EARLY[link[0]][0][own_first[link] :]:
            early(piece, link).start()

    arrived(peak_yc, yc_sem.at[0])
    best = peak[0]
    for d in range(C * Y - 1):
        best = jnp.maximum(best, peak_yc[d])
    peak1[...] = best

    for way in range(2):
        pl.semaphore_wait(known.at[way], 1)
    over_z = [remote(peak1, peak_z.at[d], peak_send.at[0], z_sem.at[0], z_at[d]) for d in range(1, Z)]
    for d in sorted(range(1, Z), key=lambda d: -min(d, Z - d)):
        over_z[d - 1].start()
    arrived(row_yc, norm_sem.at[0])
    line = row0[...]
    for d in range(C * Y - 1):
        line = jnp.maximum(line, row_yc[d])
    rows_z[z] = line
    for link in LINKS:
        for piece in EARLY[link[0]][1]:
            early(piece, link).start()
    for d in range(1, Z):
        remote(rows_z.at[z], rows_z.at[z], norm_send.at[1], norm_sem.at[1], z_at[d]).start()
    arrived(peak_z.at[pl.ds(1, Z - 1)], z_sem.at[0])
    for d in range(1, Z):
        best = jnp.maximum(best, peak_z[d])
    peak2[...] = best
    cols[c] = best

    def block_at(dz, dy):
        chip = lax.rem(z - dz + Z, Z) * Y + lax.rem(y - dy + Y, Y)
        return pl.multiple_of(chip * CHIP, CHIP)

    def scale(piece, source, base):
        for t in range(*PIECES[piece][3:]):
            lanes = slice(128 * t, 128 * t + 128)
            by = jnp.broadcast_to(peak2[t : t + 1, :], (16, 128))
            for r in range(OWN // 16):
                at = pl.multiple_of(rows_of(piece) + 16 * r, 16)
                value = source[pl.ds(at, 16), lanes] / by
                out[c, pl.ds(pl.multiple_of(base + at, 16), 16), lanes] = value.astype(jnp.bfloat16)

    def send_on(piece, dz, dy, base):
        ref = out.at[c, pl.ds(pl.multiple_of(base + rows_of(piece), OWN), OWN), lanes_of(piece)]
        for link, to_z, to_y in forwards(piece, dz, dy):
            if (dz, dy) == (0, 0) and is_early(piece, link):
                continue
            remote(ref, ref, send_sem.at[0], flag(piece, to_z, to_y), link_to[link]).start()

    def send_aside(base, rows=CHIP, lanes=pl.ds(0, COLS)):
        ref = out.at[c, pl.ds(base, rows), lanes]
        remote(ref, ref, side_send.at[0], side_recv.at[0], sibling).start()

    home = block_at(0, 0)

    def norm_beside():
        arrived(rows_z.at[pl.ds(0, Z - 1)], norm_sem.at[1])
        for d in (1, X - 1):
            remote(rows_z, rows_x.at[d], norm_send.at[2], norm_sem.at[2], m_at[d]).start()

    def norm_across():
        arrived(rows_x.at[pl.ds(0, 2)], norm_sem.at[2])
        remote(rows_x.at[1], rows_x.at[2], norm_send.at[2], norm_sem.at[3], m_at[1]).start()

    def norm_done():
        arrived(rows_x.at[2], norm_sem.at[3])
        for k in range(Z):
            line = rows_z[k]
            for d in range(1, X):
                line = jnp.maximum(line, rows_x[d, k])
            norm[k] = line

    def own_rest():
        for piece in range(len(PIECES)):
            if (piece, 0, 0) not in order:
                scale(piece, x, home)

    def own_aside():
        send_aside(home)
        remote(cols.at[c], cols.at[c], side_send.at[1], side_recv.at[1], sibling).start()

    n = len(order)
    aside = {n // 8: own_rest, n // 8 + 2: own_aside, n // 4: norm_beside, n // 2: norm_across, 3 * n // 4: norm_done}
    blocks = {}
    for k, (_, dz, dy) in enumerate(order):
        blocks.setdefault((dz % Z, dy % Y), []).append(k)
    blocks.pop((0, 0), None)
    pending = None
    for k, (piece, dz, dy) in enumerate(order):
        if k in aside:
            aside[k]()
        base = block_at(dz, dy)
        link = next((l for l in LINKS if STEP[l] == (dz, dy)), None)
        computed = (dz, dy) == (0, 0) or link is not None and is_early(piece, link)
        if (dz, dy) == (0, 0):
            scale(piece, x, base)
        elif computed:
            early(piece, link).wait_recv()
            scale(piece, raw.at[LINKS.index(link)], base)
        else:
            ref = out.at[c, pl.ds(pl.multiple_of(base + rows_of(piece), OWN), OWN), lanes_of(piece)]
            remote(ref, ref, send_sem.at[0], flag(piece, dz, dy), sibling).wait_recv()
        if pending:
            send_on(*pending)
        pending = (piece, dz, dy, base)
        if not computed:
            send_on(*pending)
            pending = None
        if (dz, dy) != (0, 0):
            last = blocks[dz % Z, dy % Y][-1]
            if last >= n - LATE:
                send_aside(pl.multiple_of(base + rows_of(piece), OWN), OWN, lanes_of(piece))
            elif last == k:
                send_aside(base)

    arrived(cols.at[0], side_send.at[1])
    arrived(cols.at[0], side_recv.at[1])
    to_sibling.wait_send()
    arrived(row_yc, norm_send.at[0])
    arrived(rows_z.at[pl.ds(0, Z - 1)], norm_send.at[1])
    arrived(rows_x.at[pl.ds(1, X - 1)], norm_send.at[2])
    arrived(theirs.at[:, pl.ds(0, 64 * (C * Y + Z - 2))], peak_send.at[0])
    wide = [last - first for _, _, _, first, last in PIECES]
    soon = [sum(is_early(piece, link) for link in LINKS) for piece in range(len(PIECES))]
    arrived(out.at[0, pl.ds(0, 16 * sum(a * b for a, b in zip(soon, wide))), pl.ds(0, 512)], raw_send.at[0])
    tiles = OWN // 8 * sum((Z * Y - 1 - a) * b for a, b in zip(soon, wide))
    across = max(w for w in range(1, TILES + 1) if tiles % w == 0)
    deep = 1 if tiles // across <= ROWS // 8 else 2
    assert tiles % (across * deep) == 0
    arrived(out.at[pl.ds(0, deep), pl.ds(0, tiles // across // deep * 8), pl.ds(0, 128 * across)], send_sem.at[0])
    whole = out.at[0]
    arrived(whole, side_send.at[0])
    arrived(whole, side_recv.at[0])


def write_kernel(tiles, cols, norm, gate, up, col_gate, col_up, gain, narrow, sem):
    parts = 4
    rows = ROWS // parts
    copies = []
    for i, ref in enumerate((gate, up)):
        for k in range(parts):
            at = pl.ds(k * rows, rows)
            copies.append(pltpu.make_async_copy(tiles.at[i, at], ref.at[at], sem.at[i * parts + k]))
    copies.append(pltpu.make_async_copy(cols.at[0], col_gate, sem.at[2 * parts]))
    copies.append(pltpu.make_async_copy(cols.at[1], col_up, sem.at[2 * parts + 1]))
    for copy in copies:
        copy.start()
    narrow[...] = jnp.concatenate([norm[k] for k in range(Z)], axis=0).astype(jnp.bfloat16)
    copies.append(pltpu.make_async_copy(narrow, gain, sem.at[2 * parts + 2]))
    copies[-1].start()
    for copy in copies:
        copy.wait()


def local(one_gate, other_gate, one_up, other_up, mix_share, norm_train, norm_step):
    f32, bf16 = jnp.float32, jnp.bfloat16
    hbm_spec = pl.BlockSpec(memory_space=pltpu.HBM)
    vmem_spec = pl.BlockSpec(memory_space=pltpu.VMEM)
    dma = pltpu.SemaphoreType.DMA
    tiles, cols, norm = pl.pallas_call(
        gather_kernel,
        out_shape=(
            pltpu.VMEM((2, ROWS, COLS), bf16),
            pltpu.VMEM((2, TILES, 128), f32),
            pltpu.VMEM((Z, 2, 128), f32),
        ),
        in_specs=[hbm_spec] * 7,
        out_specs=(vmem_spec,) * 3,
        scratch_shapes=[
            pltpu.SMEM((OWN,), f32), pltpu.SMEM((8,), f32), pltpu.SMEM((8,), f32),
            pltpu.VMEM((4, OWN, COLS), f32),
            pltpu.VMEM((OWN, COLS), f32),
            pltpu.VMEM((CHIP, COLS), f32),
            pltpu.VMEM((len(LINKS), CHIP, COLS), f32),
            pltpu.VMEM((C, TILES, 128), f32),
            pltpu.VMEM((C * Y - 1, TILES, 128), f32),
            pltpu.VMEM((TILES, 128), f32),
            pltpu.VMEM((Z, TILES, 128), f32),
            pltpu.VMEM((TILES, 128), f32),
            pltpu.VMEM((2, 128), f32),
            pltpu.VMEM((C * Y - 1, 2, 128), f32),
            pltpu.VMEM((Z, 2, 128), f32),
            pltpu.VMEM((X, Z, 2, 128), f32),
            dma((5,)), dma((2,)), dma((1,)), dma((1,)), dma((1,)), dma((3,)), dma((4,)),
            dma((1,)), dma((1,)), dma((share_flags(plan()[0])[1],)), dma((2,)), dma((2,)),
            pltpu.SemaphoreType.REGULAR((2,)),
        ],
        compiler_params=pltpu.CompilerParams(
            collective_id=0, has_side_effects=True, vmem_limit_bytes=24 * 2**20
        ),
        name="gather",
    )(
        *(
            pltpu.with_memory_space_constraint(a, pltpu.HBM)
            for a in (mix_share, one_gate, other_gate, one_up, other_up, norm_train, norm_step)
        )
    )
    tiles, cols, norm = (pltpu.with_memory_space_constraint(a, pltpu.VMEM) for a in (tiles, cols, norm))
    gate, up, col_gate, col_up, gain = pl.pallas_call(
        write_kernel,
        out_shape=(
            jax.ShapeDtypeStruct((ROWS, COLS), bf16),
            jax.ShapeDtypeStruct((ROWS, COLS), bf16),
            jax.ShapeDtypeStruct((TILES, 128), f32),
            jax.ShapeDtypeStruct((TILES, 128), f32),
            jax.ShapeDtypeStruct((2 * Z, 128), bf16),
        ),
        in_specs=[vmem_spec] * 3,
        out_specs=(hbm_spec,) * 5,
        scratch_shapes=[pltpu.VMEM((2 * Z, 128), bf16), dma((11,))],
        compiler_params=pltpu.CompilerParams(vmem_limit_bytes=8 * 2**20),
        name="write",
    )(tiles, cols, norm)
    return gate, up, col_gate.reshape(COLS), col_up.reshape(COLS), gain.reshape(ROWS)


def solution(mesh):
    torus = Mesh(mesh.devices.reshape(Z, Y, C, X), SHARD_MODEL)
    return jax.shard_map(
        local,
        mesh=torus,
        in_specs=(
            P(SHARD, "model"), P(SHARD, "model"), P(SHARD, "model"), P(SHARD, "model"),
            P(SHARD), P(SHARD_MODEL), P(SHARD_MODEL),
        ),
        out_specs=(P(None, "model"), P(None, "model"), P("model"), P("model"), P()),
        check_vma=False,
    )
```

```python
import heapq

import jax
import jax.numpy as jnp
from jax import lax
from jax.experimental import pallas as pl
from jax.experimental.pallas import tpu as pltpu
from jax.sharding import Mesh
from jax.sharding import PartitionSpec as P

SHARD = ("shard_0", "shard_1", "shard_2")
SHARD_MODEL = ("shard_0", "shard_1", "shard_2", "model")

Z, Y, C, X = 8, 4, 2, 4
ROWS, COLS, OWN = 2048, 2048, 32
CHIP = C * OWN
TILES = COLS // 128
LOW = -3.0e38
LATE = 60

PIECES = (("A", 1, "own", 0, 6), ("B", 0, "own", 6, 16), ("A", 0, "other", 0, 7), ("B", 1, "other", 7, 16))
FIRST = (3, 1, 0, 2)
EARLY = {"y": ((0, 2, 3), ()), "z": ((1,), (3,))}
LINKS = ("y+", "y-", "z+", "z-")
STEP = {"y+": (0, 1), "y-": (0, -1), "z+": (1, 0), "z-": (-1, 0)}


def is_early(piece, link):
    return any(piece in some for some in EARLY[link[0]])


def reach(half, n):
    return (n // 2, n // 2 - 1) if half == 0 else (n // 2 - 1, n // 2)


def forwards(piece, dz, dy):
    kind, half = PIECES[piece][:2]
    zp, zm = reach(half, Z)
    yp, ym = reach(half, Y)
    along_z, along_y = [], []
    if 0 <= dz < zp:
        along_z.append(("z+", dz + 1, dy))
    if -zm < dz <= 0:
        along_z.append(("z-", dz - 1, dy))
    if 0 <= dy < yp:
        along_y.append(("y+", dz, dy + 1))
    if -ym < dy <= 0:
        along_y.append(("y-", dz, dy - 1))
    if kind == "A":
        return along_z + (along_y if dz == 0 else [])
    return (along_z if dy == 0 else []) + along_y


def plan(hop=2.0, turn=0.04, block=5.6, swap=1.6, first=0.8, over_y=4.2, letters=0.9, over_z=8.2, work=0.08):
    free = {link: first if link[0] == "y" else 0.0 for link in LINKS}
    queue, order, count = [], [], 0

    def put(piece, link, z, y, at, early=False):
        nonlocal count
        width = (PIECES[piece][4] - PIECES[piece][3]) / TILES / C
        free[link] = max(at, free[link]) + width * block * (2 if early else 1)
        count += 1
        rank = FIRST.index(piece) if early else len(PIECES)
        heapq.heappush(queue, (max(free[link] + hop, over_z), rank, count, piece, z, y))

    for k, begin in enumerate((0.0, over_y)):
        for link in LINKS:
            for piece in EARLY[link[0]][k]:
                put(piece, link, *STEP[link], max(begin, swap if PIECES[piece][2] == "other" else 0.0), True)
        if k == 0:
            for link in ("z+", "z-"):
                free[link] = max(free[link], over_y) + letters
    clock = over_z
    for piece in range(len(PIECES)):
        if not all(is_early(piece, link) for link in LINKS):
            heapq.heappush(queue, (over_z, FIRST.index(piece) - 100, 0, piece, 0, 0))
    while queue:
        at, _, _, piece, dz, dy = heapq.heappop(queue)
        clock = max(clock, at) + turn
        order.append((piece, dz, dy))
        links = [l for l in LINKS if STEP[l] == (dz, dy)]
        if (dz, dy) == (0, 0) or links and is_early(piece, links[0]):
            clock += work
        for link, to_z, to_y in forwards(piece, dz, dy):
            if (dz, dy) != (0, 0) or not is_early(piece, link):
                put(piece, link, to_z, to_y, clock)
        clock += turn
    return order, clock


def came_by(piece, dz, dy):
    along_z = dz != 0 and (PIECES[piece][0] == "A" or dy == 0)
    link = ("z" if along_z else "y") + ("+" if (dz if along_z else dy) > 0 else "-")
    return link, (piece, dz - STEP[link][0], dy - STEP[link][1])


def share_flags(order):
    at = {event: k for k, event in enumerate(order)}
    known = {link: [-1] * len(order) for link in LINKS}
    for k, event in enumerate(order):
        for link in LINKS:
            known[link][k] = known[link][k - 1] if k else -1
        if event[1:] != (0, 0):
            link, before = came_by(*event)
            if before[1:] != (0, 0) or not is_early(event[0], link):
                back = link[0] + ("-" if link[1] == "+" else "+")
                known[back][k] = max(known[back][k], at[before])
    flags, last, twins = {}, [], {}
    for k, event in enumerate(order):
        if event[1:] == (0, 0) or event in flags:
            continue
        link, before = came_by(*event)
        early = before[1:] == (0, 0) and is_early(event[0], link)
        seen = -1 if early else known[link][at[before]]
        twin = order[k + 1] if k + 1 < len(order) else None
        if twin in ((event[0], -event[1], event[2]), (event[0], event[1], -event[2])):
            link2, before2 = came_by(*twin)
            if (before2[1:] == (0, 0) and is_early(twin[0], link2)) == early:
                twins[event] = twin
                if not early:
                    seen = min(seen, known[link2][at[before2]])
        free = [] if early else [i for i, used in enumerate(last) if used <= seen]
        if free:
            i = min(free, key=lambda i: last[i])
            last[i] = k
        else:
            i = len(last)
            last.append(k)
        flags[event] = i
        if event in twins:
            flags[twins[event]] = i
    return flags, len(last), twins


def gather_kernel(
    mix_h, one_g, other_g, one_u, other_u, train_h, step_h,
    out, cols, norm,
    mix, train, step, ins, theirs, x, raw, peak, peak_yc, peak1, peak_z, peak2,
    row0, row_yc, rows_z, rows_x,
    in_sem, x_sem, peak_send, yc_sem, z_sem, norm_send, norm_sem,
    raw_send, send_sem, recv_sem, side_send, side_recv, known,
):
    order, _ = plan()
    flags, _, twins = share_flags(order)
    waited = set(twins.values())
    z, y, c, m = (lax.axis_index(a) for a in SHARD_MODEL)
    mesh_id = pl.DeviceIdType.MESH
    z_at = [(lax.rem(z + d, Z), y, c, m) for d in range(Z)]
    y_at = [(z, lax.rem(y + d, Y), c, m) for d in range(Y)]
    yo_at = [(z, lax.rem(y + d, Y), 1 - c, m) for d in range(Y)]
    m_at = [(z, y, c, lax.rem(m + d, X)) for d in range(X)]
    sibling = yo_at[0]
    link_to = {"z+": z_at[1], "z-": z_at[Z - 1], "y+": y_at[1], "y-": y_at[Y - 1]}

    def remote(src, dst, send, recv, to):
        return pltpu.make_async_remote_copy(
            src_ref=src, dst_ref=dst, send_sem=send, recv_sem=recv, device_id=to, device_id_type=mesh_id
        )

    partners = [z_at[2], z_at[Z - 2], yo_at[2], y_at[2], *(z_at[d] for d in (1, Z - 1)), *(yo_at[d] for d in (1, 3))]
    partners += [y_at[1], y_at[3], sibling, m_at[1], m_at[X - 1]]
    barrier = pltpu.get_barrier_semaphore()
    for to in partners:
        pl.semaphore_signal(barrier, inc=1, device_id=to, device_id_type=mesh_id)

    small = [
        pltpu.make_async_copy(ref, to, in_sem.at[2 + i])
        for i, (ref, to) in enumerate(((mix_h, mix), (train_h, train), (step_h, step)))
    ]
    for copy in small:
        copy.start()
    for ours, pair in ((1 - c, (one_g, other_g)), (c, (one_u, other_u))):
        for k, ref in enumerate(pair):
            pltpu.make_async_copy(ref, ins.at[2 * ours + k], in_sem.at[ours]).start()
    for copy in small:
        copy.wait()

    sub = lax.broadcasted_iota(jnp.int32, (8, 128), 0)
    shares = []
    for r in range(OWN // 8):
        share = jnp.full((8, 128), mix[8 * r], jnp.float32)
        for i in range(1, 8):
            share = jnp.where(sub == i, mix[8 * r + i], share)
        shares.append((share, 1.0 - share))

    def blend(slot, to_peak, store):
        both = ins.at[pl.ds(slot, 2)]
        pltpu.make_async_copy(both, both, in_sem.at[slot // 2]).wait()
        for t in range(TILES):
            lanes = slice(128 * t, 128 * t + 128)
            best = None
            for r, (share, rest) in enumerate(shares):
                rows = slice(8 * r, 8 * r + 8)
                value = share * ins[slot, rows, lanes] + rest * ins[slot + 1, rows, lanes]
                store(r, lanes, value)
                best = jnp.abs(value) if best is None else jnp.maximum(best, jnp.abs(value))
            peak[to_peak, t : t + 1, :] = jnp.max(best, axis=0, keepdims=True)

    own_row, other_row = pl.multiple_of(OWN * c, OWN), pl.multiple_of(OWN * (1 - c), OWN)

    def store_theirs(r, lanes, value):
        theirs[8 * r : 8 * r + 8, lanes] = value

    def store_own(r, lanes, value):
        x[pl.ds(pl.multiple_of(own_row + 8 * r, 8), 8), lanes] = value

    blend(0, 1, store_theirs)
    blend(2, 0, store_own)

    lane2 = lax.broadcasted_iota(jnp.int32, (2, 128), 1)
    sub2 = lax.broadcasted_iota(jnp.int32, (2, 128), 0)
    start = (lax.rem(y, 2) * C + c) * OWN + m * 8
    line = jnp.full((2, 128), LOW, jnp.float32)
    for i in range(8):
        line = jnp.where((lane2 == start + i) & (sub2 == y // 2), train[i] + step[i], line)
    row0[...] = line

    pl.semaphore_wait(barrier, len(partners))

    for way, to in enumerate((z_at[2], z_at[Z - 2])):
        pl.semaphore_signal(known.at[way], inc=1, device_id=to, device_id_type=mesh_id)

    over_yc = []
    for d in (2, 1, 3):
        over_yc.append(remote(peak.at[1], peak_yc.at[2 * d], peak_send.at[0], yc_sem.at[0], yo_at[d]))
        over_yc.append(remote(peak.at[0], peak_yc.at[2 * d - 1], peak_send.at[0], yc_sem.at[0], y_at[d]))
    over_yc.append(remote(peak.at[1], peak_yc.at[0], peak_send.at[0], yc_sem.at[0], sibling))
    for copy in over_yc:
        copy.start()
    to_sibling = remote(theirs, x.at[pl.ds(own_row, OWN)], x_sem.at[0], x_sem.at[1], sibling)
    to_sibling.start()
    for d in (2, 1, 3):
        remote(row0, row_yc.at[2 * d], norm_send.at[0], norm_sem.at[0], yo_at[d]).start()
        remote(row0, row_yc.at[2 * d - 1], norm_send.at[0], norm_sem.at[0], y_at[d]).start()
    remote(row0, row_yc.at[0], norm_send.at[0], norm_sem.at[0], sibling).start()

    def arrived(ref, sem):
        pltpu.make_async_copy(ref, ref, sem).wait()

    def flag(*event):
        return recv_sem.at[flags[event]]

    def rows_of(piece):
        return own_row if PIECES[piece][2] == "own" else other_row

    def lanes_of(piece):
        first, last = PIECES[piece][3:]
        return pl.ds(128 * first, 128 * (last - first))

    def early(piece, link):
        at = (pl.ds(rows_of(piece), OWN), lanes_of(piece))
        return remote(
            x.at[at], raw.at[(LINKS.index(link), *at)], raw_send.at[0], flag(piece, *STEP[link]), link_to[link]
        )

    own_first = {}
    for link in LINKS:
        some = [PIECES[piece][2] for piece in EARLY[link[0]][0]] + ["other"]
        own_first[link] = some.index("other")
        for piece in EARLY[link[0]][0][: own_first[link]]:
            early(piece, link).start()
    to_sibling.wait_recv()
    for link in LINKS:
        for piece in EARLY[link[0]][0][own_first[link] :]:
            early(piece, link).start()

    arrived(peak_yc, yc_sem.at[0])
    best = peak[0]
    for d in range(C * Y - 1):
        best = jnp.maximum(best, peak_yc[d])
    peak1[...] = best

    for way in range(2):
        pl.semaphore_wait(known.at[way], 1)
    over_z = [remote(peak1, peak_z.at[d], peak_send.at[0], z_sem.at[0], z_at[d]) for d in range(1, Z)]
    for d in sorted(range(1, Z), key=lambda d: -min(d, Z - d)):
        over_z[d - 1].start()
    arrived(row_yc, norm_sem.at[0])
    line = row0[...]
    for d in range(C * Y - 1):
        line = jnp.maximum(line, row_yc[d])
    rows_z[z] = line
    for link in LINKS:
        for piece in EARLY[link[0]][1]:
            early(piece, link).start()
    for d in range(1, Z):
        remote(rows_z.at[z], rows_z.at[z], norm_send.at[1], norm_sem.at[1], z_at[d]).start()
    arrived(peak_z.at[pl.ds(1, Z - 1)], z_sem.at[0])
    for d in range(1, Z):
        best = jnp.maximum(best, peak_z[d])
    peak2[...] = best
    cols[c] = best

    def block_at(dz, dy):
        chip = lax.rem(z - dz + Z, Z) * Y + lax.rem(y - dy + Y, Y)
        return pl.multiple_of(chip * CHIP, CHIP)

    def scale(piece, source, base):
        for t in range(*PIECES[piece][3:]):
            lanes = slice(128 * t, 128 * t + 128)
            by = jnp.broadcast_to(peak2[t : t + 1, :], (16, 128))
            for r in range(OWN // 16):
                at = pl.multiple_of(rows_of(piece) + 16 * r, 16)
                value = source[pl.ds(at, 16), lanes] / by
                out[c, pl.ds(pl.multiple_of(base + at, 16), 16), lanes] = value.astype(jnp.bfloat16)

    def send_on(piece, dz, dy, base):
        ref = out.at[c, pl.ds(pl.multiple_of(base + rows_of(piece), OWN), OWN), lanes_of(piece)]
        for link, to_z, to_y in forwards(piece, dz, dy):
            if (dz, dy) == (0, 0) and is_early(piece, link):
                continue
            remote(ref, ref, send_sem.at[0], flag(piece, to_z, to_y), link_to[link]).start()

    def send_aside(base, rows=CHIP, lanes=pl.ds(0, COLS)):
        ref = out.at[c, pl.ds(base, rows), lanes]
        remote(ref, ref, side_send.at[0], side_recv.at[0], sibling).start()

    home = block_at(0, 0)

    def norm_beside():
        arrived(rows_z.at[pl.ds(0, Z - 1)], norm_sem.at[1])
        for d in (1, X - 1):
            remote(rows_z, rows_x.at[d], norm_send.at[2], norm_sem.at[2], m_at[d]).start()

    def norm_across():
        arrived(rows_x.at[pl.ds(0, 2)], norm_sem.at[2])
        remote(rows_x.at[1], rows_x.at[2], norm_send.at[2], norm_sem.at[3], m_at[1]).start()

    def norm_done():
        arrived(rows_x.at[2], norm_sem.at[3])
        for k in range(Z):
            line = rows_z[k]
            for d in range(1, X):
                line = jnp.maximum(line, rows_x[d, k])
            norm[k] = line

    def own_rest():
        for piece in range(len(PIECES)):
            if (piece, 0, 0) not in order:
                scale(piece, x, home)

    def own_aside():
        send_aside(home)
        remote(cols.at[c], cols.at[c], side_send.at[1], side_recv.at[1], sibling).start()

    n = len(order)
    aside = {n // 8: own_rest, n // 8 + 2: own_aside, n // 4: norm_beside, n // 2: norm_across, 3 * n // 4: norm_done}
    blocks = {}
    for k, (_, dz, dy) in enumerate(order):
        blocks.setdefault((dz % Z, dy % Y), []).append(k)
    blocks.pop((0, 0), None)
    pending = None
    for k, (piece, dz, dy) in enumerate(order):
        if k in aside:
            aside[k]()
        base = block_at(dz, dy)
        link = next((l for l in LINKS if STEP[l] == (dz, dy)), None)
        computed = (dz, dy) == (0, 0) or link is not None and is_early(piece, link)
        if (dz, dy) == (0, 0):
            scale(piece, x, base)
        elif computed:
            if (piece, dz, dy) not in waited:
                pair = 2 if (piece, dz, dy) in twins else 1
                arrived(ins.at[pl.ds(0, pair), :, lanes_of(piece)], flag(piece, dz, dy))
            scale(piece, raw.at[LINKS.index(link)], base)
        else:
            if (piece, dz, dy) not in waited:
                pair = 2 if (piece, dz, dy) in twins else 1
                arrived(out.at[0, pl.ds(0, pair * OWN), lanes_of(piece)], flag(piece, dz, dy))
        if pending:
            send_on(*pending)
        pending = (piece, dz, dy, base)
        if not computed:
            send_on(*pending)
            pending = None
        if (dz, dy) != (0, 0):
            last = blocks[dz % Z, dy % Y][-1]
            if last >= n - LATE:
                send_aside(pl.multiple_of(base + rows_of(piece), OWN), OWN, lanes_of(piece))
            elif last == k:
                send_aside(base)

    arrived(cols.at[0], side_send.at[1])
    arrived(cols.at[0], side_recv.at[1])
    to_sibling.wait_send()
    arrived(row_yc, norm_send.at[0])
    arrived(rows_z.at[pl.ds(0, Z - 1)], norm_send.at[1])
    arrived(rows_x.at[pl.ds(1, X - 1)], norm_send.at[2])
    arrived(theirs.at[:, pl.ds(0, 64 * (C * Y + Z - 2))], peak_send.at[0])
    wide = [last - first for _, _, _, first, last in PIECES]
    soon = [sum(is_early(piece, link) for link in LINKS) for piece in range(len(PIECES))]
    arrived(out.at[0, pl.ds(0, 16 * sum(a * b for a, b in zip(soon, wide))), pl.ds(0, 512)], raw_send.at[0])
    tiles = OWN // 8 * sum((Z * Y - 1 - a) * b for a, b in zip(soon, wide))
    across = max(w for w in range(1, TILES + 1) if tiles % w == 0)
    deep = 1 if tiles // across <= ROWS // 8 else 2
    assert tiles % (across * deep) == 0
    arrived(out.at[pl.ds(0, deep), pl.ds(0, tiles // across // deep * 8), pl.ds(0, 128 * across)], send_sem.at[0])
    whole = out.at[0]
    arrived(whole, side_send.at[0])
    arrived(whole, side_recv.at[0])


def write_kernel(tiles, cols, norm, gate, up, col_gate, col_up, gain, narrow, sem):
    parts = 4
    rows = ROWS // parts
    copies = []
    for i, ref in enumerate((gate, up)):
        for k in range(parts):
            at = pl.ds(k * rows, rows)
            copies.append(pltpu.make_async_copy(tiles.at[i, at], ref.at[at], sem.at[i * parts + k]))
    copies.append(pltpu.make_async_copy(cols.at[0], col_gate, sem.at[2 * parts]))
    copies.append(pltpu.make_async_copy(cols.at[1], col_up, sem.at[2 * parts + 1]))
    for copy in copies:
        copy.start()
    narrow[...] = jnp.concatenate([norm[k] for k in range(Z)], axis=0).astype(jnp.bfloat16)
    copies.append(pltpu.make_async_copy(narrow, gain, sem.at[2 * parts + 2]))
    copies[-1].start()
    for copy in copies:
        copy.wait()


def local(one_gate, other_gate, one_up, other_up, mix_share, norm_train, norm_step):
    f32, bf16 = jnp.float32, jnp.bfloat16
    hbm_spec = pl.BlockSpec(memory_space=pltpu.HBM)
    vmem_spec = pl.BlockSpec(memory_space=pltpu.VMEM)
    dma = pltpu.SemaphoreType.DMA
    tiles, cols, norm = pl.pallas_call(
        gather_kernel,
        out_shape=(
            pltpu.VMEM((2, ROWS, COLS), bf16),
            pltpu.VMEM((2, TILES, 128), f32),
            pltpu.VMEM((Z, 2, 128), f32),
        ),
        in_specs=[hbm_spec] * 7,
        out_specs=(vmem_spec,) * 3,
        scratch_shapes=[
            pltpu.SMEM((OWN,), f32), pltpu.SMEM((8,), f32), pltpu.SMEM((8,), f32),
            pltpu.VMEM((4, OWN, COLS), f32),
            pltpu.VMEM((OWN, COLS), f32),
            pltpu.VMEM((CHIP, COLS), f32),
            pltpu.VMEM((len(LINKS), CHIP, COLS), f32),
            pltpu.VMEM((C, TILES, 128), f32),
            pltpu.VMEM((C * Y - 1, TILES, 128), f32),
            pltpu.VMEM((TILES, 128), f32),
            pltpu.VMEM((Z, TILES, 128), f32),
            pltpu.VMEM((TILES, 128), f32),
            pltpu.VMEM((2, 128), f32),
            pltpu.VMEM((C * Y - 1, 2, 128), f32),
            pltpu.VMEM((Z, 2, 128), f32),
            pltpu.VMEM((X, Z, 2, 128), f32),
            dma((5,)), dma((2,)), dma((1,)), dma((1,)), dma((1,)), dma((3,)), dma((4,)),
            dma((1,)), dma((1,)), dma((share_flags(plan()[0])[1],)), dma((2,)), dma((2,)),
            pltpu.SemaphoreType.REGULAR((2,)),
        ],
        compiler_params=pltpu.CompilerParams(
            collective_id=0, has_side_effects=True, vmem_limit_bytes=24 * 2**20
        ),
        name="gather",
    )(
        *(
            pltpu.with_memory_space_constraint(a, pltpu.HBM)
            for a in (mix_share, one_gate, other_gate, one_up, other_up, norm_train, norm_step)
        )
    )
    tiles, cols, norm = (pltpu.with_memory_space_constraint(a, pltpu.VMEM) for a in (tiles, cols, norm))
    gate, up, col_gate, col_up, gain = pl.pallas_call(
        write_kernel,
        out_shape=(
            jax.ShapeDtypeStruct((ROWS, COLS), bf16),
            jax.ShapeDtypeStruct((ROWS, COLS), bf16),
            jax.ShapeDtypeStruct((TILES, 128), f32),
            jax.ShapeDtypeStruct((TILES, 128), f32),
            jax.ShapeDtypeStruct((2 * Z, 128), bf16),
        ),
        in_specs=[vmem_spec] * 3,
        out_specs=(hbm_spec,) * 5,
        scratch_shapes=[pltpu.VMEM((2 * Z, 128), bf16), dma((11,))],
        compiler_params=pltpu.CompilerParams(vmem_limit_bytes=8 * 2**20),
        name="write",
    )(tiles, cols, norm)
    return gate, up, col_gate.reshape(COLS), col_up.reshape(COLS), gain.reshape(ROWS)


def solution(mesh):
    torus = Mesh(mesh.devices.reshape(Z, Y, C, X), SHARD_MODEL)
    return jax.shard_map(
        local,
        mesh=torus,
        in_specs=(
            P(SHARD, "model"), P(SHARD, "model"), P(SHARD, "model"), P(SHARD, "model"),
            P(SHARD), P(SHARD_MODEL), P(SHARD_MODEL),
        ),
        out_specs=(P(None, "model"), P(None, "model"), P("model"), P("model"), P()),
        check_vma=False,
    )
```

```python
import heapq

import jax
import jax.numpy as jnp
from jax import lax
from jax.experimental import pallas as pl
from jax.experimental.pallas import tpu as pltpu
from jax.sharding import Mesh
from jax.sharding import PartitionSpec as P

SHARD = ("shard_0", "shard_1", "shard_2")
SHARD_MODEL = ("shard_0", "shard_1", "shard_2", "model")

Z, Y, C, X = 8, 4, 2, 4
ROWS, COLS, OWN = 2048, 2048, 32
CHIP = C * OWN
TILES = COLS // 128
LOW = -3.0e38
LATE = 60

PIECES = (("A", 1, "own", 0, 6), ("B", 0, "own", 6, 16), ("A", 0, "other", 0, 7), ("B", 1, "other", 7, 16))
FIRST = (3, 1, 0, 2)
EARLY = {"y": ((0, 2, 1), ()), "z": ((1,), (3,))}
LINKS = ("y+", "y-", "z+", "z-")
STEP = {"y+": (0, 1), "y-": (0, -1), "z+": (1, 0), "z-": (-1, 0)}


def is_early(piece, link):
    return any(piece in some for some in EARLY[link[0]])


def reach(half, n):
    return (n // 2, n // 2 - 1) if half == 0 else (n // 2 - 1, n // 2)


def forwards(piece, dz, dy):
    kind, half = PIECES[piece][:2]
    zp, zm = reach(half, Z)
    yp, ym = reach(half, Y)
    along_z, along_y = [], []
    if 0 <= dz < zp:
        along_z.append(("z+", dz + 1, dy))
    if -zm < dz <= 0:
        along_z.append(("z-", dz - 1, dy))
    if 0 <= dy < yp:
        along_y.append(("y+", dz, dy + 1))
    if -ym < dy <= 0:
        along_y.append(("y-", dz, dy - 1))
    if kind == "A":
        return along_z + (along_y if dz == 0 else [])
    return (along_z if dy == 0 else []) + along_y


def plan(hop=2.0, turn=0.04, block=5.6, swap=1.6, first=0.8, over_y=4.2, letters=0.9, over_z=8.2, work=0.08):
    free = {link: first if link[0] == "y" else 0.0 for link in LINKS}
    queue, order, count = [], [], 0

    def put(piece, link, z, y, at, early=False):
        nonlocal count
        width = (PIECES[piece][4] - PIECES[piece][3]) / TILES / C
        free[link] = max(at, free[link]) + width * block * (2 if early else 1)
        count += 1
        rank = FIRST.index(piece) if early else len(PIECES)
        heapq.heappush(queue, (max(free[link] + hop, over_z), rank, count, piece, z, y))

    for k, begin in enumerate((0.0, over_y)):
        for link in LINKS:
            for piece in EARLY[link[0]][k]:
                put(piece, link, *STEP[link], max(begin, swap if PIECES[piece][2] == "other" else 0.0), True)
        if k == 0:
            for link in ("z+", "z-"):
                free[link] = max(free[link], over_y) + letters
    clock = over_z
    for piece in range(len(PIECES)):
        if not all(is_early(piece, link) for link in LINKS):
            heapq.heappush(queue, (over_z, FIRST.index(piece) - 100, 0, piece, 0, 0))
    while queue:
        at, _, _, piece, dz, dy = heapq.heappop(queue)
        clock = max(clock, at) + turn
        order.append((piece, dz, dy))
        links = [l for l in LINKS if STEP[l] == (dz, dy)]
        if (dz, dy) == (0, 0) or links and is_early(piece, links[0]):
            clock += work
        for link, to_z, to_y in forwards(piece, dz, dy):
            if (dz, dy) != (0, 0) or not is_early(piece, link):
                put(piece, link, to_z, to_y, clock)
        clock += turn
    return order, clock


def came_by(piece, dz, dy):
    along_z = dz != 0 and (PIECES[piece][0] == "A" or dy == 0)
    link = ("z" if along_z else "y") + ("+" if (dz if along_z else dy) > 0 else "-")
    return link, (piece, dz - STEP[link][0], dy - STEP[link][1])


def share_flags(order):
    at = {event: k for k, event in enumerate(order)}
    known = {link: [-1] * len(order) for link in LINKS}
    for k, event in enumerate(order):
        for link in LINKS:
            known[link][k] = known[link][k - 1] if k else -1
        if event[1:] != (0, 0):
            link, before = came_by(*event)
            if before[1:] != (0, 0) or not is_early(event[0], link):
                back = link[0] + ("-" if link[1] == "+" else "+")
                known[back][k] = max(known[back][k], at[before])
    flags, last, twins = {}, [], {}
    for k, event in enumerate(order):
        if event[1:] == (0, 0) or event in flags:
            continue
        link, before = came_by(*event)
        early = before[1:] == (0, 0) and is_early(event[0], link)
        seen = -1 if early else known[link][at[before]]
        twin = order[k + 1] if k + 1 < len(order) else None
        if twin in ((event[0], -event[1], event[2]), (event[0], event[1], -event[2])):
            link2, before2 = came_by(*twin)
            if (before2[1:] == (0, 0) and is_early(twin[0], link2)) == early:
                twins[event] = twin
                if not early:
                    seen = min(seen, known[link2][at[before2]])
        free = [] if early else [i for i, used in enumerate(last) if used <= seen]
        if free:
            i = min(free, key=lambda i: last[i])
            last[i] = k
        else:
            i = len(last)
            last.append(k)
        flags[event] = i
        if event in twins:
            flags[twins[event]] = i
    return flags, len(last), twins


def gather_kernel(
    mix_h, one_g, other_g, one_u, other_u, train_h, step_h,
    out, cols, norm,
    mix, train, step, ins, theirs, x, raw, peak, peak_yc, peak1, peak_z, peak2,
    row0, row_yc, rows_z, rows_x,
    in_sem, x_sem, peak_send, yc_sem, z_sem, norm_send, norm_sem,
    raw_send, send_sem, recv_sem, side_send, side_recv, known,
):
    order, _ = plan()
    flags, _, twins = share_flags(order)
    waited = set(twins.values())
    z, y, c, m = (lax.axis_index(a) for a in SHARD_MODEL)
    mesh_id = pl.DeviceIdType.MESH
    z_at = [(lax.rem(z + d, Z), y, c, m) for d in range(Z)]
    y_at = [(z, lax.rem(y + d, Y), c, m) for d in range(Y)]
    yo_at = [(z, lax.rem(y + d, Y), 1 - c, m) for d in range(Y)]
    m_at = [(z, y, c, lax.rem(m + d, X)) for d in range(X)]
    sibling = yo_at[0]
    link_to = {"z+": z_at[1], "z-": z_at[Z - 1], "y+": y_at[1], "y-": y_at[Y - 1]}

    def remote(src, dst, send, recv, to):
        return pltpu.make_async_remote_copy(
            src_ref=src, dst_ref=dst, send_sem=send, recv_sem=recv, device_id=to, device_id_type=mesh_id
        )

    partners = [z_at[2], z_at[Z - 2], yo_at[2], y_at[2], *(z_at[d] for d in (1, Z - 1)), *(yo_at[d] for d in (1, 3))]
    partners += [y_at[1], y_at[3], sibling, m_at[1], m_at[X - 1]]
    barrier = pltpu.get_barrier_semaphore()
    for to in partners:
        pl.semaphore_signal(barrier, inc=1, device_id=to, device_id_type=mesh_id)

    small = [
        pltpu.make_async_copy(ref, to, in_sem.at[2 + i])
        for i, (ref, to) in enumerate(((mix_h, mix), (train_h, train), (step_h, step)))
    ]
    for copy in small:
        copy.start()
    for ours, pair in ((1 - c, (one_g, other_g)), (c, (one_u, other_u))):
        for k, ref in enumerate(pair):
            pltpu.make_async_copy(ref, ins.at[2 * ours + k], in_sem.at[ours]).start()
    for copy in small:
        copy.wait()

    sub = lax.broadcasted_iota(jnp.int32, (8, 128), 0)
    shares = []
    for r in range(OWN // 8):
        share = jnp.full((8, 128), mix[8 * r], jnp.float32)
        for i in range(1, 8):
            share = jnp.where(sub == i, mix[8 * r + i], share)
        shares.append((share, 1.0 - share))

    def blend(slot, to_peak, store):
        both = ins.at[pl.ds(slot, 2)]
        pltpu.make_async_copy(both, both, in_sem.at[slot // 2]).wait()
        for t in range(TILES):
            lanes = slice(128 * t, 128 * t + 128)
            best = None
            for r, (share, rest) in enumerate(shares):
                rows = slice(8 * r, 8 * r + 8)
                value = share * ins[slot, rows, lanes] + rest * ins[slot + 1, rows, lanes]
                store(r, lanes, value)
                best = jnp.abs(value) if best is None else jnp.maximum(best, jnp.abs(value))
            peak[to_peak, t : t + 1, :] = jnp.max(best, axis=0, keepdims=True)

    own_row, other_row = pl.multiple_of(OWN * c, OWN), pl.multiple_of(OWN * (1 - c), OWN)

    def store_theirs(r, lanes, value):
        theirs[8 * r : 8 * r + 8, lanes] = value

    def store_own(r, lanes, value):
        x[pl.ds(pl.multiple_of(own_row + 8 * r, 8), 8), lanes] = value

    blend(0, 1, store_theirs)
    blend(2, 0, store_own)

    lane2 = lax.broadcasted_iota(jnp.int32, (2, 128), 1)
    sub2 = lax.broadcasted_iota(jnp.int32, (2, 128), 0)
    start = (lax.rem(y, 2) * C + c) * OWN + m * 8
    line = jnp.full((2, 128), LOW, jnp.float32)
    for i in range(8):
        line = jnp.where((lane2 == start + i) & (sub2 == y // 2), train[i] + step[i], line)
    row0[...] = line

    pl.semaphore_wait(barrier, len(partners))

    for way, to in enumerate((z_at[2], z_at[Z - 2])):
        pl.semaphore_signal(known.at[way], inc=1, device_id=to, device_id_type=mesh_id)

    over_yc = []
    for d in (2, 1, 3):
        over_yc.append(remote(peak.at[1], peak_yc.at[2 * d], peak_send.at[0], yc_sem.at[0], yo_at[d]))
        over_yc.append(remote(peak.at[0], peak_yc.at[2 * d - 1], peak_send.at[0], yc_sem.at[0], y_at[d]))
    over_yc.append(remote(peak.at[1], peak_yc.at[0], peak_send.at[0], yc_sem.at[0], sibling))
    for copy in over_yc:
        copy.start()
    to_sibling = remote(theirs, x.at[pl.ds(own_row, OWN)], x_sem.at[0], x_sem.at[1], sibling)
    to_sibling.start()
    for d in (2, 1, 3):
        remote(row0, row_yc.at[2 * d], norm_send.at[0], norm_sem.at[0], yo_at[d]).start()
        remote(row0, row_yc.at[2 * d - 1], norm_send.at[0], norm_sem.at[0], y_at[d]).start()
    remote(row0, row_yc.at[0], norm_send.at[0], norm_sem.at[0], sibling).start()

    def arrived(ref, sem):
        pltpu.make_async_copy(ref, ref, sem).wait()

    def flag(*event):
        return recv_sem.at[flags[event]]

    def rows_of(piece):
        return own_row if PIECES[piece][2] == "own" else other_row

    def lanes_of(piece):
        first, last = PIECES[piece][3:]
        return pl.ds(128 * first, 128 * (last - first))

    def early(piece, link):
        at = (pl.ds(rows_of(piece), OWN), lanes_of(piece))
        return remote(
            x.at[at], raw.at[(LINKS.index(link), *at)], raw_send.at[0], flag(piece, *STEP[link]), link_to[link]
        )

    own_first = {}
    for link in LINKS:
        some = [PIECES[piece][2] for piece in EARLY[link[0]][0]] + ["other"]
        own_first[link] = some.index("other")
        for piece in EARLY[link[0]][0][: own_first[link]]:
            early(piece, link).start()
    to_sibling.wait_recv()
    for link in LINKS:
        for piece in EARLY[link[0]][0][own_first[link] :]:
            early(piece, link).start()

    arrived(peak_yc, yc_sem.at[0])
    best = peak[0]
    for d in range(C * Y - 1):
        best = jnp.maximum(best, peak_yc[d])
    peak1[...] = best

    for way in range(2):
        pl.semaphore_wait(known.at[way], 1)
    over_z = [remote(peak1, peak_z.at[d], peak_send.at[0], z_sem.at[0], z_at[d]) for d in range(1, Z)]
    for d in sorted(range(1, Z), key=lambda d: -min(d, Z - d)):
        over_z[d - 1].start()
    arrived(row_yc, norm_sem.at[0])
    line = row0[...]
    for d in range(C * Y - 1):
        line = jnp.maximum(line, row_yc[d])
    rows_z[z] = line
    for link in LINKS:
        for piece in EARLY[link[0]][1]:
            early(piece, link).start()
    for d in range(1, Z):
        remote(rows_z.at[z], rows_z.at[z], norm_send.at[1], norm_sem.at[1], z_at[d]).start()
    arrived(peak_z.at[pl.ds(1, Z - 1)], z_sem.at[0])
    for d in range(1, Z):
        best = jnp.maximum(best, peak_z[d])
    peak2[...] = best
    cols[c] = best

    def block_at(dz, dy):
        chip = lax.rem(z - dz + Z, Z) * Y + lax.rem(y - dy + Y, Y)
        return pl.multiple_of(chip * CHIP, CHIP)

    def scale(piece, source, base):
        for t in range(*PIECES[piece][3:]):
            lanes = slice(128 * t, 128 * t + 128)
            by = jnp.broadcast_to(peak2[t : t + 1, :], (16, 128))
            for r in range(OWN // 16):
                at = pl.multiple_of(rows_of(piece) + 16 * r, 16)
                value = source[pl.ds(at, 16), lanes] / by
                out[c, pl.ds(pl.multiple_of(base + at, 16), 16), lanes] = value.astype(jnp.bfloat16)

    def send_on(piece, dz, dy, base):
        ref = out.at[c, pl.ds(pl.multiple_of(base + rows_of(piece), OWN), OWN), lanes_of(piece)]
        for link, to_z, to_y in forwards(piece, dz, dy):
            if (dz, dy) == (0, 0) and is_early(piece, link):
                continue
            remote(ref, ref, send_sem.at[0], flag(piece, to_z, to_y), link_to[link]).start()

    def send_aside(base, rows=CHIP, lanes=pl.ds(0, COLS)):
        ref = out.at[c, pl.ds(base, rows), lanes]
        remote(ref, ref, side_send.at[0], side_recv.at[0], sibling).start()

    home = block_at(0, 0)

    def norm_beside():
        arrived(rows_z.at[pl.ds(0, Z - 1)], norm_sem.at[1])
        for d in (1, X - 1):
            remote(rows_z, rows_x.at[d], norm_send.at[2], norm_sem.at[2], m_at[d]).start()

    def norm_across():
        arrived(rows_x.at[pl.ds(0, 2)], norm_sem.at[2])
        remote(rows_x.at[1], rows_x.at[2], norm_send.at[2], norm_sem.at[3], m_at[1]).start()

    def norm_done():
        arrived(rows_x.at[2], norm_sem.at[3])
        for k in range(Z):
            line = rows_z[k]
            for d in range(1, X):
                line = jnp.maximum(line, rows_x[d, k])
            norm[k] = line

    def own_rest():
        for piece in range(len(PIECES)):
            if (piece, 0, 0) not in order:
                scale(piece, x, home)

    def own_aside():
        send_aside(home)
        remote(cols.at[c], cols.at[c], side_send.at[1], side_recv.at[1], sibling).start()

    n = len(order)
    aside = {n // 8: own_rest, n // 8 + 2: own_aside, n // 4: norm_beside, n // 2: norm_across, 3 * n // 4: norm_done}
    blocks = {}
    for k, (_, dz, dy) in enumerate(order):
        blocks.setdefault((dz % Z, dy % Y), []).append(k)
    blocks.pop((0, 0), None)
    pending = None
    for k, (piece, dz, dy) in enumerate(order):
        if k in aside:
            aside[k]()
        base = block_at(dz, dy)
        link = next((l for l in LINKS if STEP[l] == (dz, dy)), None)
        computed = (dz, dy) == (0, 0) or link is not None and is_early(piece, link)
        if (dz, dy) == (0, 0):
            scale(piece, x, base)
        elif computed:
            if (piece, dz, dy) not in waited:
                pair = 2 if (piece, dz, dy) in twins else 1
                arrived(ins.at[pl.ds(0, pair), :, lanes_of(piece)], flag(piece, dz, dy))
            scale(piece, raw.at[LINKS.index(link)], base)
        else:
            if (piece, dz, dy) not in waited:
                pair = 2 if (piece, dz, dy) in twins else 1
                arrived(out.at[0, pl.ds(0, pair * OWN), lanes_of(piece)], flag(piece, dz, dy))
        if pending:
            send_on(*pending)
        pending = (piece, dz, dy, base)
        if not computed:
            send_on(*pending)
            pending = None
        if (dz, dy) != (0, 0):
            last = blocks[dz % Z, dy % Y][-1]
            if last >= n - LATE:
                send_aside(pl.multiple_of(base + rows_of(piece), OWN), OWN, lanes_of(piece))
            elif last == k:
                send_aside(base)

    arrived(cols.at[0], side_send.at[1])
    arrived(cols.at[0], side_recv.at[1])
    to_sibling.wait_send()
    arrived(row_yc, norm_send.at[0])
    arrived(rows_z.at[pl.ds(0, Z - 1)], norm_send.at[1])
    arrived(rows_x.at[pl.ds(1, X - 1)], norm_send.at[2])
    arrived(theirs.at[:, pl.ds(0, 64 * (C * Y + Z - 2))], peak_send.at[0])
    wide = [last - first for _, _, _, first, last in PIECES]
    soon = [sum(is_early(piece, link) for link in LINKS) for piece in range(len(PIECES))]
    arrived(out.at[0, pl.ds(0, 16 * sum(a * b for a, b in zip(soon, wide))), pl.ds(0, 512)], raw_send.at[0])
    tiles = OWN // 8 * sum((Z * Y - 1 - a) * b for a, b in zip(soon, wide))
    across = max(w for w in range(1, TILES + 1) if tiles % w == 0)
    deep = 1 if tiles // across <= ROWS // 8 else 2
    assert tiles % (across * deep) == 0
    arrived(out.at[pl.ds(0, deep), pl.ds(0, tiles // across // deep * 8), pl.ds(0, 128 * across)], send_sem.at[0])
    whole = out.at[0]
    arrived(whole, side_send.at[0])
    arrived(whole, side_recv.at[0])


def write_kernel(tiles, cols, norm, gate, up, col_gate, col_up, gain, narrow, sem):
    parts = 4
    rows = ROWS // parts
    copies = []
    for i, ref in enumerate((gate, up)):
        for k in range(parts):
            at = pl.ds(k * rows, rows)
            copies.append(pltpu.make_async_copy(tiles.at[i, at], ref.at[at], sem.at[i * parts + k]))
    copies.append(pltpu.make_async_copy(cols.at[0], col_gate, sem.at[2 * parts]))
    copies.append(pltpu.make_async_copy(cols.at[1], col_up, sem.at[2 * parts + 1]))
    for copy in copies:
        copy.start()
    narrow[...] = jnp.concatenate([norm[k] for k in range(Z)], axis=0).astype(jnp.bfloat16)
    copies.append(pltpu.make_async_copy(narrow, gain, sem.at[2 * parts + 2]))
    copies[-1].start()
    for copy in copies:
        copy.wait()


def local(one_gate, other_gate, one_up, other_up, mix_share, norm_train, norm_step):
    f32, bf16 = jnp.float32, jnp.bfloat16
    hbm_spec = pl.BlockSpec(memory_space=pltpu.HBM)
    vmem_spec = pl.BlockSpec(memory_space=pltpu.VMEM)
    dma = pltpu.SemaphoreType.DMA
    tiles, cols, norm = pl.pallas_call(
        gather_kernel,
        out_shape=(
            pltpu.VMEM((2, ROWS, COLS), bf16),
            pltpu.VMEM((2, TILES, 128), f32),
            pltpu.VMEM((Z, 2, 128), f32),
        ),
        in_specs=[hbm_spec] * 7,
        out_specs=(vmem_spec,) * 3,
        scratch_shapes=[
            pltpu.SMEM((OWN,), f32), pltpu.SMEM((8,), f32), pltpu.SMEM((8,), f32),
            pltpu.VMEM((4, OWN, COLS), f32),
            pltpu.VMEM((OWN, COLS), f32),
            pltpu.VMEM((CHIP, COLS), f32),
            pltpu.VMEM((len(LINKS), CHIP, COLS), f32),
            pltpu.VMEM((C, TILES, 128), f32),
            pltpu.VMEM((C * Y - 1, TILES, 128), f32),
            pltpu.VMEM((TILES, 128), f32),
            pltpu.VMEM((Z, TILES, 128), f32),
            pltpu.VMEM((TILES, 128), f32),
            pltpu.VMEM((2, 128), f32),
            pltpu.VMEM((C * Y - 1, 2, 128), f32),
            pltpu.VMEM((Z, 2, 128), f32),
            pltpu.VMEM((X, Z, 2, 128), f32),
            dma((5,)), dma((2,)), dma((1,)), dma((1,)), dma((1,)), dma((3,)), dma((4,)),
            dma((1,)), dma((1,)), dma((share_flags(plan()[0])[1],)), dma((2,)), dma((2,)),
            pltpu.SemaphoreType.REGULAR((2,)),
        ],
        compiler_params=pltpu.CompilerParams(
            collective_id=0, has_side_effects=True, vmem_limit_bytes=24 * 2**20
        ),
        name="gather",
    )(
        *(
            pltpu.with_memory_space_constraint(a, pltpu.HBM)
            for a in (mix_share, one_gate, other_gate, one_up, other_up, norm_train, norm_step)
        )
    )
    tiles, cols, norm = (pltpu.with_memory_space_constraint(a, pltpu.VMEM) for a in (tiles, cols, norm))
    gate, up, col_gate, col_up, gain = pl.pallas_call(
        write_kernel,
        out_shape=(
            jax.ShapeDtypeStruct((ROWS, COLS), bf16),
            jax.ShapeDtypeStruct((ROWS, COLS), bf16),
            jax.ShapeDtypeStruct((TILES, 128), f32),
            jax.ShapeDtypeStruct((TILES, 128), f32),
            jax.ShapeDtypeStruct((2 * Z, 128), bf16),
        ),
        in_specs=[vmem_spec] * 3,
        out_specs=(hbm_spec,) * 5,
        scratch_shapes=[pltpu.VMEM((2 * Z, 128), bf16), dma((11,))],
        compiler_params=pltpu.CompilerParams(vmem_limit_bytes=8 * 2**20),
        name="write",
    )(tiles, cols, norm)
    return gate, up, col_gate.reshape(COLS), col_up.reshape(COLS), gain.reshape(ROWS)


def solution(mesh):
    torus = Mesh(mesh.devices.reshape(Z, Y, C, X), SHARD_MODEL)
    return jax.shard_map(
        local,
        mesh=torus,
        in_specs=(
            P(SHARD, "model"), P(SHARD, "model"), P(SHARD, "model"), P(SHARD, "model"),
            P(SHARD), P(SHARD_MODEL), P(SHARD_MODEL),
        ),
        out_specs=(P(None, "model"), P(None, "model"), P("model"), P("model"), P()),
        check_vma=False,
    )
```
